256 devices in a mesh: section: 16 (over y, x), row: 16 (over z, core).
Axes of the slice: x: 4, y: 4, z: 8, core: 2. Of those that a mesh axis runs over, the one named last changes fastest.
Arguments:
- omega: bfloat16 [8192, 16384], P('section', 'row'), may hold values from -0.25 to 0.25
- basis: bfloat16 [16384, 4096], P('row', 'section'), may hold values from -6 to 6
- vectors: bfloat16 [4, 16384], P(None, 'row'), may hold values from -6 to 6
Outputs:
- ortho: float32 [4, 16384], P(None, ('row', 'section'))
- coeffs: float32 [4, 4096], P(None, 'section')
The draws below stay inside these ranges and needn't reach their ends.
All inputs are finite; a program needn't handle non-finite values.
Results may differ from the reference program's by a relative error of at most 0.0021.
Values may be sent and summed in bfloat16 or wider, within the bound.
A program may use at most 64 MiB of HBM per device.

```python
import jax
import jax.numpy as jnp
from jax import lax

BLOCK = 256
NVEC = 4
SKETCH = 8192
NROWS = 16384
COLUMNS = 4096
N_SECTION = 16


def block_levels(own_key, extent, split, least, largest):
    gain = 1.0
    for position, parts in split:
        draws = jax.random.uniform(jax.random.fold_in(jax.random.fold_in(own_key, 6), position), (parts,), jnp.float32, least / len(split), largest / len(split))
        gain = gain * jnp.repeat(jnp.exp(draws), extent[position] // parts).reshape((-1,) + (1,) * (len(extent) - 1 - position))
    return gain


def centred(own_key, extent, width, bound, shards=(), dtype=jnp.bfloat16):
    result = width * jax.random.normal(own_key, extent, jnp.float32)
    if shards:
        result = result * block_levels(own_key, extent, shards, -0.22, 0.18)
    return jnp.clip(result, -bound, bound).astype(dtype)


def setup_inputs(seed: int = 0) -> dict:
    arg_keys = jax.random.split(jax.random.key(seed), 4)
    return {
        "omega": centred(arg_keys[0], (SKETCH, NROWS), (SKETCH // 16) ** -0.5, 0.25, ((0, 16), (1, 16))),
        "basis": centred(arg_keys[1], (NROWS, COLUMNS), 1.0, 6.0, ((0, 16), (1, 16))),
        "vectors": centred(arg_keys[2], (NVEC, NROWS), 1.0, 6.0, ((1, 16),)),
    }


def lower_solve(factor, right):
    return lax.linalg.triangular_solve(factor, right, left_side=True, lower=True, transpose_a=False)

def factor_solve(factor, right):
    half = lower_solve(factor, right)
    return lax.linalg.triangular_solve(factor, half, left_side=True, lower=True, transpose_a=True)

def reference(omega, basis, vectors):
    hi = lax.Precision.HIGHEST
    probe = lax.dot_general(vectors.astype(jnp.float32), omega.astype(jnp.float32), (((1,), (1,)), ((), ())), preferred_element_type=jnp.float32)
    remain = vectors.astype(jnp.float32)
    pieces = []
    for block_id in range(N_SECTION):
        columns = basis[:, block_id * BLOCK:(block_id + 1) * BLOCK]
        sketch = jnp.dot(omega.astype(jnp.float32), columns.astype(jnp.float32), preferred_element_type=jnp.float32)
        gram = jnp.dot(sketch.T, sketch, precision=hi)
        factor = jnp.linalg.cholesky(gram)
        inner = jnp.dot(probe, sketch, precision=hi)
        coef = factor_solve(factor, inner.T).T
        probe = probe - jnp.dot(coef, sketch.T, precision=hi)
        pieces.append(coef)
        rounded = coef.astype(jnp.bfloat16)
        remain = remain - lax.dot_general(rounded.astype(jnp.float32), columns.astype(jnp.float32), (((1,), (1,)), ((), ())), preferred_element_type=jnp.float32)
    small = jnp.dot(probe, probe.T, precision=hi)
    lower = jnp.linalg.cholesky(small)
    ortho = lower_solve(lower, remain)
    return (ortho, jnp.concatenate(pieces, axis=1))
```

```python
import functools

import jax
import jax.numpy as jnp
from jax import lax
from jax.experimental import pallas as pl
from jax.experimental.pallas import tpu as pltpu
from jax.sharding import PartitionSpec as P

F32 = jnp.float32
BF16 = jnp.bfloat16
HI = lax.Precision.HIGHEST
MESH = pl.DeviceIdType.MESH


def split(x):
    hi = x.astype(BF16)
    return hi, (x - hi.astype(F32)).astype(BF16)


def dot3(a, b, dims):
    (ah, al), (bh, bl) = a, b

    def one(x, y):
        return lax.dot_general(x, y, (dims, ((), ())), preferred_element_type=F32)

    return one(ah, bh) + (one(al, bh) + one(ah, bl))


NN = ((1,), (0,))
NT = ((1,), (1,))
TN = ((0,), (0,))


def remote(src, dst, send, recv, section, row):
    return pltpu.make_async_remote_copy(
        src_ref=src,
        dst_ref=dst,
        send_sem=send,
        recv_sem=recv,
        device_id=(section, row),
        device_id_type=MESH,
    )


def gram_kernel(
    ns, nr, s_ref, gram_ref, next_ref, part, got, red, rs_send, rs_recv, ag_send, ag_recv, n_send, n_recv
):
    s, r = lax.axis_index("section"), lax.axis_index("row")
    rows = part.shape[0] // nr
    barrier = pltpu.get_barrier_semaphore()
    after, before = lax.rem(s + 1, ns), lax.rem(s + ns - 1, ns)
    for step in range(1, nr):
        pl.semaphore_signal(barrier, inc=1, device_id=(s, lax.rem(r + step, nr)), device_id_type=MESH)
    pl.semaphore_signal(barrier, inc=1, device_id=(after, r), device_id_type=MESH)
    pl.semaphore_signal(barrier, inc=1, device_id=(before, r), device_id_type=MESH)
    sp = split(s_ref[...])
    part[...] = dot3(sp, sp, TN)
    pl.semaphore_wait(barrier, nr + 1)
    shift = remote(s_ref, next_ref, n_send, n_recv, before, r)
    shift.start()
    scatter = []
    for step in range(1, nr):
        peer = lax.rem(r + step, nr)
        cp = remote(
            part.at[pl.ds(pl.multiple_of(peer * rows, rows), rows)],
            got.at[step],
            rs_send.at[step],
            rs_recv.at[step],
            s,
            peer,
        )
        cp.start()
        scatter.append(cp)
    for cp in scatter:
        cp.wait_recv()
    total = part[pl.ds(pl.multiple_of(r * rows, rows), rows), :]
    for step in range(1, nr):
        total = total + got[step]
    red[...] = total
    mine = pl.ds(pl.multiple_of(r * rows, rows), rows)
    gather = []
    for step in range(1, nr):
        peer = lax.rem(r + step, nr)
        cp = remote(red, gram_ref.at[mine], ag_send.at[step], ag_recv.at[step], s, peer)
        cp.start()
        gather.append(cp)
    gram_ref[mine, :] = total
    for step in range(1, nr):
        peer = lax.rem(r + nr - step, nr)
        theirs = pl.ds(pl.multiple_of(peer * rows, rows), rows)
        remote(red, gram_ref.at[theirs], ag_send.at[step], ag_recv.at[step], s, peer).wait_recv()
    for cp in scatter + gather:
        cp.wait_send()
    shift.wait()


def gram_call(sketch, ns, nr):
    n = sketch.shape[1]
    vm = pl.BlockSpec(memory_space=pltpu.VMEM)
    dma = pltpu.SemaphoreType.DMA
    return pl.pallas_call(
        functools.partial(gram_kernel, ns, nr),
        out_shape=(
            jax.ShapeDtypeStruct((n, n), F32),
            jax.ShapeDtypeStruct(sketch.shape, F32),
        ),
        in_specs=[vm],
        out_specs=(vm, vm),
        scratch_shapes=[
            pltpu.VMEM((n, n), F32),
            pltpu.VMEM((nr, n // nr, n), F32),
            pltpu.VMEM((n // nr, n), F32),
            dma((nr,)),
            dma((nr,)),
            dma((nr,)),
            dma((nr,)),
            dma,
            dma,
        ],
        compiler_params=pltpu.CompilerParams(collective_id=0, has_side_effects=True),
    )(sketch)


def packed(c):
    half = c.shape[1] // 2
    return jnp.concatenate([c[:4, :half], c[:4, half:]], axis=0)


def unpacked(c):
    wide = jnp.concatenate([c[:4], c[4:]], axis=1)
    return jnp.concatenate([wide, jnp.zeros_like(wide)], axis=0)


def chain_kernel(
    ns,
    nr,
    s_ref,
    next_ref,
    inv_ref,
    p0_ref,
    basis_ref,
    vec_ref,
    ortho_ref,
    coef_ref,
    cross,
    probe,
    moved,
    cout,
    cin,
    own,
    oin,
    sout,
    sin,
    bout,
    bin_,
    c_send,
    c_recv,
    p_send,
    p_recv,
    o_send,
    o_recv,
    s_send,
    s_recv,
    b_send,
    b_recv,
):
    s, r = lax.axis_index("section"), lax.axis_index("row")
    barrier = pltpu.get_barrier_semaphore()
    after, before = lax.rem(s + 1, ns), lax.rem(s + ns - 1, ns)
    for q in range(nr):
        for other in (after, before):
            pl.semaphore_signal(barrier, inc=1, device_id=(other, q), device_id_type=MESH)
    for step in range(1, nr):
        pl.semaphore_signal(barrier, inc=1, device_id=(s, lax.rem(r + step, nr)), device_id_type=MESH)
    for step in range(1, ns):
        pl.semaphore_signal(barrier, inc=1, device_id=(lax.rem(s + step, ns), r), device_id_type=MESH)

    sp = split(s_ref[...])
    nx = split(next_ref[...])
    iv = split(inv_ref[...])
    cross[...] = dot3(sp, nx, TN)
    pl.semaphore_wait(barrier, 3 * nr + ns - 2)

    @pl.when(s == 0)
    def _():
        p = p0_ref[...]
        probe[...] = p
        cout[...] = packed(dot3(split(p), sp, NN))
        copies = []
        for step in range(1, nr):
            peer = lax.rem(r + step, nr)
            cp = remote(cout, cin.at[r], c_send.at[step], c_recv.at[r], 0, peer)
            cp.start()
            copies.append(cp)
        cin[pl.ds(r, 1)] = cout[...][None]
        for cp in copies:
            cp.wait_send()
        for step in range(1, nr):
            peer = lax.rem(r + step, nr)
            remote(cout, cin.at[peer], c_send.at[step], c_recv.at[peer], 0, peer).wait_recv()

    @pl.when(s > 0)
    def _():
        remote(moved, probe, p_send, p_recv, before, r).wait_recv()

    p = probe[...]
    ahead = dot3(split(p), nx, NN)

    @pl.when(s > 0)
    def _():
        for q in range(nr):
            remote(cout, cin.at[q], c_send.at[q], c_recv.at[q], before, q).wait_recv()

    total = cin[0]
    for q in range(1, nr):
        total = total + cin[q]
    inner = unpacked(total)
    coef = dot3(split(inner), iv, NN)
    cs = split(coef)

    @pl.when(s < ns - 1)
    def _():
        cout[...] = packed(ahead - dot3(cs, split(cross[...]), NN))
        for q in range(nr):
            remote(cout, cin.at[r], c_send.at[q], c_recv.at[r], after, q).start()

    moved[...] = p - dot3(cs, sp, NT)

    @pl.when(s < ns - 1)
    def _():
        remote(moved, probe, p_send, p_recv, after, r).start()

    coef_ref[...] = coef[:4]
    term = lax.dot_general(coef.astype(BF16), basis_ref[...], (NT, ((), ())), preferred_element_type=F32)
    for k in range(ns // 2):
        own[k] = term[:, k * 128 : (k + 1) * 128]
    outs = []
    for step in range(1, ns):
        t = lax.rem(s + step, ns)
        cp = remote(own.at[lax.div(t, 2)], oin.at[s], o_send.at[step], o_recv.at[s], t, r)
        cp.start()
        outs.append(cp)
    oin[pl.ds(s, 1)] = own[pl.ds(lax.div(s, 2), 1)]

    @pl.when(s == ns - 1)
    def _():
        m = split(moved[...])
        sq = dot3(m, m, NT)
        sout[...] = jnp.concatenate([sq, jnp.zeros((8, 120), F32)], axis=1)
        copies = []
        for step in range(1, nr):
            peer = lax.rem(r + step, nr)
            cp = remote(sout, sin.at[r], s_send.at[step], s_recv.at[r], s, peer)
            cp.start()
            copies.append(cp)
        sin[pl.ds(r, 1)] = sout[...][None]
        for step in range(1, nr):
            peer = lax.rem(r + step, nr)
            remote(sout, sin.at[peer], s_send.at[step], s_recv.at[peer], s, peer).wait_recv()
        tot = sin[0]
        for q in range(1, nr):
            tot = tot + sin[q]
        bout[...] = tot
        bcs = []
        for t in range(ns - 1):
            cp = remote(bout, bin_, b_send.at[t], b_recv, t, r)
            cp.start()
            bcs.append(cp)
        for cp in copies + bcs:
            cp.wait_send()
        bin_[...] = tot

    for step in range(1, ns):
        t = lax.rem(s + step, ns)
        remote(own.at[0], oin.at[t], o_send.at[step], o_recv.at[t], t, r).wait_recv()
    removed = oin[0]
    for t in range(1, ns):
        removed = removed + oin[t]
    odd = lax.rem(s, 2) == 1
    removed = jnp.where(odd, removed[:4, 64:], removed[:4, :64])
    remain = vec_ref[...].astype(F32) - removed

    @pl.when(s < ns - 1)
    def _():
        remote(bout, bin_, b_send.at[0], b_recv, ns - 1, r).wait_recv()
        for q in range(nr):
            remote(cout, cin.at[q], c_send.at[q], c_recv.at[q], after, q).wait_send()
        remote(moved, probe, p_send, p_recv, after, r).wait_send()

    small = bin_[...]

    def at(i, k):
        return small[i : i + 1, k : k + 1]

    low = [[None] * 4 for _ in range(4)]
    rows = []
    for i in range(4):
        for k in range(i + 1):
            v = at(i, k)
            for m in range(k):
                v = v - low[i][m] * low[k][m]
            low[i][k] = jnp.sqrt(v) if i == k else v / low[k][k]
        x = remain[i : i + 1]
        for k in range(i):
            x = x - low[i][k] * rows[k]
        rows.append(x / low[i][i])
    ortho_ref[...] = jnp.concatenate(rows, axis=0)
    for cp in outs:
        cp.wait_send()


def chain_call(sketch, nxt, inv, probe, basis, mine, ns, nr):
    vm = pl.BlockSpec(memory_space=pltpu.VMEM)
    dma = pltpu.SemaphoreType.DMA
    k, n = sketch.shape
    return pl.pallas_call(
        functools.partial(chain_kernel, ns, nr),
        out_shape=(
            jax.ShapeDtypeStruct((4, mine.shape[1]), F32),
            jax.ShapeDtypeStruct((4, n), F32),
        ),
        in_specs=[vm] * 6,
        out_specs=(vm, vm),
        scratch_shapes=[
            pltpu.VMEM((n, n), F32),
            pltpu.VMEM((8, k), F32),
            pltpu.VMEM((8, k), F32),
            pltpu.VMEM((8, 128), F32),
            pltpu.VMEM((nr, 8, 128), F32),
            pltpu.VMEM((ns // 2, 8, 128), F32),
            pltpu.VMEM((ns, 8, 128), F32),
            pltpu.VMEM((8, 128), F32),
            pltpu.VMEM((nr, 8, 128), F32),
            pltpu.VMEM((8, 128), F32),
            pltpu.VMEM((8, 128), F32),
            dma((nr,)),
            dma((nr,)),
            dma,
            dma,
            dma((ns,)),
            dma((ns,)),
            dma((nr,)),
            dma((nr,)),
            dma((ns,)),
            dma,
        ],
        compiler_params=pltpu.CompilerParams(collective_id=1, has_side_effects=True),
    )(sketch, nxt, inv, probe, basis, mine)


def lower_solve(factor, right):
    return lax.linalg.triangular_solve(factor, right, left_side=True, lower=True, transpose_a=False)


def inverse(gram):
    factor = jnp.linalg.cholesky(gram)
    half = lower_solve(factor, jnp.eye(gram.shape[0], dtype=F32))
    return jnp.dot(half.T, half, precision=HI)


def body(omega, basis, vectors):
    ns, nr = lax.axis_size("section"), lax.axis_size("row")
    s = lax.axis_index("section")
    every = lax.all_gather(basis, "section", axis=1, tiled=True)
    spread = lax.psum_scatter(
        jnp.dot(omega, every, preferred_element_type=F32), "row", scatter_dimension=0, tiled=True
    )
    sketch = lax.all_to_all(spread, "section", split_axis=1, concat_axis=0, tiled=True)
    term = lax.dot_general(vectors, omega, (NT, ((), ())), preferred_element_type=F32)
    tiles = jnp.moveaxis(term.reshape(4, nr, -1), 1, 0)
    piece = lax.all_to_all(tiles, "row", 0, 0, tiled=True).sum(0)
    probe = lax.all_to_all(jnp.broadcast_to(piece[None], (ns, *piece.shape)), "section", 0, 0, tiled=True)
    probe = jnp.moveaxis(probe, 0, 1).reshape(4, -1)
    probe = jnp.concatenate([probe, jnp.zeros_like(probe)], axis=0)
    gram, nxt = gram_call(sketch, ns, nr)
    inv = inverse(gram)
    width = vectors.shape[1] // ns
    mine = lax.dynamic_slice_in_dim(vectors, s * width, width, 1)
    return chain_call(sketch, nxt, inv, probe, basis, mine, ns, nr)


def solution(mesh):
    placed = (P("section", "row"), P("row", "section"), P(None, "row"))
    return jax.shard_map(
        body,
        mesh=mesh,
        in_specs=placed,
        out_specs=(P(None, ("row", "section")), P(None, "section")),
        check_vma=False,
    )
```

```python
import functools

import jax
import jax.numpy as jnp
from jax import lax
from jax.experimental import pallas as pl
from jax.experimental.pallas import tpu as pltpu
from jax.sharding import PartitionSpec as P

F32 = jnp.float32
BF16 = jnp.bfloat16
HI = lax.Precision.HIGHEST
MESH = pl.DeviceIdType.MESH


def split(x):
    hi = x.astype(BF16)
    return hi, (x - hi.astype(F32)).astype(BF16)


def dot3(a, b, dims):
    (ah, al), (bh, bl) = a, b

    def one(x, y):
        return lax.dot_general(x, y, (dims, ((), ())), preferred_element_type=F32)

    return one(ah, bh) + (one(al, bh) + one(ah, bl))


NN = ((1,), (0,))
NT = ((1,), (1,))
TN = ((0,), (0,))


def remote(src, dst, send, recv, section, row):
    return pltpu.make_async_remote_copy(
        src_ref=src,
        dst_ref=dst,
        send_sem=send,
        recv_sem=recv,
        device_id=(section, row),
        device_id_type=MESH,
    )


def gram_kernel(
    ns, nr, s_ref, gram_ref, next_ref, part, got, red, rs_send, rs_recv, ag_send, ag_recv, n_send, n_recv
):
    s, r = lax.axis_index("section"), lax.axis_index("row")
    rows = part.shape[0] // nr
    barrier = pltpu.get_barrier_semaphore()
    after, before = lax.rem(s + 1, ns), lax.rem(s + ns - 1, ns)
    for step in range(1, nr):
        pl.semaphore_signal(barrier, inc=1, device_id=(s, lax.rem(r + step, nr)), device_id_type=MESH)
    pl.semaphore_signal(barrier, inc=1, device_id=(after, r), device_id_type=MESH)
    pl.semaphore_signal(barrier, inc=1, device_id=(before, r), device_id_type=MESH)
    sp = split(s_ref[...])
    part[...] = dot3(sp, sp, TN)
    pl.semaphore_wait(barrier, nr + 1)
    shift = remote(s_ref, next_ref, n_send, n_recv, before, r)
    shift.start()
    scatter = []
    for step in range(1, nr):
        peer = lax.rem(r + step, nr)
        cp = remote(
            part.at[pl.ds(pl.multiple_of(peer * rows, rows), rows)],
            got.at[step],
            rs_send.at[step],
            rs_recv.at[step],
            s,
            peer,
        )
        cp.start()
        scatter.append(cp)
    for cp in scatter:
        cp.wait_recv()
    total = part[pl.ds(pl.multiple_of(r * rows, rows), rows), :]
    for step in range(1, nr):
        total = total + got[step]
    red[...] = total
    mine = pl.ds(pl.multiple_of(r * rows, rows), rows)
    gather = []
    for step in range(1, nr):
        peer = lax.rem(r + step, nr)
        cp = remote(red, gram_ref.at[mine], ag_send.at[step], ag_recv.at[step], s, peer)
        cp.start()
        gather.append(cp)
    gram_ref[mine, :] = total
    for step in range(1, nr):
        peer = lax.rem(r + nr - step, nr)
        theirs = pl.ds(pl.multiple_of(peer * rows, rows), rows)
        remote(red, gram_ref.at[theirs], ag_send.at[step], ag_recv.at[step], s, peer).wait_recv()
    for cp in scatter + gather:
        cp.wait_send()
    shift.wait()


def gram_call(sketch, ns, nr):
    n = sketch.shape[1]
    vm = pl.BlockSpec(memory_space=pltpu.VMEM)
    dma = pltpu.SemaphoreType.DMA
    return pl.pallas_call(
        functools.partial(gram_kernel, ns, nr),
        out_shape=(
            jax.ShapeDtypeStruct((n, n), F32),
            jax.ShapeDtypeStruct(sketch.shape, F32),
        ),
        in_specs=[vm],
        out_specs=(vm, vm),
        scratch_shapes=[
            pltpu.VMEM((n, n), F32),
            pltpu.VMEM((nr, n // nr, n), F32),
            pltpu.VMEM((n // nr, n), F32),
            dma((nr,)),
            dma((nr,)),
            dma((nr,)),
            dma((nr,)),
            dma,
            dma,
        ],
        compiler_params=pltpu.CompilerParams(collective_id=0, has_side_effects=True),
    )(sketch)


def packed(c):
    half = c.shape[1] // 2
    return jnp.concatenate([c[:4, :half], c[:4, half:]], axis=0)


def unpacked(c):
    wide = jnp.concatenate([c[:4], c[4:]], axis=1)
    return jnp.concatenate([wide, jnp.zeros_like(wide)], axis=0)


def chain_kernel(
    ns,
    nr,
    s_ref,
    next_ref,
    inv_ref,
    p0_ref,
    basis_ref,
    vec_ref,
    ortho_ref,
    coef_ref,
    cross,
    probe,
    moved,
    cout,
    cin,
    own,
    oin,
    sout,
    sin,
    bout,
    bin_,
    c_send,
    c_recv,
    p_send,
    p_recv,
    o_send,
    o_recv,
    s_send,
    s_recv,
    b_send,
    b_recv,
):
    s, r = lax.axis_index("section"), lax.axis_index("row")
    barrier = pltpu.get_barrier_semaphore()
    after, before = lax.rem(s + 1, ns), lax.rem(s + ns - 1, ns)
    for q in range(nr):
        for other in (after, before):
            pl.semaphore_signal(barrier, inc=1, device_id=(other, q), device_id_type=MESH)
    for step in range(1, nr):
        pl.semaphore_signal(barrier, inc=1, device_id=(s, lax.rem(r + step, nr)), device_id_type=MESH)
    for step in range(1, ns):
        pl.semaphore_signal(barrier, inc=1, device_id=(lax.rem(s + step, ns), r), device_id_type=MESH)

    sp = split(s_ref[...])
    nx = split(next_ref[...])
    iv = split(inv_ref[...])
    cross[...] = dot3(sp, nx, TN)
    pl.semaphore_wait(barrier, 3 * nr + ns - 2)

    @pl.when(s == 0)
    def _():
        p = p0_ref[...]
        probe[...] = p
        cout[...] = packed(dot3(split(p), sp, NN))
        copies = []
        for step in range(1, nr):
            peer = lax.rem(r + step, nr)
            cp = remote(cout, cin.at[r], c_send.at[step], c_recv.at[r], 0, peer)
            cp.start()
            copies.append(cp)
        cin[pl.ds(r, 1)] = cout[...][None]
        for cp in copies:
            cp.wait_send()
        for step in range(1, nr):
            peer = lax.rem(r + step, nr)
            remote(cout, cin.at[peer], c_send.at[step], c_recv.at[peer], 0, peer).wait_recv()

    @pl.when(s > 0)
    def _():
        remote(moved, probe, p_send, p_recv, before, r).wait_recv()

    p = probe[...]
    ahead = dot3(split(p), nx, NN)

    @pl.when(s > 0)
    def _():
        for q in range(nr):
            remote(cout, cin.at[q], c_send.at[q], c_recv.at[q], before, q).wait_recv()

    total = cin[0]
    for q in range(1, nr):
        total = total + cin[q]
    inner = unpacked(total)
    coef = dot3(split(inner), iv, NN)
    cs = split(coef)

    @pl.when(s < ns - 1)
    def _():
        cout[...] = packed(ahead - dot3(cs, split(cross[...]), NN))
        for q in range(nr):
            remote(cout, cin.at[r], c_send.at[q], c_recv.at[r], after, q).start()

    moved[...] = p - dot3(cs, sp, NT)

    @pl.when(s < ns - 1)
    def _():
        remote(moved, probe, p_send, p_recv, after, r).start()

    coef_ref[...] = coef[:4]
    term = lax.dot_general(coef.astype(BF16), basis_ref[...], (NT, ((), ())), preferred_element_type=F32)
    for k in range(ns // 2):
        own[k] = term[:, k * 128 : (k + 1) * 128]
    outs = []
    for step in range(1, ns):
        t = lax.rem(s + step, ns)
        cp = remote(own.at[lax.div(t, 2)], oin.at[s], o_send.at[step], o_recv.at[s], t, r)
        cp.start()
        outs.append(cp)
    oin[pl.ds(s, 1)] = own[pl.ds(lax.div(s, 2), 1)]

    @pl.when(s == ns - 1)
    def _():
        m = split(moved[...])
        sq = dot3(m, m, NT)
        sout[...] = jnp.concatenate([sq, jnp.zeros((8, 120), F32)], axis=1)
        copies = []
        for step in range(1, nr):
            peer = lax.rem(r + step, nr)
            cp = remote(sout, sin.at[r], s_send.at[step], s_recv.at[r], s, peer)
            cp.start()
            copies.append(cp)
        sin[pl.ds(r, 1)] = sout[...][None]
        for step in range(1, nr):
            peer = lax.rem(r + step, nr)
            remote(sout, sin.at[peer], s_send.at[step], s_recv.at[peer], s, peer).wait_recv()
        tot = sin[0]
        for q in range(1, nr):
            tot = tot + sin[q]
        bout[...] = tot
        bcs = []
        for t in range(ns - 1):
            cp = remote(bout, bin_, b_send.at[t], b_recv, t, r)
            cp.start()
            bcs.append(cp)
        for cp in copies + bcs:
            cp.wait_send()
        bin_[...] = tot

    for step in range(1, ns):
        t = lax.rem(s + step, ns)
        remote(own.at[0], oin.at[t], o_send.at[step], o_recv.at[t], t, r).wait_recv()
    removed = oin[0]
    for t in range(1, ns):
        removed = removed + oin[t]
    odd = lax.rem(s, 2) == 1
    removed = jnp.where(odd, removed[:4, 64:], removed[:4, :64])
    remain = vec_ref[...].astype(F32) - removed

    @pl.when(s < ns - 1)
    def _():
        remote(bout, bin_, b_send.at[0], b_recv, ns - 1, r).wait_recv()
        for q in range(nr):
            remote(cout, cin.at[q], c_send.at[q], c_recv.at[q], after, q).wait_send()
        remote(moved, probe, p_send, p_recv, after, r).wait_send()

    small = bin_[...]

    def at(i, k):
        return small[i : i + 1, k : k + 1]

    low = [[None] * 4 for _ in range(4)]
    rows = []
    for i in range(4):
        for k in range(i + 1):
            v = at(i, k)
            for m in range(k):
                v = v - low[i][m] * low[k][m]
            low[i][k] = jnp.sqrt(v) if i == k else v / low[k][k]
        x = remain[i : i + 1]
        for k in range(i):
            x = x - low[i][k] * rows[k]
        rows.append(x / low[i][i])
    ortho_ref[...] = jnp.concatenate(rows, axis=0)
    for cp in outs:
        cp.wait_send()


def chain_call(sketch, nxt, inv, probe, basis, mine, ns, nr):
    vm = pl.BlockSpec(memory_space=pltpu.VMEM)
    dma = pltpu.SemaphoreType.DMA
    k, n = sketch.shape
    return pl.pallas_call(
        functools.partial(chain_kernel, ns, nr),
        out_shape=(
            jax.ShapeDtypeStruct((4, mine.shape[1]), F32),
            jax.ShapeDtypeStruct((4, n), F32),
        ),
        in_specs=[vm] * 6,
        out_specs=(vm, vm),
        scratch_shapes=[
            pltpu.VMEM((n, n), F32),
            pltpu.VMEM((8, k), F32),
            pltpu.VMEM((8, k), F32),
            pltpu.VMEM((8, 128), F32),
            pltpu.VMEM((nr, 8, 128), F32),
            pltpu.VMEM((ns // 2, 8, 128), F32),
            pltpu.VMEM((ns, 8, 128), F32),
            pltpu.VMEM((8, 128), F32),
            pltpu.VMEM((nr, 8, 128), F32),
            pltpu.VMEM((8, 128), F32),
            pltpu.VMEM((8, 128), F32),
            dma((nr,)),
            dma((nr,)),
            dma,
            dma,
            dma((ns,)),
            dma((ns,)),
            dma((nr,)),
            dma((nr,)),
            dma((ns,)),
            dma,
        ],
        compiler_params=pltpu.CompilerParams(collective_id=1, has_side_effects=True),
    )(sketch, nxt, inv, probe, basis, mine)


def eliminate(a):
    n = a.shape[0]
    rows = lax.broadcasted_iota(jnp.int32, (n, n), 0)
    cols = lax.broadcasted_iota(jnp.int32, (n, n), 1)
    lane = lax.broadcasted_iota(jnp.int32, (1, n), 1)
    for k in range(0, n, 2):
        c1 = jnp.broadcast_to(a[:, k : k + 1], (n, n))
        c2 = jnp.broadcast_to(a[:, k + 1 : k + 2], (n, n))
        p, q, s = c1[k : k + 1], c2[k : k + 1], c2[k + 1 : k + 2]
        e = 1.0 / (p * s - q * q)
        r1 = jnp.where(lane == k, 1.0, jnp.where(lane == k + 1, 0.0, a[k : k + 1, :]))
        r2 = jnp.where(lane == k + 1, 1.0, jnp.where(lane == k, 0.0, a[k + 1 : k + 2, :]))
        w1 = (s * e) * r1 - (q * e) * r2
        w2 = (p * e) * r2 - (q * e) * r1
        base = jnp.where((cols == k) | (cols == k + 1), 0.0, a)
        new = base - c1 * w1 - c2 * w2
        last = jnp.where(rows == k + 1, jnp.broadcast_to(w2, (n, n)), new)
        a = jnp.where(rows == k, jnp.broadcast_to(w1, (n, n)), last)
    return a


def inverse_kernel(g_ref, out_ref):
    g = g_ref[...]
    n = g.shape[0]
    h = n // 2
    eye = lax.broadcasted_iota(jnp.int32, (n, n), 0) == lax.broadcasted_iota(jnp.int32, (n, n), 1)
    d = jnp.where(eye, g, 0.0)
    rs = lax.rsqrt(jnp.sum(d, axis=1, keepdims=True))
    cs = lax.rsqrt(jnp.sum(d, axis=0, keepdims=True))
    g = g * rs * cs

    def dot(x, y, dims):
        return lax.dot_general(x, y, (dims, ((), ())), precision=HI, preferred_element_type=F32)

    a, b, c = g[:h, :h], g[:h, h:], g[h:, h:]
    ai = eliminate(a)
    t = dot(ai, b, NN)
    ci = eliminate(c - dot(b, t, TN))
    u = dot(t, ci, NN)
    top = jnp.concatenate([ai + dot(u, t, NT), -u], axis=1)
    low = jnp.concatenate([-u.T, ci], axis=1)
    out_ref[...] = jnp.concatenate([top, low], axis=0) * rs * cs


def inverse(gram):
    vm = pl.BlockSpec(memory_space=pltpu.VMEM)
    return pl.pallas_call(
        inverse_kernel,
        out_shape=jax.ShapeDtypeStruct(gram.shape, F32),
        in_specs=[vm],
        out_specs=vm,
    )(gram)


def body(omega, basis, vectors):
    ns, nr = lax.axis_size("section"), lax.axis_size("row")
    s = lax.axis_index("section")
    every = lax.all_gather(basis, "section", axis=1, tiled=True)
    spread = lax.psum_scatter(
        jnp.dot(omega, every, preferred_element_type=F32), "row", scatter_dimension=0, tiled=True
    )
    sketch = lax.all_to_all(spread, "section", split_axis=1, concat_axis=0, tiled=True)
    term = lax.dot_general(vectors, omega, (NT, ((), ())), preferred_element_type=F32)
    tiles = jnp.moveaxis(term.reshape(4, nr, -1), 1, 0)
    piece = lax.all_to_all(tiles, "row", 0, 0, tiled=True).sum(0)
    probe = lax.all_to_all(jnp.broadcast_to(piece[None], (ns, *piece.shape)), "section", 0, 0, tiled=True)
    probe = jnp.moveaxis(probe, 0, 1).reshape(4, -1)
    probe = jnp.concatenate([probe, jnp.zeros_like(probe)], axis=0)
    gram, nxt = gram_call(sketch, ns, nr)
    inv = inverse(gram)
    width = vectors.shape[1] // ns
    mine = lax.dynamic_slice_in_dim(vectors, s * width, width, 1)
    return chain_call(sketch, nxt, inv, probe, basis, mine, ns, nr)


def solution(mesh):
    placed = (P("section", "row"), P("row", "section"), P(None, "row"))
    return jax.shard_map(
        body,
        mesh=mesh,
        in_specs=placed,
        out_specs=(P(None, ("row", "section")), P(None, "section")),
        check_vma=False,
    )
```

```python
import functools

import jax
import jax.numpy as jnp
from jax import lax
from jax.experimental import pallas as pl
from jax.experimental.pallas import tpu as pltpu
from jax.sharding import PartitionSpec as P

F32 = jnp.float32
BF16 = jnp.bfloat16
HI = lax.Precision.HIGHEST
MESH = pl.DeviceIdType.MESH


def split(x):
    hi = x.astype(BF16)
    return hi, (x - hi.astype(F32)).astype(BF16)


def dot3(a, b, dims):
    (ah, al), (bh, bl) = a, b

    def one(x, y):
        return lax.dot_general(x, y, (dims, ((), ())), preferred_element_type=F32)

    return one(ah, bh) + (one(al, bh) + one(ah, bl))


NN = ((1,), (0,))
NT = ((1,), (1,))
TN = ((0,), (0,))


def remote(src, dst, send, recv, section, row):
    return pltpu.make_async_remote_copy(
        src_ref=src,
        dst_ref=dst,
        send_sem=send,
        recv_sem=recv,
        device_id=(section, row),
        device_id_type=MESH,
    )


def gram_kernel(
    ns, nr, s_ref, gram_ref, next_ref, part, got, red, rs_send, rs_recv, ag_send, ag_recv, n_send, n_recv
):
    s, r = lax.axis_index("section"), lax.axis_index("row")
    rows = part.shape[0] // nr
    barrier = pltpu.get_barrier_semaphore()
    after, before = lax.rem(s + 1, ns), lax.rem(s + ns - 1, ns)
    for step in range(1, nr):
        pl.semaphore_signal(barrier, inc=1, device_id=(s, lax.rem(r + step, nr)), device_id_type=MESH)
    pl.semaphore_signal(barrier, inc=1, device_id=(after, r), device_id_type=MESH)
    pl.semaphore_signal(barrier, inc=1, device_id=(before, r), device_id_type=MESH)
    sp = split(s_ref[...])
    part[...] = dot3(sp, sp, TN)
    pl.semaphore_wait(barrier, nr + 1)
    shift = remote(s_ref, next_ref, n_send, n_recv, before, r)
    shift.start()
    scatter = []
    for step in range(1, nr):
        peer = lax.rem(r + step, nr)
        cp = remote(
            part.at[pl.ds(pl.multiple_of(peer * rows, rows), rows)],
            got.at[step],
            rs_send.at[step],
            rs_recv.at[step],
            s,
            peer,
        )
        cp.start()
        scatter.append(cp)
    for cp in scatter:
        cp.wait_recv()
    total = part[pl.ds(pl.multiple_of(r * rows, rows), rows), :]
    for step in range(1, nr):
        total = total + got[step]
    red[...] = total
    mine = pl.ds(pl.multiple_of(r * rows, rows), rows)
    gather = []
    for step in range(1, nr):
        peer = lax.rem(r + step, nr)
        cp = remote(red, gram_ref.at[mine], ag_send.at[step], ag_recv.at[step], s, peer)
        cp.start()
        gather.append(cp)
    gram_ref[mine, :] = total
    for step in range(1, nr):
        peer = lax.rem(r + nr - step, nr)
        theirs = pl.ds(pl.multiple_of(peer * rows, rows), rows)
        remote(red, gram_ref.at[theirs], ag_send.at[step], ag_recv.at[step], s, peer).wait_recv()
    for cp in scatter + gather:
        cp.wait_send()
    shift.wait()


def gram_call(sketch, ns, nr):
    n = sketch.shape[1]
    vm = pl.BlockSpec(memory_space=pltpu.VMEM)
    dma = pltpu.SemaphoreType.DMA
    return pl.pallas_call(
        functools.partial(gram_kernel, ns, nr),
        out_shape=(
            jax.ShapeDtypeStruct((n, n), F32),
            jax.ShapeDtypeStruct(sketch.shape, F32),
        ),
        in_specs=[vm],
        out_specs=(vm, vm),
        scratch_shapes=[
            pltpu.VMEM((n, n), F32),
            pltpu.VMEM((nr, n // nr, n), F32),
            pltpu.VMEM((n // nr, n), F32),
            dma((nr,)),
            dma((nr,)),
            dma((nr,)),
            dma((nr,)),
            dma,
            dma,
        ],
        compiler_params=pltpu.CompilerParams(collective_id=0, has_side_effects=True),
    )(sketch)


def packed(c):
    half = c.shape[1] // 2
    return jnp.concatenate([c[:4, :half], c[:4, half:]], axis=0)


def unpacked(c):
    wide = jnp.concatenate([c[:4], c[4:]], axis=1)
    return jnp.concatenate([wide, jnp.zeros_like(wide)], axis=0)


def chain_kernel(
    ns,
    nr,
    s_ref,
    next_ref,
    inv_ref,
    p0_ref,
    basis_ref,
    vec_ref,
    ortho_ref,
    coef_ref,
    cross,
    probe,
    moved,
    cout,
    cin,
    own,
    oin,
    sout,
    sin,
    bout,
    bin_,
    c_send,
    c_recv,
    p_send,
    p_recv,
    o_send,
    o_recv,
    s_send,
    s_recv,
    b_send,
    b_recv,
):
    s, r = lax.axis_index("section"), lax.axis_index("row")
    barrier = pltpu.get_barrier_semaphore()
    after, before = lax.rem(s + 1, ns), lax.rem(s + ns - 1, ns)
    for q in range(nr):
        for other in (after, before):
            pl.semaphore_signal(barrier, inc=1, device_id=(other, q), device_id_type=MESH)
    for step in range(1, nr):
        pl.semaphore_signal(barrier, inc=1, device_id=(s, lax.rem(r + step, nr)), device_id_type=MESH)
    for step in range(1, ns):
        pl.semaphore_signal(barrier, inc=1, device_id=(lax.rem(s + step, ns), r), device_id_type=MESH)

    sp = split(s_ref[...])
    nx = split(next_ref[...])
    iv = split(inv_ref[...])
    cross[...] = dot3(sp, nx, TN)
    pl.semaphore_wait(barrier, 3 * nr + ns - 2)

    @pl.when(s == 0)
    def _():
        p = p0_ref[...].T[:8]
        probe[...] = p
        cout[...] = packed(dot3(split(p), sp, NN))
        copies = []
        for step in range(1, nr):
            peer = lax.rem(r + step, nr)
            cp = remote(cout, cin.at[r], c_send.at[step], c_recv.at[r], 0, peer)
            cp.start()
            copies.append(cp)
        cin[pl.ds(r, 1)] = cout[...][None]
        for cp in copies:
            cp.wait_send()
        for step in range(1, nr):
            peer = lax.rem(r + step, nr)
            remote(cout, cin.at[peer], c_send.at[step], c_recv.at[peer], 0, peer).wait_recv()

    @pl.when(s > 0)
    def _():
        remote(moved, probe, p_send, p_recv, before, r).wait_recv()

    p = probe[...]
    ahead = dot3(split(p), nx, NN)

    @pl.when(s > 0)
    def _():
        for q in range(nr):
            remote(cout, cin.at[q], c_send.at[q], c_recv.at[q], before, q).wait_recv()

    total = cin[0]
    for q in range(1, nr):
        total = total + cin[q]
    inner = unpacked(total)
    coef = dot3(split(inner), iv, NN)
    cs = split(coef)

    @pl.when(s < ns - 1)
    def _():
        cout[...] = packed(ahead - dot3(cs, split(cross[...]), NN))
        for q in range(nr):
            remote(cout, cin.at[r], c_send.at[q], c_recv.at[r], after, q).start()

    moved[...] = p - dot3(cs, sp, NT)

    @pl.when(s < ns - 1)
    def _():
        remote(moved, probe, p_send, p_recv, after, r).start()

    coef_ref[...] = coef[:4]
    term = lax.dot_general(coef.astype(BF16), basis_ref[...], (NT, ((), ())), preferred_element_type=F32)
    for k in range(ns // 2):
        own[k] = term[:, k * 128 : (k + 1) * 128]
    outs = []
    for step in range(1, ns):
        t = lax.rem(s + step, ns)
        cp = remote(own.at[lax.div(t, 2)], oin.at[s], o_send.at[step], o_recv.at[s], t, r)
        cp.start()
        outs.append(cp)
    oin[pl.ds(s, 1)] = own[pl.ds(lax.div(s, 2), 1)]

    @pl.when(s == ns - 1)
    def _():
        m = split(moved[...])
        sq = dot3(m, m, NT)
        sout[...] = jnp.concatenate([sq, jnp.zeros((8, 120), F32)], axis=1)
        copies = []
        for step in range(1, nr):
            peer = lax.rem(r + step, nr)
            cp = remote(sout, sin.at[r], s_send.at[step], s_recv.at[r], s, peer)
            cp.start()
            copies.append(cp)
        sin[pl.ds(r, 1)] = sout[...][None]
        for step in range(1, nr):
            peer = lax.rem(r + step, nr)
            remote(sout, sin.at[peer], s_send.at[step], s_recv.at[peer], s, peer).wait_recv()
        tot = sin[0]
        for q in range(1, nr):
            tot = tot + sin[q]
        bout[...] = tot
        bcs = []
        for t in range(ns - 1):
            cp = remote(bout, bin_, b_send.at[t], b_recv, t, r)
            cp.start()
            bcs.append(cp)
        for cp in copies + bcs:
            cp.wait_send()
        bin_[...] = tot

    for step in range(1, ns):
        t = lax.rem(s + step, ns)
        remote(own.at[0], oin.at[t], o_send.at[step], o_recv.at[t], t, r).wait_recv()
    removed = oin[0]
    for t in range(1, ns):
        removed = removed + oin[t]
    odd = lax.rem(s, 2) == 1
    removed = jnp.where(odd, removed[:4, 64:], removed[:4, :64])
    remain = vec_ref[...].astype(F32) - removed

    @pl.when(s < ns - 1)
    def _():
        remote(bout, bin_, b_send.at[0], b_recv, ns - 1, r).wait_recv()
        for q in range(nr):
            remote(cout, cin.at[q], c_send.at[q], c_recv.at[q], after, q).wait_send()
        remote(moved, probe, p_send, p_recv, after, r).wait_send()

    small = bin_[...]

    def at(i, k):
        return small[i : i + 1, k : k + 1]

    low = [[None] * 4 for _ in range(4)]
    rows = []
    for i in range(4):
        for k in range(i + 1):
            v = at(i, k)
            for m in range(k):
                v = v - low[i][m] * low[k][m]
            low[i][k] = jnp.sqrt(v) if i == k else v / low[k][k]
        x = remain[i : i + 1]
        for k in range(i):
            x = x - low[i][k] * rows[k]
        rows.append(x / low[i][i])
    ortho_ref[...] = jnp.concatenate(rows, axis=0)
    for cp in outs:
        cp.wait_send()


def chain_call(sketch, nxt, inv, probe, basis, mine, ns, nr):
    vm = pl.BlockSpec(memory_space=pltpu.VMEM)
    dma = pltpu.SemaphoreType.DMA
    k, n = sketch.shape
    return pl.pallas_call(
        functools.partial(chain_kernel, ns, nr),
        out_shape=(
            jax.ShapeDtypeStruct((4, mine.shape[1]), F32),
            jax.ShapeDtypeStruct((4, n), F32),
        ),
        in_specs=[vm] * 6,
        out_specs=(vm, vm),
        scratch_shapes=[
            pltpu.VMEM((n, n), F32),
            pltpu.VMEM((8, k), F32),
            pltpu.VMEM((8, k), F32),
            pltpu.VMEM((8, 128), F32),
            pltpu.VMEM((nr, 8, 128), F32),
            pltpu.VMEM((ns // 2, 8, 128), F32),
            pltpu.VMEM((ns, 8, 128), F32),
            pltpu.VMEM((8, 128), F32),
            pltpu.VMEM((nr, 8, 128), F32),
            pltpu.VMEM((8, 128), F32),
            pltpu.VMEM((8, 128), F32),
            dma((nr,)),
            dma((nr,)),
            dma,
            dma,
            dma((ns,)),
            dma((ns,)),
            dma((nr,)),
            dma((nr,)),
            dma((ns,)),
            dma,
        ],
        compiler_params=pltpu.CompilerParams(collective_id=1, has_side_effects=True),
    )(sketch, nxt, inv, probe, basis, mine)


def eliminate(a):
    n = a.shape[0]
    rows = lax.broadcasted_iota(jnp.int32, (n, n), 0)
    cols = lax.broadcasted_iota(jnp.int32, (n, n), 1)
    lane = lax.broadcasted_iota(jnp.int32, (1, n), 1)
    for k in range(0, n, 2):
        c1 = jnp.broadcast_to(a[:, k : k + 1], (n, n))
        c2 = jnp.broadcast_to(a[:, k + 1 : k + 2], (n, n))
        p, q, s = c1[k : k + 1], c2[k : k + 1], c2[k + 1 : k + 2]
        e = 1.0 / (p * s - q * q)
        r1 = jnp.where(lane == k, 1.0, jnp.where(lane == k + 1, 0.0, a[k : k + 1, :]))
        r2 = jnp.where(lane == k + 1, 1.0, jnp.where(lane == k, 0.0, a[k + 1 : k + 2, :]))
        w1 = (s * e) * r1 - (q * e) * r2
        w2 = (p * e) * r2 - (q * e) * r1
        base = jnp.where((cols == k) | (cols == k + 1), 0.0, a)
        new = base - c1 * w1 - c2 * w2
        last = jnp.where(rows == k + 1, jnp.broadcast_to(w2, (n, n)), new)
        a = jnp.where(rows == k, jnp.broadcast_to(w1, (n, n)), last)
    return a


def inverse_kernel(g_ref, out_ref):
    g = g_ref[...]
    n = g.shape[0]
    h = n // 2
    eye = lax.broadcasted_iota(jnp.int32, (n, n), 0) == lax.broadcasted_iota(jnp.int32, (n, n), 1)
    d = jnp.where(eye, g, 0.0)
    rs = lax.rsqrt(jnp.sum(d, axis=1, keepdims=True))
    cs = lax.rsqrt(jnp.sum(d, axis=0, keepdims=True))
    g = g * rs * cs

    def dot(x, y, dims):
        return lax.dot_general(x, y, (dims, ((), ())), precision=HI, preferred_element_type=F32)

    a, b, c = g[:h, :h], g[:h, h:], g[h:, h:]
    ai = eliminate(a)
    t = dot(ai, b, NN)
    ci = eliminate(c - dot(b, t, TN))
    u = dot(t, ci, NN)
    top = jnp.concatenate([ai + dot(u, t, NT), -u], axis=1)
    low = jnp.concatenate([-u.T, ci], axis=1)
    out_ref[...] = jnp.concatenate([top, low], axis=0) * rs * cs


def inverse(gram):
    vm = pl.BlockSpec(memory_space=pltpu.VMEM)
    return pl.pallas_call(
        inverse_kernel,
        out_shape=jax.ShapeDtypeStruct(gram.shape, F32),
        in_specs=[vm],
        out_specs=vm,
    )(gram)


def slot_offset(d):
    return jnp.where(d == 0, 0, jnp.where(d == 1, 3, d - 1))


def sketch_kernel(
    nz,
    omega_ref,
    basis_ref,
    vec_ref,
    s_ref,
    p_ref,
    obuf,
    bbuf,
    keep,
    give,
    dbuf,
    rbuf,
    fbuf,
    pbuf,
    l_sem,
    o_send,
    o_recv,
    b_send,
    b_recv,
    d_send,
    d_recv,
    r_send,
    r_recv,
    f_send,
    f_recv,
    p_send,
    p_recv,
):
    s, r = lax.axis_index("section"), lax.axis_index("row")
    y, x = lax.div(s, 4), lax.rem(s, 4)
    z, c = lax.div(r, 2), lax.rem(r, 2)
    units, hops = 17, nz - 1

    def at(dy, dx):
        return lax.rem(y + dy, 4) * 4 + lax.rem(x + dx, 4)

    zp = lax.rem(z + 1, nz) * 2 + c
    zm = lax.rem(z + nz - 1, nz) * 2 + c
    mate = z * 2 + (1 - c)

    local = [
        pltpu.make_async_copy(basis_ref, bbuf.at[0], l_sem.at[0]),
        pltpu.make_async_copy(omega_ref, obuf.at[0], l_sem.at[1]),
        pltpu.make_async_copy(vec_ref, bbuf.at[4], l_sem.at[2]),
    ]
    for cp in local:
        cp.start()

    barrier = pltpu.get_barrier_semaphore()

    def hello(section, row):
        pl.semaphore_signal(barrier, inc=1, device_id=(section, row), device_id_type=MESH)

    for dy, dx in ((1, 0), (3, 0), (0, 1), (0, 2), (0, 3)):
        hello(at(dy, dx), r)
    for row in (zp, zm, mate):
        hello(s, row)

    @pl.when(s == 0)
    def _():
        for t in range(1, 16):
            hello(t, r)

    for cp in local:
        cp.wait()
    pl.semaphore_wait(barrier, 8 + jnp.minimum(s, 1))

    def ocopy(src, dst, half, sem, dy):
        a, b = obuf.at[src], obuf.at[dst]
        if half is not None:
            a, b = a.at[pl.ds(4 * half, 4)], b.at[pl.ds(4 * half, 4)]
        return remote(a, b, o_send.at[sem], o_recv.at[sem], at(dy, 0), r)

    def bcopy(src, dst, half, sem, dx):
        a, b = bbuf.at[src], bbuf.at[dst]
        if half is not None:
            a, b = a.at[pl.ds(512 * half, 512)], b.at[pl.ds(512 * half, 512)]
        return remote(a, b, b_send.at[sem], b_recv.at[sem], at(0, dx), r)

    b_own = [bcopy(0, 1, None, 0, 1), bcopy(0, 2, None, 1, 3)]
    o_own = [ocopy(0, 1, None, 0, 1), ocopy(0, 2, None, 1, 3)]
    b_fwd = [bcopy(1, 3, 0, 2, 1), bcopy(2, 3, 1, 3, 3)]
    o_fwd = [ocopy(1, 3, 0, 2, 1), ocopy(2, 3, 1, 3, 3)]
    for cp in b_own + o_own:
        cp.start()

    def dcopy(u):
        return remote(give.at[u], dbuf.at[u], d_send.at[u], d_recv.at[u], s, mate)

    def chunk(h, k):
        return lax.rem(z + nz - 1 - k, nz) if h == 0 else lax.rem(z + 1 + k, nz)

    def rcopy(u, h, k):
        return remote(
            keep.at[u, h, chunk(h, k)],
            rbuf.at[u, h, k],
            r_send.at[u, h, k],
            r_recv.at[u, h, k],
            s,
            zp if h == 0 else zm,
        )

    def place(u):
        v = u - 1
        return slot_offset(lax.div(v, 4)), slot_offset(lax.rem(v, 4))

    def fcopy(u):
        dy, dx = place(u)
        rows = pl.ds(pl.multiple_of((lax.rem(y + dy, 4) * 4 + x) * 32, 32), 32)
        return remote(fbuf.at[u], s_ref.at[rows], f_send.at[u], f_recv.at[u], at(0, dx), r)

    def pcopy(sender):
        return remote(pbuf, p_ref.at[sender], p_send, p_recv.at[sender], 0, r)

    def step(t, carry):
        for k in range(hops, -1, -1):
            u = t - 1 - k
            for h in range(2):
                first = 0 if h == 0 else 1

                @pl.when((u >= first) & (u < units))
                def _():
                    if k == 0:
                        if h == 0:
                            dcopy(u).wait_recv()
                    else:
                        rcopy(u, h, k - 1).wait_recv()
                    ch = chunk(h, k)
                    val = keep[u, h, ch] + dbuf[u, h, ch]
                    if k > 0:
                        val = val + rbuf[u, h, k - 1]
                    if k < hops:
                        keep[u, h, ch] = val
                        rcopy(u, h, k).start()
                    else:
                        fbuf[u, :, h * 128 : (h + 1) * 128] = val

        done = t - 1 - hops

        @pl.when((done >= 1) & (done < units))
        def _():
            dy, dx = place(done)

            @pl.when(dx == 0)
            def _():
                rows = pl.ds(pl.multiple_of((lax.rem(y + dy, 4) * 4 + x) * 32, 32), 32)
                s_ref[rows, :] = fbuf[done]

            @pl.when(dx > 0)
            def _():
                fcopy(done).start()

        @pl.when(done == 0)
        def _():
            @pl.when(s == 0)
            def _():
                p_ref[0] = fbuf[0, :, :128]

            @pl.when(s > 0)
            def _():
                pbuf[...] = fbuf[0, :, :128]
                pcopy(s).start()

        @pl.when(t == 2)
        def _():
            for cp in b_own:
                cp.wait_recv()
            for cp in b_fwd:
                cp.start()

        @pl.when(t == 4)
        def _():
            for cp in b_fwd:
                cp.wait_recv()

        @pl.when(t == 5)
        def _():
            for cp in o_own:
                cp.wait_recv()
            for cp in o_fwd:
                cp.start()

        @pl.when(t == 13)
        def _():
            for cp in o_fwd:
                cp.wait_recv()

        @pl.when(t < units)
        def _():
            v = jnp.maximum(t - 1, 0)
            oslot = lax.div(v, 4)
            bslot = jnp.where(t == 0, 4, lax.rem(v, 4))
            b = bbuf[bslot]
            for which, dst in ((1 - c, give), (c, keep)):
                o = obuf[oslot, :, which].reshape(256, 1024)
                out = jnp.dot(o, b, preferred_element_type=F32)
                for h in range(2):
                    dst[t, h] = out[:, h * 128 : (h + 1) * 128].reshape(8, 32, 128)
                if dst is give:
                    dcopy(t).start()

        return carry

    lax.fori_loop(0, units + nz, step, 0)

    for u in range(1, units):
        if (u - 1) % 4:
            fcopy(u).wait()

    @pl.when(s == 0)
    def _():
        for t in range(1, 16):
            pcopy(t).wait_recv()

    @pl.when(s > 0)
    def _():
        pcopy(s).wait_send()

    for cp in b_own + o_own + b_fwd + o_fwd:
        cp.wait_send()

    def drain(u, carry):
        dcopy(u).wait_send()
        for h in range(2):
            for k in range(hops):

                @pl.when(u >= h)
                def _():
                    rcopy(u, h, k).wait_send()

        return carry

    lax.fori_loop(0, units, drain, 0)


def sketch_call(omega, basis, vecs, nr):
    vm = pl.BlockSpec(memory_space=pltpu.VMEM)
    anym = pl.BlockSpec(memory_space=pl.ANY)
    dma = pltpu.SemaphoreType.DMA
    nz = nr // 2
    m, k = omega.shape
    n = basis.shape[1]
    part = m // nr
    units = 17
    return pl.pallas_call(
        functools.partial(sketch_kernel, nz),
        out_shape=(
            jax.ShapeDtypeStruct((m, n), F32),
            jax.ShapeDtypeStruct((16, part, 128), F32),
        ),
        in_specs=[anym] * 3,
        out_specs=(vm, vm),
        scratch_shapes=[
            pltpu.VMEM((4, nz, 2, part, k), BF16),
            pltpu.VMEM((5, k, n), BF16),
            pltpu.VMEM((units, 2, nz, part, 128), F32),
            pltpu.VMEM((units, 2, nz, part, 128), F32),
            pltpu.VMEM((units, 2, nz, part, 128), F32),
            pltpu.VMEM((units, 2, nz - 1, part, 128), F32),
            pltpu.VMEM((units, part, n), F32),
            pltpu.VMEM((part, 128), F32),
            dma((3,)),
            dma((4,)),
            dma((4,)),
            dma((4,)),
            dma((4,)),
            dma((units,)),
            dma((units,)),
            dma((units, 2, nz - 1)),
            dma((units, 2, nz - 1)),
            dma((units,)),
            dma((units,)),
            dma,
            dma((16,)),
        ],
        compiler_params=pltpu.CompilerParams(collective_id=2, has_side_effects=True),
    )(omega.reshape(nz, 2, part, k), basis, vecs)


def body(omega, basis, vectors):
    ns, nr = lax.axis_size("section"), lax.axis_size("row")
    s = lax.axis_index("section")
    vecs = jnp.pad(vectors.T, ((0, 0), (0, basis.shape[1] - vectors.shape[0])))
    sketch, probe = sketch_call(omega, basis, vecs, nr)
    gram, nxt = gram_call(sketch, ns, nr)
    inv = inverse(gram)
    width = vectors.shape[1] // ns
    mine = lax.dynamic_slice_in_dim(vectors, s * width, width, 1)
    return chain_call(sketch, nxt, inv, probe.reshape(-1, 128), basis, mine, ns, nr)


def solution(mesh):
    placed = (P("section", "row"), P("row", "section"), P(None, "row"))
    return jax.shard_map(
        body,
        mesh=mesh,
        in_specs=placed,
        out_specs=(P(None, ("row", "section")), P(None, "section")),
        check_vma=False,
    )
```

```python
import functools

import jax
import jax.numpy as jnp
from jax import lax
from jax.experimental import pallas as pl
from jax.experimental.pallas import tpu as pltpu
from jax.sharding import PartitionSpec as P

F32 = jnp.float32
BF16 = jnp.bfloat16
HI = lax.Precision.HIGHEST
MESH = pl.DeviceIdType.MESH


def split(x):
    hi = x.astype(BF16)
    return hi, (x - hi.astype(F32)).astype(BF16)


def dot3(a, b, dims):
    (ah, al), (bh, bl) = a, b

    def one(x, y):
        return lax.dot_general(x, y, (dims, ((), ())), preferred_element_type=F32)

    return one(ah, bh) + (one(al, bh) + one(ah, bl))


NN = ((1,), (0,))
NT = ((1,), (1,))
TN = ((0,), (0,))


def remote(src, dst, send, recv, section, row):
    return pltpu.make_async_remote_copy(
        src_ref=src,
        dst_ref=dst,
        send_sem=send,
        recv_sem=recv,
        device_id=(section, row),
        device_id_type=MESH,
    )


def gram_kernel(
    ns, nr, s_ref, gram_ref, next_ref, part, got, red, rs_send, rs_recv, ag_send, ag_recv, n_send, n_recv
):
    s, r = lax.axis_index("section"), lax.axis_index("row")
    rows = part.shape[0] // nr
    barrier = pltpu.get_barrier_semaphore()
    after, before = lax.rem(s + 1, ns), lax.rem(s + ns - 1, ns)
    for step in range(1, nr):
        pl.semaphore_signal(barrier, inc=1, device_id=(s, lax.rem(r + step, nr)), device_id_type=MESH)
    pl.semaphore_signal(barrier, inc=1, device_id=(after, r), device_id_type=MESH)
    pl.semaphore_signal(barrier, inc=1, device_id=(before, r), device_id_type=MESH)
    sp = split(s_ref[...])
    part[...] = dot3(sp, sp, TN)
    pl.semaphore_wait(barrier, nr + 1)
    shift = remote(s_ref, next_ref, n_send, n_recv, before, r)
    shift.start()
    scatter = []
    for step in range(1, nr):
        peer = lax.rem(r + step, nr)
        cp = remote(
            part.at[pl.ds(pl.multiple_of(peer * rows, rows), rows)],
            got.at[step],
            rs_send.at[step],
            rs_recv.at[step],
            s,
            peer,
        )
        cp.start()
        scatter.append(cp)
    for cp in scatter:
        cp.wait_recv()
    total = part[pl.ds(pl.multiple_of(r * rows, rows), rows), :]
    for step in range(1, nr):
        total = total + got[step]
    red[...] = total
    mine = pl.ds(pl.multiple_of(r * rows, rows), rows)
    gather = []
    for step in range(1, nr):
        peer = lax.rem(r + step, nr)
        cp = remote(red, gram_ref.at[mine], ag_send.at[step], ag_recv.at[step], s, peer)
        cp.start()
        gather.append(cp)
    gram_ref[mine, :] = total
    for step in range(1, nr):
        peer = lax.rem(r + nr - step, nr)
        theirs = pl.ds(pl.multiple_of(peer * rows, rows), rows)
        remote(red, gram_ref.at[theirs], ag_send.at[step], ag_recv.at[step], s, peer).wait_recv()
    for cp in scatter + gather:
        cp.wait_send()
    shift.wait()


def gram_call(sketch, ns, nr):
    n = sketch.shape[1]
    vm = pl.BlockSpec(memory_space=pltpu.VMEM)
    dma = pltpu.SemaphoreType.DMA
    return pl.pallas_call(
        functools.partial(gram_kernel, ns, nr),
        out_shape=(
            jax.ShapeDtypeStruct((n, n), F32),
            jax.ShapeDtypeStruct(sketch.shape, F32),
        ),
        in_specs=[vm],
        out_specs=(vm, vm),
        scratch_shapes=[
            pltpu.VMEM((n, n), F32),
            pltpu.VMEM((nr, n // nr, n), F32),
            pltpu.VMEM((n // nr, n), F32),
            dma((nr,)),
            dma((nr,)),
            dma((nr,)),
            dma((nr,)),
            dma,
            dma,
        ],
        compiler_params=pltpu.CompilerParams(collective_id=0, has_side_effects=True),
    )(sketch)


def packed(c):
    half = c.shape[1] // 2
    return jnp.concatenate([c[:4, :half], c[:4, half:]], axis=0)


def unpacked(c):
    wide = jnp.concatenate([c[:4], c[4:]], axis=1)
    return jnp.concatenate([wide, jnp.zeros_like(wide)], axis=0)


def chain_kernel(
    ns,
    nr,
    s_ref,
    next_ref,
    inv_ref,
    p0_ref,
    basis_ref,
    vec_ref,
    ortho_ref,
    coef_ref,
    hi_ref,
    lo_ref,
    probe,
    moved,
    cout,
    cin,
    own,
    oin,
    sout,
    sin,
    bout,
    bin_,
    c_send,
    c_recv,
    p_send,
    p_recv,
    o_send,
    o_recv,
    s_send,
    s_recv,
    b_send,
    b_recv,
):
    s, r = lax.axis_index("section"), lax.axis_index("row")
    barrier = pltpu.get_barrier_semaphore()
    after, before = lax.rem(s + 1, ns), lax.rem(s + ns - 1, ns)
    for q in range(nr):
        for other in (after, before):
            pl.semaphore_signal(barrier, inc=1, device_id=(other, q), device_id_type=MESH)
    for step in range(1, nr):
        pl.semaphore_signal(barrier, inc=1, device_id=(s, lax.rem(r + step, nr)), device_id_type=MESH)
    for step in range(1, ns):
        pl.semaphore_signal(barrier, inc=1, device_id=(lax.rem(s + step, ns), r), device_id_type=MESH)

    sp = split(s_ref[...])
    nx = split(next_ref[...])
    iv = split(inv_ref[...])
    hi_ref[...], lo_ref[...] = split(dot3(iv, split(dot3(sp, nx, TN)), NN))
    pl.semaphore_wait(barrier, 3 * nr + ns - 2)

    @pl.when(s == 0)
    def _():
        p = p0_ref[:, :128].T[:8]
        probe[...] = p
        cout[...] = packed(dot3(split(p), sp, NN))
        copies = []
        for step in range(1, nr):
            peer = lax.rem(r + step, nr)
            cp = remote(cout, cin.at[r], c_send.at[step], c_recv.at[r], 0, peer)
            cp.start()
            copies.append(cp)
        cin[pl.ds(r, 1)] = cout[...][None]
        for cp in copies:
            cp.wait_send()
        for step in range(1, nr):
            peer = lax.rem(r + step, nr)
            remote(cout, cin.at[peer], c_send.at[step], c_recv.at[peer], 0, peer).wait_recv()

    @pl.when(s > 0)
    def _():
        remote(moved, probe, p_send, p_recv, before, r).wait_recv()

    p = probe[...]
    ahead = dot3(split(p), nx, NN)

    @pl.when(s > 0)
    def _():
        for q in range(nr):
            remote(cout, cin.at[q], c_send.at[q], c_recv.at[q], before, q).wait_recv()

    total = cin[0]
    for q in range(1, nr):
        total = total + cin[q]
    inner = unpacked(total)
    cin_parts = split(inner)

    @pl.when(s < ns - 1)
    def _():
        cout[...] = packed(ahead - dot3(cin_parts, (hi_ref[...], lo_ref[...]), NN))
        for q in range(nr):
            remote(cout, cin.at[r], c_send.at[q], c_recv.at[r], after, q).start()

    coef = dot3(cin_parts, iv, NN)
    cs = split(coef)
    moved[...] = p - dot3(cs, sp, NT)

    @pl.when(s < ns - 1)
    def _():
        remote(moved, probe, p_send, p_recv, after, r).start()

    coef_ref[...] = coef[:4]
    term = lax.dot_general(coef.astype(BF16), basis_ref[...], (NT, ((), ())), preferred_element_type=F32)
    for k in range(ns // 2):
        own[k] = term[:, k * 128 : (k + 1) * 128]
    outs = []
    for step in range(1, ns):
        t = lax.rem(s + step, ns)
        cp = remote(own.at[lax.div(t, 2)], oin.at[s], o_send.at[step], o_recv.at[s], t, r)
        cp.start()
        outs.append(cp)
    oin[pl.ds(s, 1)] = own[pl.ds(lax.div(s, 2), 1)]

    @pl.when(s == ns - 1)
    def _():
        m = split(moved[...])
        sq = dot3(m, m, NT)
        sout[...] = jnp.concatenate([sq, jnp.zeros((8, 120), F32)], axis=1)
        copies = []
        for step in range(1, nr):
            peer = lax.rem(r + step, nr)
            cp = remote(sout, sin.at[r], s_send.at[step], s_recv.at[r], s, peer)
            cp.start()
            copies.append(cp)
        sin[pl.ds(r, 1)] = sout[...][None]
        for step in range(1, nr):
            peer = lax.rem(r + step, nr)
            remote(sout, sin.at[peer], s_send.at[step], s_recv.at[peer], s, peer).wait_recv()
        tot = sin[0]
        for q in range(1, nr):
            tot = tot + sin[q]
        bout[...] = tot
        bcs = []
        for t in range(ns - 1):
            cp = remote(bout, bin_, b_send.at[t], b_recv, t, r)
            cp.start()
            bcs.append(cp)
        for cp in copies + bcs:
            cp.wait_send()
        bin_[...] = tot

    for step in range(1, ns):
        t = lax.rem(s + step, ns)
        remote(own.at[0], oin.at[t], o_send.at[step], o_recv.at[t], t, r).wait_recv()
    removed = oin[0]
    for t in range(1, ns):
        removed = removed + oin[t]
    odd = lax.rem(s, 2) == 1
    removed = jnp.where(odd, removed[:4, 64:], removed[:4, :64])
    remain = vec_ref[...].astype(F32) - removed

    @pl.when(s < ns - 1)
    def _():
        remote(bout, bin_, b_send.at[0], b_recv, ns - 1, r).wait_recv()
        for q in range(nr):
            remote(cout, cin.at[q], c_send.at[q], c_recv.at[q], after, q).wait_send()
        remote(moved, probe, p_send, p_recv, after, r).wait_send()

    small = bin_[...]

    def at(i, k):
        return small[i : i + 1, k : k + 1]

    low = [[None] * 4 for _ in range(4)]
    rows = []
    for i in range(4):
        for k in range(i + 1):
            v = at(i, k)
            for m in range(k):
                v = v - low[i][m] * low[k][m]
            low[i][k] = jnp.sqrt(v) if i == k else v / low[k][k]
        x = remain[i : i + 1]
        for k in range(i):
            x = x - low[i][k] * rows[k]
        rows.append(x / low[i][i])
    ortho_ref[...] = jnp.concatenate(rows, axis=0)
    for cp in outs:
        cp.wait_send()


def chain_call(sketch, nxt, inv, probe, basis, mine, ns, nr):
    vm = pl.BlockSpec(memory_space=pltpu.VMEM)
    dma = pltpu.SemaphoreType.DMA
    k, n = sketch.shape
    return pl.pallas_call(
        functools.partial(chain_kernel, ns, nr),
        out_shape=(
            jax.ShapeDtypeStruct((4, mine.shape[1]), F32),
            jax.ShapeDtypeStruct((4, n), F32),
        ),
        in_specs=[vm] * 6,
        out_specs=(vm, vm),
        scratch_shapes=[
            pltpu.VMEM((n, n), BF16),
            pltpu.VMEM((n, n), BF16),
            pltpu.VMEM((8, k), F32),
            pltpu.VMEM((8, k), F32),
            pltpu.VMEM((8, 128), F32),
            pltpu.VMEM((nr, 8, 128), F32),
            pltpu.VMEM((ns // 2, 8, 128), F32),
            pltpu.VMEM((ns, 8, 128), F32),
            pltpu.VMEM((8, 128), F32),
            pltpu.VMEM((nr, 8, 128), F32),
            pltpu.VMEM((8, 128), F32),
            pltpu.VMEM((8, 128), F32),
            dma((nr,)),
            dma((nr,)),
            dma,
            dma,
            dma((ns,)),
            dma((ns,)),
            dma((nr,)),
            dma((nr,)),
            dma((ns,)),
            dma,
        ],
        compiler_params=pltpu.CompilerParams(collective_id=1, has_side_effects=True),
    )(sketch, nxt, inv, probe, basis, mine)


def eliminate(a):
    n = a.shape[0]
    rows = lax.broadcasted_iota(jnp.int32, (n, n), 0)
    cols = lax.broadcasted_iota(jnp.int32, (n, n), 1)
    lane = lax.broadcasted_iota(jnp.int32, (1, n), 1)
    for k in range(0, n, 2):
        c1 = jnp.broadcast_to(a[:, k : k + 1], (n, n))
        c2 = jnp.broadcast_to(a[:, k + 1 : k + 2], (n, n))
        p, q, s = c1[k : k + 1], c2[k : k + 1], c2[k + 1 : k + 2]
        e = 1.0 / (p * s - q * q)
        r1 = jnp.where(lane == k, 1.0, jnp.where(lane == k + 1, 0.0, a[k : k + 1, :]))
        r2 = jnp.where(lane == k + 1, 1.0, jnp.where(lane == k, 0.0, a[k + 1 : k + 2, :]))
        w1 = (s * e) * r1 - (q * e) * r2
        w2 = (p * e) * r2 - (q * e) * r1
        base = jnp.where((cols == k) | (cols == k + 1), 0.0, a)
        new = base - c1 * w1 - c2 * w2
        last = jnp.where(rows == k + 1, jnp.broadcast_to(w2, (n, n)), new)
        a = jnp.where(rows == k, jnp.broadcast_to(w1, (n, n)), last)
    return a


def inverse_kernel(g_ref, out_ref):
    g = g_ref[...]
    n = g.shape[0]
    h = n // 2
    eye = lax.broadcasted_iota(jnp.int32, (n, n), 0) == lax.broadcasted_iota(jnp.int32, (n, n), 1)
    d = jnp.where(eye, g, 0.0)
    rs = lax.rsqrt(jnp.sum(d, axis=1, keepdims=True))
    cs = lax.rsqrt(jnp.sum(d, axis=0, keepdims=True))
    g = g * rs * cs

    def dot(x, y, dims):
        return lax.dot_general(x, y, (dims, ((), ())), precision=HI, preferred_element_type=F32)

    a, b, c = g[:h, :h], g[:h, h:], g[h:, h:]
    ai = eliminate(a)
    t = dot(ai, b, NN)
    ci = eliminate(c - dot(b, t, TN))
    u = dot(t, ci, NN)
    top = jnp.concatenate([ai + dot(u, t, NT), -u], axis=1)
    low = jnp.concatenate([-u.T, ci], axis=1)
    out_ref[...] = jnp.concatenate([top, low], axis=0) * rs * cs


def inverse(gram):
    vm = pl.BlockSpec(memory_space=pltpu.VMEM)
    return pl.pallas_call(
        inverse_kernel,
        out_shape=jax.ShapeDtypeStruct(gram.shape, F32),
        in_specs=[vm],
        out_specs=vm,
    )(gram)


def within(t, first, yes, no):
    return jnp.where(t >= first, yes, no)


def unit(t):
    def seg(first, width):
        return lax.div(jnp.maximum(t - first, 0), width), lax.rem(jnp.maximum(t - first, 0), width)

    a, b = seg(4, 2)
    row, half, col = within(t, 2, 0, 0), lax.rem(t, 2), within(t, 2, 0, 4)
    row, half, col = row, within(t, 4, b, half), within(t, 4, 1 + a, col)
    a, b = seg(8, 3)
    row, half, col = within(t, 8, 1 + a, row), within(t, 8, a, half), within(t, 8, b, col)
    row, half, col = within(t, 14, 0, row), within(t, 14, t - 14, half), within(t, 14, 3, col)
    row, half, col = within(t, 16, t - 15, row), within(t, 16, t - 16, half), within(t, 16, 3, col)
    a, b = seg(18, 4)
    row, half, col = within(t, 18, 1 + a, row), within(t, 18, 1 - a, half), within(t, 18, b, col)
    a, b = seg(26, 4)
    row, half, col = within(t, 26, 3, row), within(t, 26, a, half), within(t, 26, b, col)
    return row, half, col


def slot_offset(d):
    return jnp.where(d == 0, 0, jnp.where(d == 1, 3, d - 1))


UNITS = 34
REACH = 4
LAG = 3


def sketch_kernel(
    nz,
    omega_ref,
    basis_ref,
    vec_ref,
    s_ref,
    p_ref,
    obuf,
    bbuf,
    part,
    dbuf,
    rbuf,
    fbuf,
    l_sem,
    o_send,
    o_recv,
    b_send,
    b_recv,
    d_send,
    d_recv,
    r_send,
    r_recv,
    f_send,
    f_recv,
    p_send,
    p_recv,
):
    s, r = lax.axis_index("section"), lax.axis_index("row")
    y, x = lax.div(s, 4), lax.rem(s, 4)
    z, c = lax.div(r, 2), lax.rem(r, 2)

    def at(dy, dx):
        return lax.rem(y + dy, 4) * 4 + lax.rem(x + dx, 4)

    beside = (lax.rem(z + 1, nz) * 2 + c, lax.rem(z + nz - 1, nz) * 2 + c)
    mate = z * 2 + (1 - c)

    local = [
        pltpu.make_async_copy(omega_ref, obuf.at[0], l_sem.at[0]),
        pltpu.make_async_copy(basis_ref, bbuf.at[0], l_sem.at[1]),
        pltpu.make_async_copy(vec_ref, bbuf.at[4], l_sem.at[2]),
    ]
    for cp in local:
        cp.start()

    barrier = pltpu.get_barrier_semaphore()

    def hello(section, row):
        pl.semaphore_signal(barrier, inc=1, device_id=(section, row), device_id_type=MESH)

    for dy, dx in ((1, 0), (3, 0), (0, 1), (0, 2), (0, 3)):
        hello(at(dy, dx), r)
    for row in (*beside, mate):
        hello(s, row)

    @pl.when(s == 0)
    def _():
        for t in range(1, 16):
            hello(t, r)

    for cp in local:
        cp.wait()
    pl.semaphore_wait(barrier, 8 + jnp.minimum(s, 1))

    def ocopy(src, dst, half, sem, dy):
        return remote(obuf.at[src, half], obuf.at[dst, half], o_send.at[sem], o_recv.at[sem], at(dy, 0), r)

    def bcopy(src, dst, half, sem, dx):
        a, b = bbuf.at[src], bbuf.at[dst]
        if half is not None:
            a, b = a.at[pl.ds(512 * half, 512)], b.at[pl.ds(512 * half, 512)]
        return remote(a, b, b_send.at[sem], b_recv.at[sem], at(0, dx), r)

    b_own = [bcopy(0, 1, None, 0, 1), bcopy(0, 2, None, 1, 3)]
    o_own = [ocopy(0, 1, 0, 0, 1), ocopy(0, 2, 1, 1, 3)]
    o_rest = [ocopy(0, 1, 1, 2, 1), ocopy(0, 2, 0, 3, 3)]
    b_fwd = [bcopy(1, 3, 0, 2, 1), bcopy(2, 3, 1, 3, 3)]
    o_fwd = [ocopy(1, 3, 0, 4, 1), ocopy(2, 3, 1, 5, 3)]
    for cp in o_own + b_own + o_rest:
        cp.start()

    def dcopy(u):
        return remote(part.at[u, :, 1 - c], dbuf.at[u], d_send.at[u], d_recv.at[u], s, mate)

    def chunk(d, k):
        far = REACH - k
        return lax.rem(z + (far if d == 0 else nz - far), nz)

    def rcopy(u, d, k):
        return remote(
            part.at[u, chunk(d, k), c],
            rbuf.at[u, d, k],
            r_send.at[u, d, k],
            r_recv.at[u, d, k],
            s,
            beside[d],
        )

    def place(u):
        row, half, col = unit(u)
        dy, dx = slot_offset(row), slot_offset(col)
        start = (lax.rem(y + dy, 4) * 4 + x) * 32 + half * 16
        return dx, pl.ds(pl.multiple_of(start, 16), 16)

    def fcopy(u):
        dx, rows = place(u)
        return remote(fbuf.at[u], s_ref.at[rows], f_send.at[u], f_recv.at[u], at(0, dx), r)

    def pcopy(u, sender):
        return remote(fbuf.at[u], p_ref.at[sender, u], p_send.at[u], p_recv.at[sender, u], 0, r)

    def step(t, carry):
        done = t - 2 - LAG * REACH

        @pl.when((done >= 0) & (done < UNITS))
        def _():
            rcopy(done, 0, REACH - 1).wait_recv()
            rcopy(done, 1, REACH - 1).wait_recv()
            fbuf[done] = (part[done, z, c] + dbuf[done, z]) + (
                rbuf[done, 0, REACH - 1] + rbuf[done, 1, REACH - 1]
            )

        @pl.when((done >= 2) & (done < UNITS))
        def _():
            dx, rows = place(done)

            @pl.when(dx == 0)
            def _():
                s_ref[rows, :] = fbuf[done]

            @pl.when(dx > 0)
            def _():
                fcopy(done).start()

        @pl.when((done >= 0) & (done < 2))
        def _():
            @pl.when(s == 0)
            def _():
                p_ref[0, done] = fbuf[done]

            @pl.when(s > 0)
            def _():
                pcopy(done, s).start()

        for k in range(REACH - 1, -1, -1):
            u = t - 2 - LAG * k
            valid = (u >= 0) & (u < UNITS)
            if k == 0:

                @pl.when(valid)
                def _():
                    dcopy(u).wait_recv()

            for d in range(2):
                longer = lax.rem(jnp.maximum(u, 0), 2) == d

                def own():
                    return part[u, chunk(d, k), c] + dbuf[u, chunk(d, k)]

                def send(val):
                    part[u, chunk(d, k), c] = val
                    rcopy(u, d, k).start()

                def pass_on():
                    rcopy(u, d, k - 1).wait_recv()
                    send(own() + rbuf[u, d, k - 1])

                if k == 0:

                    @pl.when(valid & longer)
                    def _():
                        send(own())

                elif k == 1:

                    @pl.when(valid & longer)
                    def _():
                        pass_on()

                    @pl.when(valid & jnp.logical_not(longer))
                    def _():
                        send(own())

                else:

                    @pl.when(valid)
                    def _():
                        pass_on()

        @pl.when(t == 4)
        def _():
            for cp in b_own:
                cp.wait_recv()
            for cp in b_fwd:
                cp.start()

        @pl.when(t == 8)
        def _():
            for cp in o_own:
                cp.wait_recv()
            for cp in o_fwd:
                cp.start()

        @pl.when(t == 14)
        def _():
            for cp in b_fwd:
                cp.wait_recv()

        @pl.when(t == 18)
        def _():
            for cp in o_rest:
                cp.wait_recv()

        @pl.when(t == 26)
        def _():
            for cp in o_fwd:
                cp.wait_recv()

        @pl.when(t < UNITS)
        def _():
            row, half, col = unit(t)
            out = jnp.dot(obuf[row, half], bbuf[col], preferred_element_type=F32)
            part[t] = out.reshape(part.shape[1:])
            dcopy(t).start()

        return carry

    lax.fori_loop(0, UNITS + 2 + LAG * REACH + 1, step, 0)

    def finish(u, carry):
        dx, _ = place(u)

        @pl.when(dx > 0)
        def _():
            fcopy(u).wait()

        return carry

    lax.fori_loop(2, UNITS, finish, 0)

    @pl.when(s == 0)
    def _():
        for t in range(1, 16):
            for u in range(2):
                pcopy(u, t).wait_recv()

    @pl.when(s > 0)
    def _():
        for u in range(2):
            pcopy(u, s).wait_send()

    for cp in b_own + o_own + o_rest + b_fwd + o_fwd:
        cp.wait_send()

    def drain(u, carry):
        dcopy(u).wait_send()
        for d in range(2):
            for k in range(REACH):
                if k:
                    rcopy(u, d, k).wait_send()
                else:

                    @pl.when(lax.rem(u, 2) == d)
                    def _():
                        rcopy(u, d, k).wait_send()

        return carry

    lax.fori_loop(0, UNITS, drain, 0)


def sketch_call(omega, basis, vecs, nr):
    vm = pl.BlockSpec(memory_space=pltpu.VMEM)
    anym = pl.BlockSpec(memory_space=pl.ANY)
    dma = pltpu.SemaphoreType.DMA
    nz = nr // 2
    m, k = omega.shape
    n = basis.shape[1]
    piece = m // nr // 2
    return pl.pallas_call(
        functools.partial(sketch_kernel, nz),
        out_shape=(
            jax.ShapeDtypeStruct((m, n), F32),
            jax.ShapeDtypeStruct((16, 2, piece, n), F32),
        ),
        in_specs=[anym] * 3,
        out_specs=(vm, vm),
        scratch_shapes=[
            pltpu.VMEM((4, 2, m // 2, k), BF16),
            pltpu.VMEM((5, k, n), BF16),
            pltpu.VMEM((UNITS, nz, 2, piece, n), F32),
            pltpu.VMEM((UNITS, nz, piece, n), F32),
            pltpu.VMEM((UNITS, 2, REACH, piece, n), F32),
            pltpu.VMEM((UNITS, piece, n), F32),
            dma((3,)),
            dma((6,)),
            dma((6,)),
            dma((4,)),
            dma((4,)),
            dma((UNITS,)),
            dma((UNITS,)),
            dma((UNITS, 2, REACH)),
            dma((UNITS, 2, REACH)),
            dma((UNITS,)),
            dma((UNITS,)),
            dma((2,)),
            dma((16, 2)),
        ],
        compiler_params=pltpu.CompilerParams(collective_id=2, has_side_effects=True),
    )(omega.reshape(2, m // 2, k), basis, vecs)


def body(omega, basis, vectors):
    ns, nr = lax.axis_size("section"), lax.axis_size("row")
    s = lax.axis_index("section")
    vecs = jnp.pad(vectors.T, ((0, 0), (0, basis.shape[1] - vectors.shape[0])))
    sketch, probe = sketch_call(omega, basis, vecs, nr)
    gram, nxt = gram_call(sketch, ns, nr)
    inv = inverse(gram)
    width = vectors.shape[1] // ns
    mine = lax.dynamic_slice_in_dim(vectors, s * width, width, 1)
    return chain_call(sketch, nxt, inv, probe.reshape(-1, probe.shape[-1]), basis, mine, ns, nr)


def solution(mesh):
    placed = (P("section", "row"), P("row", "section"), P(None, "row"))
    return jax.shard_map(
        body,
        mesh=mesh,
        in_specs=placed,
        out_specs=(P(None, ("row", "section")), P(None, "section")),
        check_vma=False,
    )
```

```python
import functools

import jax
import jax.numpy as jnp
from jax import lax
from jax.experimental import pallas as pl
from jax.experimental.pallas import tpu as pltpu
from jax.sharding import PartitionSpec as P

F32 = jnp.float32
BF16 = jnp.bfloat16
HI = lax.Precision.HIGHEST
MESH = pl.DeviceIdType.MESH


def split(x):
    hi = x.astype(BF16)
    return hi, (x - hi.astype(F32)).astype(BF16)


def dot3(a, b, dims):
    (ah, al), (bh, bl) = a, b

    def one(x, y):
        return lax.dot_general(x, y, (dims, ((), ())), preferred_element_type=F32)

    return one(ah, bh) + (one(al, bh) + one(ah, bl))


NN = ((1,), (0,))
NT = ((1,), (1,))
TN = ((0,), (0,))


def remote(src, dst, send, recv, section, row):
    return pltpu.make_async_remote_copy(
        src_ref=src,
        dst_ref=dst,
        send_sem=send,
        recv_sem=recv,
        device_id=(section, row),
        device_id_type=MESH,
    )


def packed(c):
    half = c.shape[1] // 2
    return jnp.concatenate([c[:4, :half], c[:4, half:]], axis=0)


def unpacked(c):
    wide = jnp.concatenate([c[:4], c[4:]], axis=1)
    return jnp.concatenate([wide, jnp.zeros_like(wide)], axis=0)


def chain_kernel(
    ns,
    nr,
    s_ref,
    next_ref,
    inv_ref,
    p0_ref,
    basis_ref,
    vec_ref,
    ortho_ref,
    coef_ref,
    hi_ref,
    lo_ref,
    kept,
    low_part,
    probe,
    moved,
    cout,
    cin,
    own,
    oin,
    sout,
    sin,
    bout,
    bin_,
    c_send,
    c_recv,
    p_send,
    p_recv,
    o_send,
    o_recv,
    s_send,
    s_recv,
    b_send,
    b_recv,
    k_send,
    k_recv,
):
    s, r = lax.axis_index("section"), lax.axis_index("row")
    n = kept.shape[1]
    odd = lax.rem(s, 2) == 1
    barrier = pltpu.get_barrier_semaphore()
    after, before = lax.rem(s + 2, ns), lax.rem(s + ns - 2, ns)
    for q in range(nr):
        for other in (after, before):
            pl.semaphore_signal(barrier, inc=1, device_id=(other, q), device_id_type=MESH)
    for step in range(1, nr):
        pl.semaphore_signal(barrier, inc=1, device_id=(s, lax.rem(r + step, nr)), device_id_type=MESH)
    for step in range(1, ns):
        pl.semaphore_signal(barrier, inc=1, device_id=(lax.rem(s + step, ns), r), device_id_type=MESH)

    pl.semaphore_wait(barrier, 3 * nr + ns - 2)
    pass_coef = remote(low_part, kept, k_send, k_recv, lax.rem(s + ns - 1, ns), r)
    take_coef = remote(low_part, kept, k_send, k_recv, lax.rem(s + 1, ns), r)

    @pl.when(odd)
    def _():
        sp = split(s_ref[...])
        nx = split(next_ref[...])
        iv = split(inv_ref[...])

        @pl.when(s == 1)
        def _():
            p = p0_ref[:, :128].T[:8]
            probe[...] = p
            cout[...] = packed(dot3(split(p), sp, NN))
            copies = []
            for step in range(1, nr):
                peer = lax.rem(r + step, nr)
                cp = remote(cout, cin.at[r], c_send.at[step], c_recv.at[r], 1, peer)
                cp.start()
                copies.append(cp)
            cin[pl.ds(r, 1)] = cout[...][None]
            for cp in copies:
                cp.wait_send()

        hi_ref[...], lo_ref[...] = split(dot3(iv, split(dot3(sp, nx, TN)), NN))

        @pl.when(s == 1)
        def _():
            for step in range(1, nr):
                peer = lax.rem(r + step, nr)
                remote(cout, cin.at[peer], c_send.at[step], c_recv.at[peer], 1, peer).wait_recv()

        @pl.when(s > 1)
        def _():
            remote(moved, probe, p_send, p_recv, before, r).wait_recv()

        p = probe[...]
        ahead = dot3(split(p), nx, NN)

        @pl.when(s > 1)
        def _():
            for q in range(nr):
                remote(cout, cin.at[q], c_send.at[q], c_recv.at[q], before, q).wait_recv()

        total = cin[0]
        for q in range(1, nr):
            total = total + cin[q]
        inner = split(unpacked(total))

        @pl.when(s < ns - 1)
        def _():
            cout[...] = packed(ahead - dot3(inner, (hi_ref[...], lo_ref[...]), NN))
            for q in range(nr):
                remote(cout, cin.at[r], c_send.at[q], c_recv.at[r], after, q).start()

        coef = dot3(inner, iv, NN)
        low_part[...] = coef[:, :n]
        kept[...] = coef[:, n:]
        moved[...] = p - dot3(split(coef), sp, NT)

        @pl.when(s < ns - 1)
        def _():
            remote(moved, probe, p_send, p_recv, after, r).start()

        pass_coef.start()

    @pl.when(lax.rem(s, 2) == 0)
    def _():
        take_coef.wait_recv()

    coef = kept[...]
    coef_ref[...] = coef[:4]
    term = lax.dot_general(coef.astype(BF16), basis_ref[...], (NT, ((), ())), preferred_element_type=F32)
    for k in range(ns // 2):
        own[k] = term[:, k * 128 : (k + 1) * 128]
    outs = []
    for step in range(1, ns):
        t = lax.rem(s + step, ns)
        cp = remote(own.at[lax.div(t, 2)], oin.at[s], o_send.at[step], o_recv.at[s], t, r)
        cp.start()
        outs.append(cp)
    oin[pl.ds(s, 1)] = own[pl.ds(lax.div(s, 2), 1)]

    @pl.when(s == ns - 1)
    def _():
        m = split(moved[...])
        sq = dot3(m, m, NT)
        sout[...] = jnp.concatenate([sq, jnp.zeros((8, 120), F32)], axis=1)
        copies = []
        for step in range(1, nr):
            peer = lax.rem(r + step, nr)
            cp = remote(sout, sin.at[r], s_send.at[step], s_recv.at[r], s, peer)
            cp.start()
            copies.append(cp)
        sin[pl.ds(r, 1)] = sout[...][None]
        for step in range(1, nr):
            peer = lax.rem(r + step, nr)
            remote(sout, sin.at[peer], s_send.at[step], s_recv.at[peer], s, peer).wait_recv()
        tot = sin[0]
        for q in range(1, nr):
            tot = tot + sin[q]
        bout[...] = tot
        bcs = []
        for t in range(ns - 1):
            cp = remote(bout, bin_, b_send.at[t], b_recv, t, r)
            cp.start()
            bcs.append(cp)
        for cp in copies + bcs:
            cp.wait_send()
        bin_[...] = tot

    for step in range(1, ns):
        t = lax.rem(s + step, ns)
        remote(own.at[0], oin.at[t], o_send.at[step], o_recv.at[t], t, r).wait_recv()
    removed = oin[0]
    for t in range(1, ns):
        removed = removed + oin[t]
    odd = lax.rem(s, 2) == 1
    removed = jnp.where(odd, removed[:4, 64:], removed[:4, :64])
    remain = vec_ref[...].astype(F32) - removed

    @pl.when(s < ns - 1)
    def _():
        remote(bout, bin_, b_send.at[0], b_recv, ns - 1, r).wait_recv()

    @pl.when(odd & (s < ns - 1))
    def _():
        for q in range(nr):
            remote(cout, cin.at[q], c_send.at[q], c_recv.at[q], after, q).wait_send()
        remote(moved, probe, p_send, p_recv, after, r).wait_send()

    @pl.when(odd)
    def _():
        pass_coef.wait_send()

    small = bin_[...]

    def at(i, k):
        return small[i : i + 1, k : k + 1]

    low = [[None] * 4 for _ in range(4)]
    rows = []
    for i in range(4):
        for k in range(i + 1):
            v = at(i, k)
            for m in range(k):
                v = v - low[i][m] * low[k][m]
            low[i][k] = jnp.sqrt(v) if i == k else v / low[k][k]
        x = remain[i : i + 1]
        for k in range(i):
            x = x - low[i][k] * rows[k]
        rows.append(x / low[i][i])
    ortho_ref[...] = jnp.concatenate(rows, axis=0)
    for cp in outs:
        cp.wait_send()


def chain_call(sketch, nxt, inv, probe, basis, mine, ns, nr):
    vm = pl.BlockSpec(memory_space=pltpu.VMEM)
    dma = pltpu.SemaphoreType.DMA
    k, n = sketch.shape
    return pl.pallas_call(
        functools.partial(chain_kernel, ns, nr),
        out_shape=(
            jax.ShapeDtypeStruct((4, mine.shape[1]), F32),
            jax.ShapeDtypeStruct((4, n // 2), F32),
        ),
        in_specs=[vm] * 6,
        out_specs=(vm, vm),
        scratch_shapes=[
            pltpu.VMEM((n, n), BF16),
            pltpu.VMEM((n, n), BF16),
            pltpu.VMEM((8, n // 2), F32),
            pltpu.VMEM((8, n // 2), F32),
            pltpu.VMEM((8, k), F32),
            pltpu.VMEM((8, k), F32),
            pltpu.VMEM((8, n // 2), F32),
            pltpu.VMEM((nr, 8, n // 2), F32),
            pltpu.VMEM((ns // 2, 8, 128), F32),
            pltpu.VMEM((ns, 8, 128), F32),
            pltpu.VMEM((8, 128), F32),
            pltpu.VMEM((nr, 8, 128), F32),
            pltpu.VMEM((8, 128), F32),
            pltpu.VMEM((8, 128), F32),
            dma((nr,)),
            dma((nr,)),
            dma,
            dma,
            dma((ns,)),
            dma((ns,)),
            dma((nr,)),
            dma((nr,)),
            dma((ns,)),
            dma,
            dma,
            dma,
        ],
        compiler_params=pltpu.CompilerParams(collective_id=1, has_side_effects=True),
    )(sketch, nxt, inv, probe, basis, mine)


def eliminate(a):
    n = a.shape[0]
    rows = lax.broadcasted_iota(jnp.int32, (n, n), 0)
    cols = lax.broadcasted_iota(jnp.int32, (n, n), 1)
    lane = lax.broadcasted_iota(jnp.int32, (1, n), 1)
    for k in range(0, n, 2):
        c1 = jnp.broadcast_to(a[:, k : k + 1], (n, n))
        c2 = jnp.broadcast_to(a[:, k + 1 : k + 2], (n, n))
        p, q, s = c1[k : k + 1], c2[k : k + 1], c2[k + 1 : k + 2]
        e = 1.0 / (p * s - q * q)
        r1 = jnp.where(lane == k, 1.0, jnp.where(lane == k + 1, 0.0, a[k : k + 1, :]))
        r2 = jnp.where(lane == k + 1, 1.0, jnp.where(lane == k, 0.0, a[k + 1 : k + 2, :]))
        w1 = (s * e) * r1 - (q * e) * r2
        w2 = (p * e) * r2 - (q * e) * r1
        base = jnp.where((cols == k) | (cols == k + 1), 0.0, a)
        new = base - c1 * w1 - c2 * w2
        last = jnp.where(rows == k + 1, jnp.broadcast_to(w2, (n, n)), new)
        a = jnp.where(rows == k, jnp.broadcast_to(w1, (n, n)), last)
    return a


def pair_kernel(
    ns,
    nr,
    s_ref,
    pair_ref,
    ahead_ref,
    uinv_ref,
    part,
    got,
    red,
    full,
    inv,
    mate_inv,
    n_send,
    n_recv,
    rs_send,
    rs_recv,
    ag_send,
    ag_recv,
    i_send,
    i_recv,
):
    s, r = lax.axis_index("section"), lax.axis_index("row")
    n = s_ref.shape[1]
    rows = n // nr
    odd = lax.rem(s, 2) == 1
    even = lax.rem(s, 2) == 0
    barrier = pltpu.get_barrier_semaphore()
    for step in range(1, nr):
        pl.semaphore_signal(barrier, inc=1, device_id=(s, lax.rem(r + step, nr)), device_id_type=MESH)
    for step in (1, 2, ns - 2, ns - 1):
        pl.semaphore_signal(barrier, inc=1, device_id=(lax.rem(s + step, ns), r), device_id_type=MESH)

    low, high = pl.ds(0, n), pl.ds(n, n)
    to_mate = remote(s_ref, pair_ref.at[:, low], n_send.at[0], n_recv.at[0], lax.rem(s + 1, ns), r)
    to_last = remote(s_ref, ahead_ref.at[:, low], n_send.at[1], n_recv.at[1], lax.rem(s + ns - 1, ns), r)
    to_odd = remote(s_ref, ahead_ref.at[:, high], n_send.at[2], n_recv.at[2], lax.rem(s + ns - 2, ns), r)

    def span(peer):
        return pl.ds(pl.multiple_of(peer * rows, rows), rows)

    def scatter(i, step):
        peer = lax.rem(r + step, nr)
        return remote(
            part.at[i, span(peer)], got.at[i, step], rs_send.at[i, step], rs_recv.at[i, step], s, peer
        )

    def gather(i, step, sending):
        peer = lax.rem(r + (step if sending else nr - step), nr)
        where = span(r if sending else peer)
        return remote(red.at[i], full.at[i, where], ag_send.at[i, step], ag_recv.at[i, step], s, peer)

    def begin(i):
        for step in range(1, nr):
            scatter(i, step).start()

    def middle(i):
        for step in range(1, nr):
            scatter(i, step).wait_recv()
        total = part[i, span(r), :]
        for step in range(1, nr):
            total = total + got[i, step]
        red[i] = total
        for step in range(1, nr):
            gather(i, step, True).start()
        full[i, span(r), :] = total

    def end(i):
        for step in range(1, nr):
            gather(i, step, False).wait_recv()
        for step in range(1, nr):
            scatter(i, step).wait_send()
            gather(i, step, True).wait_send()

    sp = split(s_ref[...])
    part[0] = dot3(sp, sp, TN)
    pl.semaphore_wait(barrier, nr + 3)
    begin(0)

    @pl.when(even)
    def _():
        to_mate.start()

        @pl.when(s > 0)
        def _():
            to_last.start()

    @pl.when(odd & (s > 1))
    def _():
        to_odd.start()

    pair_ref[:, n:] = s_ref[...]
    middle(0)

    @pl.when(odd)
    def _():
        to_mate.wait_recv()
        part[1] = dot3(split(pair_ref[:, :n]), sp, TN)
        begin(1)

    end(0)

    def dot(x, y, dims):
        return lax.dot_general(x, y, (dims, ((), ())), precision=HI, preferred_element_type=F32)

    g = full[0]
    h = n // 2
    eye = lax.broadcasted_iota(jnp.int32, (n, n), 0) == lax.broadcasted_iota(jnp.int32, (n, n), 1)
    d = jnp.where(eye, g, 0.0)
    rs = lax.rsqrt(jnp.sum(d, axis=1, keepdims=True))
    cs = lax.rsqrt(jnp.sum(d, axis=0, keepdims=True))
    g = g * rs * cs
    a, b, c = g[:h, :h], g[:h, h:], g[h:, h:]
    ai = eliminate(a)
    t = dot(ai, b, NN)
    rest = c - dot(b, t, TN)

    @pl.when(odd)
    def _():
        middle(1)

    ci = eliminate(rest)
    u = dot(t, ci, NN)
    top = jnp.concatenate([ai + dot(u, t, NT), -u], axis=1)
    bottom = jnp.concatenate([-u.T, ci], axis=1)
    inv[...] = jnp.concatenate([top, bottom], axis=0) * rs * cs
    pass_inv = remote(inv, mate_inv, i_send, i_recv, lax.rem(s + 1, ns), r)

    @pl.when(even)
    def _():
        pass_inv.start()

    @pl.when(odd)
    def _():
        end(1)
        mine = inv[...]
        right = dot3(split(full[1]), split(mine), NN)
        uinv_ref[n:, n:] = mine
        uinv_ref[n:, :n] = jnp.zeros((n, n), F32)
        pass_inv.wait_recv()
        theirs = mate_inv[...]
        uinv_ref[:n, :n] = theirs
        uinv_ref[:n, n:] = -dot3(split(theirs), split(right), NN)

        @pl.when(s < ns - 1)
        def _():
            to_last.wait_recv()
            to_odd.wait_recv()

        @pl.when(s == ns - 1)
        def _():
            ahead_ref[...] = jnp.zeros(ahead_ref.shape, F32)

    @pl.when(even)
    def _():
        pass_inv.wait_send()
        to_mate.wait_send()

        @pl.when(s > 0)
        def _():
            to_last.wait_send()

    @pl.when(odd & (s > 1))
    def _():
        to_odd.wait_send()


def pair_call(sketch, ns, nr):
    k, n = sketch.shape
    vm = pl.BlockSpec(memory_space=pltpu.VMEM)
    dma = pltpu.SemaphoreType.DMA
    return pl.pallas_call(
        functools.partial(pair_kernel, ns, nr),
        out_shape=(
            jax.ShapeDtypeStruct((k, 2 * n), F32),
            jax.ShapeDtypeStruct((k, 2 * n), F32),
            jax.ShapeDtypeStruct((2 * n, 2 * n), F32),
        ),
        in_specs=[vm],
        out_specs=(vm, vm, vm),
        scratch_shapes=[
            pltpu.VMEM((2, n, n), F32),
            pltpu.VMEM((2, nr, n // nr, n), F32),
            pltpu.VMEM((2, n // nr, n), F32),
            pltpu.VMEM((2, n, n), F32),
            pltpu.VMEM((n, n), F32),
            pltpu.VMEM((n, n), F32),
            dma((3,)),
            dma((3,)),
            dma((2, nr)),
            dma((2, nr)),
            dma((2, nr)),
            dma((2, nr)),
            dma,
            dma,
        ],
        compiler_params=pltpu.CompilerParams(collective_id=0, has_side_effects=True),
    )(sketch)


def within(t, first, yes, no):
    return jnp.where(t >= first, yes, no)


def unit(t):
    def seg(first, width):
        return lax.div(jnp.maximum(t - first, 0), width), lax.rem(jnp.maximum(t - first, 0), width)

    a, b = seg(4, 2)
    row, half, col = within(t, 2, 0, 0), lax.rem(t, 2), within(t, 2, 0, 4)
    row, half, col = row, within(t, 4, b, half), within(t, 4, 1 + a, col)
    a, b = seg(8, 3)
    row, half, col = within(t, 8, 1 + a, row), within(t, 8, a, half), within(t, 8, b, col)
    row, half, col = within(t, 14, 0, row), within(t, 14, t - 14, half), within(t, 14, 3, col)
    row, half, col = within(t, 16, t - 15, row), within(t, 16, t - 16, half), within(t, 16, 3, col)
    a, b = seg(18, 4)
    row, half, col = within(t, 18, 1 + a, row), within(t, 18, 1 - a, half), within(t, 18, b, col)
    a, b = seg(26, 4)
    row, half, col = within(t, 26, 3, row), within(t, 26, a, half), within(t, 26, b, col)
    return row, half, col


def slot_offset(d):
    return jnp.where(d == 0, 0, jnp.where(d == 1, 3, d - 1))


UNITS = 34
HOME = 1
REACH = 4
LAG = 3


def sketch_kernel(
    nz,
    omega_ref,
    basis_ref,
    vec_ref,
    s_ref,
    p_ref,
    obuf,
    bbuf,
    part,
    dbuf,
    rbuf,
    fbuf,
    l_sem,
    o_send,
    o_recv,
    b_send,
    b_recv,
    d_send,
    d_recv,
    r_send,
    r_recv,
    f_send,
    f_recv,
    p_send,
    p_recv,
):
    s, r = lax.axis_index("section"), lax.axis_index("row")
    y, x = lax.div(s, 4), lax.rem(s, 4)
    z, c = lax.div(r, 2), lax.rem(r, 2)

    def at(dy, dx):
        return lax.rem(y + dy, 4) * 4 + lax.rem(x + dx, 4)

    beside = (lax.rem(z + 1, nz) * 2 + c, lax.rem(z + nz - 1, nz) * 2 + c)
    mate = z * 2 + (1 - c)

    local = [
        pltpu.make_async_copy(omega_ref, obuf.at[0], l_sem.at[0]),
        pltpu.make_async_copy(basis_ref, bbuf.at[0], l_sem.at[1]),
        pltpu.make_async_copy(vec_ref, bbuf.at[4], l_sem.at[2]),
    ]
    for cp in local:
        cp.start()

    barrier = pltpu.get_barrier_semaphore()

    def hello(section, row):
        pl.semaphore_signal(barrier, inc=1, device_id=(section, row), device_id_type=MESH)

    for dy, dx in ((1, 0), (3, 0), (0, 1), (0, 2), (0, 3)):
        hello(at(dy, dx), r)
    for row in (*beside, mate):
        hello(s, row)

    @pl.when(s == HOME)
    def _():
        for t in range(16):
            if t != HOME:
                hello(t, r)

    for cp in local:
        cp.wait()
    pl.semaphore_wait(barrier, 8 + jnp.where(s == HOME, 0, 1))

    def ocopy(src, dst, half, sem, dy):
        return remote(obuf.at[src, half], obuf.at[dst, half], o_send.at[sem], o_recv.at[sem], at(dy, 0), r)

    def bcopy(src, dst, half, sem, dx):
        a, b = bbuf.at[src], bbuf.at[dst]
        if half is not None:
            a, b = a.at[pl.ds(512 * half, 512)], b.at[pl.ds(512 * half, 512)]
        return remote(a, b, b_send.at[sem], b_recv.at[sem], at(0, dx), r)

    b_own = [bcopy(0, 1, None, 0, 1), bcopy(0, 2, None, 1, 3)]
    o_own = [ocopy(0, 1, 0, 0, 1), ocopy(0, 2, 1, 1, 3)]
    o_rest = [ocopy(0, 1, 1, 2, 1), ocopy(0, 2, 0, 3, 3)]
    b_fwd = [bcopy(1, 3, 0, 2, 1), bcopy(2, 3, 1, 3, 3)]
    o_fwd = [ocopy(1, 3, 0, 4, 1), ocopy(2, 3, 1, 5, 3)]
    for cp in o_own + b_own + o_rest:
        cp.start()

    def dcopy(u):
        return remote(part.at[u, :, 1 - c], dbuf.at[u], d_send.at[u], d_recv.at[u], s, mate)

    def chunk(d, k):
        far = REACH - k
        return lax.rem(z + (far if d == 0 else nz - far), nz)

    def rcopy(u, d, k):
        return remote(
            part.at[u, chunk(d, k), c],
            rbuf.at[u, d, k],
            r_send.at[u, d, k],
            r_recv.at[u, d, k],
            s,
            beside[d],
        )

    def place(u):
        row, half, col = unit(u)
        dy, dx = slot_offset(row), slot_offset(col)
        start = (lax.rem(y + dy, 4) * 4 + x) * 32 + half * 16
        return dx, pl.ds(pl.multiple_of(start, 16), 16)

    def fcopy(u):
        dx, rows = place(u)
        return remote(fbuf.at[u], s_ref.at[rows], f_send.at[u], f_recv.at[u], at(0, dx), r)

    def pcopy(u, sender):
        return remote(fbuf.at[u], p_ref.at[sender, u], p_send.at[u], p_recv.at[sender, u], HOME, r)

    def step(t, carry):
        done = t - 2 - LAG * REACH

        @pl.when((done >= 0) & (done < UNITS))
        def _():
            rcopy(done, 0, REACH - 1).wait_recv()
            rcopy(done, 1, REACH - 1).wait_recv()
            fbuf[done] = (part[done, z, c] + dbuf[done, z]) + (
                rbuf[done, 0, REACH - 1] + rbuf[done, 1, REACH - 1]
            )

        @pl.when((done >= 2) & (done < UNITS))
        def _():
            dx, rows = place(done)

            @pl.when(dx == 0)
            def _():
                s_ref[rows, :] = fbuf[done]

            @pl.when(dx > 0)
            def _():
                fcopy(done).start()

        @pl.when((done >= 0) & (done < 2))
        def _():
            @pl.when(s == HOME)
            def _():
                p_ref[HOME, done] = fbuf[done]

            @pl.when(s != HOME)
            def _():
                pcopy(done, s).start()

        for k in range(REACH - 1, -1, -1):
            u = t - 2 - LAG * k
            valid = (u >= 0) & (u < UNITS)
            if k == 0:

                @pl.when(valid)
                def _():
                    dcopy(u).wait_recv()

            for d in range(2):
                longer = lax.rem(jnp.maximum(u, 0), 2) == d

                def own():
                    return part[u, chunk(d, k), c] + dbuf[u, chunk(d, k)]

                def send(val):
                    part[u, chunk(d, k), c] = val
                    rcopy(u, d, k).start()

                def pass_on():
                    rcopy(u, d, k - 1).wait_recv()
                    send(own() + rbuf[u, d, k - 1])

                if k == 0:

                    @pl.when(valid & longer)
                    def _():
                        send(own())

                elif k == 1:

                    @pl.when(valid & longer)
                    def _():
                        pass_on()

                    @pl.when(valid & jnp.logical_not(longer))
                    def _():
                        send(own())

                else:

                    @pl.when(valid)
                    def _():
                        pass_on()

        @pl.when(t == 4)
        def _():
            for cp in b_own:
                cp.wait_recv()
            for cp in b_fwd:
                cp.start()

        @pl.when(t == 8)
        def _():
            for cp in o_own:
                cp.wait_recv()
            for cp in o_fwd:
                cp.start()

        @pl.when(t == 14)
        def _():
            for cp in b_fwd:
                cp.wait_recv()

        @pl.when(t == 18)
        def _():
            for cp in o_rest:
                cp.wait_recv()

        @pl.when(t == 26)
        def _():
            for cp in o_fwd:
                cp.wait_recv()

        @pl.when(t < UNITS)
        def _():
            row, half, col = unit(t)
            out = jnp.dot(obuf[row, half], bbuf[col], preferred_element_type=F32)
            part[t] = out.reshape(part.shape[1:])
            dcopy(t).start()

        return carry

    lax.fori_loop(0, UNITS + 2 + LAG * REACH + 1, step, 0)

    def finish(u, carry):
        dx, _ = place(u)

        @pl.when(dx > 0)
        def _():
            fcopy(u).wait()

        return carry

    lax.fori_loop(2, UNITS, finish, 0)

    @pl.when(s == HOME)
    def _():
        for t in range(16):
            if t != HOME:
                for u in range(2):
                    pcopy(u, t).wait_recv()

    @pl.when(s != HOME)
    def _():
        for u in range(2):
            pcopy(u, s).wait_send()

    for cp in b_own + o_own + o_rest + b_fwd + o_fwd:
        cp.wait_send()

    def drain(u, carry):
        dcopy(u).wait_send()
        for d in range(2):
            for k in range(REACH):
                if k:
                    rcopy(u, d, k).wait_send()
                else:

                    @pl.when(lax.rem(u, 2) == d)
                    def _():
                        rcopy(u, d, k).wait_send()

        return carry

    lax.fori_loop(0, UNITS, drain, 0)


def sketch_call(omega, basis, vecs, nr):
    vm = pl.BlockSpec(memory_space=pltpu.VMEM)
    anym = pl.BlockSpec(memory_space=pl.ANY)
    dma = pltpu.SemaphoreType.DMA
    nz = nr // 2
    m, k = omega.shape
    n = basis.shape[1]
    piece = m // nr // 2
    return pl.pallas_call(
        functools.partial(sketch_kernel, nz),
        out_shape=(
            jax.ShapeDtypeStruct((m, n), F32),
            jax.ShapeDtypeStruct((16, 2, piece, n), F32),
        ),
        in_specs=[anym] * 3,
        out_specs=(vm, vm),
        scratch_shapes=[
            pltpu.VMEM((4, 2, m // 2, k), BF16),
            pltpu.VMEM((5, k, n), BF16),
            pltpu.VMEM((UNITS, nz, 2, piece, n), F32),
            pltpu.VMEM((UNITS, nz, piece, n), F32),
            pltpu.VMEM((UNITS, 2, REACH, piece, n), F32),
            pltpu.VMEM((UNITS, piece, n), F32),
            dma((3,)),
            dma((6,)),
            dma((6,)),
            dma((4,)),
            dma((4,)),
            dma((UNITS,)),
            dma((UNITS,)),
            dma((UNITS, 2, REACH)),
            dma((UNITS, 2, REACH)),
            dma((UNITS,)),
            dma((UNITS,)),
            dma((2,)),
            dma((16, 2)),
        ],
        compiler_params=pltpu.CompilerParams(collective_id=2, has_side_effects=True),
    )(omega.reshape(2, m // 2, k), basis, vecs)


def body(omega, basis, vectors):
    ns, nr = lax.axis_size("section"), lax.axis_size("row")
    s = lax.axis_index("section")
    vecs = jnp.pad(vectors.T, ((0, 0), (0, basis.shape[1] - vectors.shape[0])))
    sketch, probe = sketch_call(omega, basis, vecs, nr)
    pair, ahead, inv = pair_call(sketch, ns, nr)
    width = vectors.shape[1] // ns
    mine = lax.dynamic_slice_in_dim(vectors, s * width, width, 1)
    return chain_call(pair, ahead, inv, probe.reshape(-1, probe.shape[-1]), basis, mine, ns, nr)


def solution(mesh):
    placed = (P("section", "row"), P("row", "section"), P(None, "row"))
    return jax.shard_map(
        body,
        mesh=mesh,
        in_specs=placed,
        out_specs=(P(None, ("row", "section")), P(None, "section")),
        check_vma=False,
    )
```

```python
import functools

import jax
import jax.numpy as jnp
from jax import lax
from jax.experimental import pallas as pl
from jax.experimental.pallas import tpu as pltpu
from jax.sharding import PartitionSpec as P

F32 = jnp.float32
BF16 = jnp.bfloat16
HI = lax.Precision.HIGHEST
MESH = pl.DeviceIdType.MESH


def split(x):
    hi = x.astype(BF16)
    return hi, (x - hi.astype(F32)).astype(BF16)


def dot3(a, b, dims):
    (ah, al), (bh, bl) = a, b

    def one(x, y):
        return lax.dot_general(x, y, (dims, ((), ())), preferred_element_type=F32)

    return one(ah, bh) + (one(al, bh) + one(ah, bl))


NN = ((1,), (0,))
NT = ((1,), (1,))
TN = ((0,), (0,))


def remote(src, dst, send, recv, section, row):
    return pltpu.make_async_remote_copy(
        src_ref=src,
        dst_ref=dst,
        send_sem=send,
        recv_sem=recv,
        device_id=(section, row),
        device_id_type=MESH,
    )


def packed(c):
    half = c.shape[1] // 2
    return jnp.concatenate([c[:4, :half], c[:4, half:]], axis=0)


def unpacked(c):
    wide = jnp.concatenate([c[:4], c[4:]], axis=1)
    return jnp.concatenate([wide, jnp.zeros_like(wide)], axis=0)


def chain_kernel(
    ns,
    nr,
    s_ref,
    next_ref,
    inv_ref,
    p0_ref,
    basis_ref,
    vec_ref,
    ortho_ref,
    coef_ref,
    hi_ref,
    lo_ref,
    kept,
    low_part,
    probe,
    moved,
    cout,
    cin,
    own,
    oin,
    sout,
    sin,
    bout,
    bin_,
    c_send,
    c_recv,
    p_send,
    p_recv,
    o_send,
    o_recv,
    s_send,
    s_recv,
    b_send,
    b_recv,
    k_send,
    k_recv,
    dout,
    din,
    d_send,
    d_recv,
):
    s, r = lax.axis_index("section"), lax.axis_index("row")
    n = kept.shape[1]
    on = active(s)
    off = jnp.logical_not(on)
    odd = lax.rem(s, 2) == 1
    mate = mate_of(s)
    c = lax.rem(r, 2)
    other_core = r + 1 - 2 * c
    after, before = next_of(s, ns)

    pass_coef = remote(low_part, kept, k_send, k_recv, mate, r)

    def combine(i, value):
        first, second = value[:, :128], value[:, 128:]
        dout[i] = jnp.where(c == 0, second, first)
        swap = remote(dout.at[i], din.at[i], d_send.at[i], d_recv.at[i], s, other_core)
        swap.start()
        keep = jnp.where(c == 0, first, second)
        swap.wait_recv()
        cout[...] = keep + din[i]
        swap.wait_send()

    @pl.when(on)
    def _():
        sp = split(s_ref[...])
        nx = split(next_ref[...])
        iv = split(inv_ref[...])

        @pl.when(s == 1)
        def _():
            p = p0_ref[...].reshape(moved.shape[1], n)[:, :128].T[:8]
            probe[...] = p
            combine(0, packed(dot3(split(p), sp, NN)))
            copies = []
            for step in range(1, nr):
                peer = lax.rem(r + step, nr)
                cp = remote(cout, cin.at[r], c_send.at[step], c_recv.at[r], 1, peer)
                cp.start()
                copies.append(cp)
            cin[pl.ds(r, 1)] = cout[...][None]
            for cp in copies:
                cp.wait_send()

        hi_ref[...], lo_ref[...] = split(dot3(iv, split(dot3(sp, nx, TN)), NN))

        @pl.when(s == 1)
        def _():
            for step in range(1, nr):
                peer = lax.rem(r + step, nr)
                remote(cout, cin.at[peer], c_send.at[step], c_recv.at[peer], 1, peer).wait_recv()

        @pl.when(s > 1)
        def _():
            remote(moved, probe, p_send, p_recv, before, r).wait_recv()

        p = probe[...]
        ahead = dot3(split(p), nx, NN)

        @pl.when(s > 1)
        def _():
            for q in range(nr):
                remote(cout, cin.at[q], c_send.at[q], c_recv.at[q], before, q).wait_recv()

        sums = [cin[0], cin[1]]
        for q in range(2, nr):
            sums[q % 2] = sums[q % 2] + cin[q]
        inner = split(unpacked(jnp.concatenate(sums, axis=1)))

        @pl.when(s != LAST)
        def _():
            combine(1, packed(ahead - dot3(inner, (hi_ref[...], lo_ref[...]), NN)))
            for q in range(nr):
                remote(cout, cin.at[r], c_send.at[q], c_recv.at[r], after, q).start()

        coef = dot3(inner, iv, NN)
        low_part[...] = jnp.where(odd, coef[:, :n], coef[:, n:])
        kept[...] = jnp.where(odd, coef[:, n:], coef[:, :n])
        moved[...] = p - dot3(split(coef), sp, NT)

        @pl.when(s != LAST)
        def _():
            remote(moved, probe, p_send, p_recv, after, r).start()

        pass_coef.start()

    @pl.when(off)
    def _():
        pass_coef.wait_recv()

    coef = kept[...]
    coef_ref[...] = coef[:4]
    term = lax.dot_general(coef.astype(BF16), basis_ref[...], (NT, ((), ())), preferred_element_type=F32)
    for k in range(ns // 2):
        own[k] = term[:, k * 128 : (k + 1) * 128]
    outs = []
    for step in range(1, ns):
        t = lax.rem(s + step, ns)
        cp = remote(own.at[lax.div(t, 2)], oin.at[s], o_send.at[step], o_recv.at[s], t, r)
        cp.start()
        outs.append(cp)
    oin[pl.ds(s, 1)] = own[pl.ds(lax.div(s, 2), 1)]

    @pl.when(s == LAST)
    def _():
        m = split(moved[...])
        sq = dot3(m, m, NT)
        sout[...] = jnp.concatenate([sq, jnp.zeros((8, 120), F32)], axis=1)
        copies = []
        for step in range(1, nr):
            peer = lax.rem(r + step, nr)
            cp = remote(sout, sin.at[r], s_send.at[step], s_recv.at[r], s, peer)
            cp.start()
            copies.append(cp)
        sin[pl.ds(r, 1)] = sout[...][None]
        for step in range(1, nr):
            peer = lax.rem(r + step, nr)
            remote(sout, sin.at[peer], s_send.at[step], s_recv.at[peer], s, peer).wait_recv()
        tot = sin[0]
        for q in range(1, nr):
            tot = tot + sin[q]
        bout[...] = tot
        bcs = []
        for t in range(ns):
            if t != LAST:
                cp = remote(bout, bin_, b_send.at[t], b_recv, t, r)
                cp.start()
                bcs.append(cp)
        for cp in copies + bcs:
            cp.wait_send()
        bin_[...] = tot

    for step in range(1, ns):
        t = lax.rem(s + step, ns)
        remote(own.at[0], oin.at[t], o_send.at[step], o_recv.at[t], t, r).wait_recv()
    removed = oin[0]
    for t in range(1, ns):
        removed = removed + oin[t]
    window = pl.ds(pl.multiple_of(lax.div(s, 2) * 128, 128), 128)
    remain = vec_ref[:, window].astype(F32) - removed[:4]
    remain = jnp.where(odd, remain[:, 64:], remain[:, :64])

    @pl.when(s != LAST)
    def _():
        remote(bout, bin_, b_send.at[0], b_recv, LAST, r).wait_recv()

    @pl.when(on & (s != LAST))
    def _():
        for q in range(nr):
            remote(cout, cin.at[q], c_send.at[q], c_recv.at[q], after, q).wait_send()
        remote(moved, probe, p_send, p_recv, after, r).wait_send()

    @pl.when(on)
    def _():
        pass_coef.wait_send()

    small = bin_[...]

    def at(i, k):
        return small[i : i + 1, k : k + 1]

    low = [[None] * 4 for _ in range(4)]
    rows = []
    for i in range(4):
        for k in range(i + 1):
            v = at(i, k)
            for m in range(k):
                v = v - low[i][m] * low[k][m]
            low[i][k] = jnp.sqrt(v) if i == k else v / low[k][k]
        x = remain[i : i + 1]
        for k in range(i):
            x = x - low[i][k] * rows[k]
        rows.append(x / low[i][i])
    ortho_ref[...] = jnp.concatenate(rows, axis=0)
    for cp in outs:
        cp.wait_send()


def eliminate(a):
    n = a.shape[0]
    rows = lax.broadcasted_iota(jnp.int32, (n, n), 0)
    cols = lax.broadcasted_iota(jnp.int32, (n, n), 1)
    lane = lax.broadcasted_iota(jnp.int32, (1, n), 1)
    for k in range(0, n, 2):
        c1 = jnp.broadcast_to(a[:, k : k + 1], (n, n))
        c2 = jnp.broadcast_to(a[:, k + 1 : k + 2], (n, n))
        p, q, s = c1[k : k + 1], c2[k : k + 1], c2[k + 1 : k + 2]
        e = 1.0 / (p * s - q * q)
        r1 = jnp.where(lane == k, 1.0, jnp.where(lane == k + 1, 0.0, a[k : k + 1, :]))
        r2 = jnp.where(lane == k + 1, 1.0, jnp.where(lane == k, 0.0, a[k + 1 : k + 2, :]))
        w1 = (s * e) * r1 - (q * e) * r2
        w2 = (p * e) * r2 - (q * e) * r1
        base = jnp.where((cols == k) | (cols == k + 1), 0.0, a)
        new = base - c1 * w1 - c2 * w2
        last = jnp.where(rows == k + 1, jnp.broadcast_to(w2, (n, n)), new)
        a = jnp.where(rows == k, jnp.broadcast_to(w1, (n, n)), last)
    return a


FIRST, LAST = 1, 14


def active(s):
    x = lax.rem(s, 4)
    return (x == 1) | (x == 2)


def mate_of(s):
    return s + 1 - 2 * lax.rem(s, 2)


def next_of(s, ns):
    odd = lax.rem(s, 2) == 1
    return lax.rem(s + jnp.where(odd, 1, 3), ns), lax.rem(s + ns - jnp.where(odd, 3, 1), ns)


def pair_kernel(
    ns,
    nr,
    close,
    s_ref,
    pair_ref,
    ahead_ref,
    uinv_ref,
    part,
    got,
    red,
    full,
    inv,
    mate_inv,
    n_send,
    n_recv,
    rs_send,
    rs_recv,
    ag_send,
    ag_recv,
    i_send,
    i_recv,
):
    s, r = lax.axis_index("section"), lax.axis_index("row")
    n = s_ref.shape[1]
    rows = n // nr
    on = active(s)
    off = jnp.logical_not(on)
    odd = lax.rem(s, 2) == 1
    even = lax.rem(s, 2) == 0
    mate = mate_of(s)
    low, high = pl.ds(0, n), pl.ds(n, n)
    x = lax.rem(s, 4)
    back = jnp.where(x == 1, 3, jnp.where(x == 2, 1, 2))
    last = lax.rem(s + ns - back, ns)
    to_mate = [
        remote(s_ref, pair_ref.at[:, where], n_send.at[0], n_recv.at[0], mate, r) for where in (low, high)
    ]
    to_last = [
        remote(s_ref, ahead_ref.at[:, where], n_send.at[1], n_recv.at[1 + k], last, r)
        for k, where in enumerate((low, high))
    ]

    def span(peer):
        return pl.ds(pl.multiple_of(peer * rows, rows), rows)

    def scatter(i, step):
        peer = lax.rem(r + step, nr)
        return remote(
            part.at[i, span(peer)], got.at[i, step], rs_send.at[i, step], rs_recv.at[i, step], s, peer
        )

    def gather(i, step, sending):
        peer = lax.rem(r + (step if sending else nr - step), nr)
        where = span(r if sending else peer)
        return remote(red.at[i], full.at[i, where], ag_send.at[i, step], ag_recv.at[i, step], s, peer)

    def begin(i):
        for step in range(1, nr):
            scatter(i, step).start()

    def middle(i):
        for step in range(1, nr):
            scatter(i, step).wait_recv()
        total = part[i, span(r), :]
        for step in range(1, nr):
            total = total + got[i, step]
        red[i] = total
        for step in range(1, nr):
            gather(i, step, True).start()
        full[i, span(r), :] = total

    def end(i):
        for step in range(1, nr):
            gather(i, step, False).wait_recv()
        for step in range(1, nr):
            scatter(i, step).wait_send()
            gather(i, step, True).wait_send()

    sp = split(s_ref[...])
    part[0] = dot3(sp, sp, TN)
    begin(0)
    close()

    for k, mine in enumerate((even, odd)):

        @pl.when(mine & off)
        def _():
            to_mate[k].start()

        @pl.when(mine & (s >= 2))
        def _():
            to_last[k].start()

        @pl.when(mine)
        def _():
            pair_ref[:, k * n : (k + 1) * n] = s_ref[...]

    middle(0)

    for k, mine in enumerate((even, odd)):

        @pl.when(mine & on)
        def _():
            to_mate[1 - k].wait_recv()

    @pl.when(on)
    def _():
        part[1] = dot3(split(pair_ref[:, :n]), split(pair_ref[:, n:]), TN)
        begin(1)

    end(0)

    def dot(x, y, dims):
        return lax.dot_general(x, y, (dims, ((), ())), precision=HI, preferred_element_type=F32)

    g = full[0]
    h = n // 2
    eye = lax.broadcasted_iota(jnp.int32, (n, n), 0) == lax.broadcasted_iota(jnp.int32, (n, n), 1)
    d = jnp.where(eye, g, 0.0)
    rs = lax.rsqrt(jnp.sum(d, axis=1, keepdims=True))
    cs = lax.rsqrt(jnp.sum(d, axis=0, keepdims=True))
    g = g * rs * cs
    a, b, c = g[:h, :h], g[:h, h:], g[h:, h:]
    ai = eliminate(a)
    t = dot(ai, b, NN)
    rest = c - dot(b, t, TN)

    @pl.when(on)
    def _():
        middle(1)

    ci = eliminate(rest)
    u = dot(t, ci, NN)
    top = jnp.concatenate([ai + dot(u, t, NT), -u], axis=1)
    bottom = jnp.concatenate([-u.T, ci], axis=1)
    inv[...] = jnp.concatenate([top, bottom], axis=0) * rs * cs
    pass_inv = remote(inv, mate_inv, i_send, i_recv, mate, r)

    @pl.when(off)
    def _():
        pass_inv.start()

    @pl.when(on)
    def _():
        end(1)
        uinv_ref[n:, :n] = jnp.zeros((n, n), F32)

    @pl.when(on & odd)
    def _():
        mine = inv[...]
        right = dot3(split(full[1]), split(mine), NN)
        uinv_ref[n:, n:] = mine
        pass_inv.wait_recv()
        theirs = mate_inv[...]
        uinv_ref[:n, :n] = theirs
        uinv_ref[:n, n:] = -dot3(split(theirs), split(right), NN)

    @pl.when(on & even)
    def _():
        mine = inv[...]
        left = dot3(split(mine), split(full[1]), NN)
        uinv_ref[:n, :n] = mine
        pass_inv.wait_recv()
        theirs = mate_inv[...]
        uinv_ref[n:, n:] = theirs
        uinv_ref[:n, n:] = -dot3(split(left), split(theirs), NN)

    @pl.when(on & (s != LAST))
    def _():
        for cp in to_last:
            cp.wait_recv()

    @pl.when(s == LAST)
    def _():
        ahead_ref[...] = jnp.zeros(ahead_ref.shape, F32)

    @pl.when(off)
    def _():
        pass_inv.wait_send()
        to_mate[0].wait_send()

    @pl.when(s >= 2)
    def _():
        to_last[0].wait_send()


def within(t, first, yes, no):
    return jnp.where(t >= first, yes, no)


def unit(t):
    def seg(first, width):
        return lax.div(jnp.maximum(t - first, 0), width), lax.rem(jnp.maximum(t - first, 0), width)

    a, b = seg(4, 2)
    row, half, col = within(t, 2, 0, 0), lax.rem(t, 2), within(t, 2, 0, 4)
    row, half, col = row, within(t, 4, b, half), within(t, 4, 1 + a, col)
    a, b = seg(8, 3)
    row, half, col = within(t, 8, 1 + a, row), within(t, 8, a, half), within(t, 8, b, col)
    row, half, col = within(t, 14, 0, row), within(t, 14, t - 14, half), within(t, 14, 3, col)
    row, half, col = within(t, 16, t - 15, row), within(t, 16, t - 16, half), within(t, 16, 3, col)
    a, b = seg(18, 4)
    row, half, col = within(t, 18, 1 + a, row), within(t, 18, 1 - a, half), within(t, 18, b, col)
    a, b = seg(26, 4)
    row, half, col = within(t, 26, 3, row), within(t, 26, a, half), within(t, 26, b, col)
    return row, half, col


def slot_offset(d):
    return jnp.where(d == 0, 0, jnp.where(d == 1, 3, d - 1))


UNITS = 34
HOME = 1
REACH = 4
LAG = 3


def sketch_kernel(
    nz,
    omega_ref,
    basis_ref,
    vec_ref,
    s_ref,
    p_ref,
    obuf,
    bbuf,
    part,
    dbuf,
    rbuf,
    fbuf,
    l_sem,
    o_send,
    o_recv,
    b_send,
    b_recv,
    d_send,
    d_recv,
    r_send,
    r_recv,
    f_send,
    f_recv,
    p_send,
    p_recv,
):
    s, r = lax.axis_index("section"), lax.axis_index("row")
    y, x = lax.div(s, 4), lax.rem(s, 4)
    z, c = lax.div(r, 2), lax.rem(r, 2)

    def at(dy, dx):
        return lax.rem(y + dy, 4) * 4 + lax.rem(x + dx, 4)

    beside = (lax.rem(z + 1, nz) * 2 + c, lax.rem(z + nz - 1, nz) * 2 + c)
    mate = z * 2 + (1 - c)

    local = [
        pltpu.make_async_copy(omega_ref, obuf.at[0], l_sem.at[0]),
        pltpu.make_async_copy(basis_ref, bbuf.at[0], l_sem.at[1]),
    ]
    for cp in local:
        cp.start()

    barrier = pltpu.get_barrier_semaphore()
    ns, nr = 16, 2 * nz

    def hello(section, row):
        pl.semaphore_signal(barrier, inc=1, device_id=(section, row), device_id_type=MESH)

    for q in range(nr):
        for other in next_of(s, ns):
            hello(other, q)
    for step in range(1, nr):
        hello(s, lax.rem(r + step, nr))
    for step in range(1, ns):
        hello(lax.rem(s + step, ns), r)

    v = vec_ref[...].astype(F32)
    v = jnp.concatenate([v, jnp.zeros_like(v)], axis=0)
    v = jnp.concatenate([v, jnp.zeros((120, v.shape[1]), F32)], axis=0)
    bbuf[4, :, :128] = v.T.astype(BF16)
    bbuf[4, :, 128:] = jnp.zeros((v.shape[1], bbuf.shape[2] - 128), BF16)
    for cp in local:
        cp.wait()
    pl.semaphore_wait(barrier, 3 * nr + ns - 2)

    def ocopy(src, dst, half, sem, dy):
        return remote(obuf.at[src, half], obuf.at[dst, half], o_send.at[sem], o_recv.at[sem], at(dy, 0), r)

    def bcopy(src, dst, half, sem, dx):
        a, b = bbuf.at[src], bbuf.at[dst]
        if half is not None:
            a, b = a.at[pl.ds(512 * half, 512)], b.at[pl.ds(512 * half, 512)]
        return remote(a, b, b_send.at[sem], b_recv.at[sem], at(0, dx), r)

    b_own = [bcopy(0, 1, None, 0, 1), bcopy(0, 2, None, 1, 3)]
    o_own = [ocopy(0, 1, 0, 0, 1), ocopy(0, 2, 1, 1, 3)]
    o_rest = [ocopy(0, 1, 1, 2, 1), ocopy(0, 2, 0, 3, 3)]
    b_fwd = [bcopy(1, 3, 0, 2, 1), bcopy(2, 3, 1, 3, 3)]
    o_fwd = [ocopy(1, 3, 0, 4, 1), ocopy(2, 3, 1, 5, 3)]
    for cp in o_own + b_own + o_rest:
        cp.start()

    def dcopy(u):
        return remote(part.at[u, :, 1 - c], dbuf.at[u], d_send.at[u], d_recv.at[u], s, mate)

    def chunk(d, k):
        far = REACH - k
        return lax.rem(z + (far if d == 0 else nz - far), nz)

    def rcopy(u, d, k):
        return remote(
            part.at[u, chunk(d, k), c],
            rbuf.at[u, d, k],
            r_send.at[u, d, k],
            r_recv.at[u, d, k],
            s,
            beside[d],
        )

    def place(u):
        row, half, col = unit(u)
        dy, dx = slot_offset(row), slot_offset(col)
        start = (lax.rem(y + dy, 4) * 4 + x) * 32 + half * 16
        return dx, pl.ds(pl.multiple_of(start, 16), 16)

    def fcopy(u):
        dx, rows = place(u)
        return remote(fbuf.at[u], s_ref.at[rows], f_send.at[u], f_recv.at[u], at(0, dx), r)

    def pcopy(u, sender):
        return remote(fbuf.at[u], p_ref.at[sender, u], p_send.at[u], p_recv.at[sender, u], HOME, r)

    def step(t, carry):
        done = t - 2 - LAG * REACH

        @pl.when((done >= 0) & (done < UNITS))
        def _():
            rcopy(done, 0, REACH - 1).wait_recv()
            rcopy(done, 1, REACH - 1).wait_recv()
            fbuf[done] = (part[done, z, c] + dbuf[done, z]) + (
                rbuf[done, 0, REACH - 1] + rbuf[done, 1, REACH - 1]
            )

        @pl.when((done >= 2) & (done < UNITS))
        def _():
            dx, rows = place(done)

            @pl.when(dx == 0)
            def _():
                s_ref[rows, :] = fbuf[done]

            @pl.when(dx > 0)
            def _():
                fcopy(done).start()

        @pl.when((done >= 0) & (done < 2))
        def _():
            @pl.when(s == HOME)
            def _():
                p_ref[HOME, done] = fbuf[done]

            @pl.when(s != HOME)
            def _():
                pcopy(done, s).start()

        for k in range(REACH - 1, -1, -1):
            u = t - 2 - LAG * k
            valid = (u >= 0) & (u < UNITS)
            if k == 0:

                @pl.when(valid)
                def _():
                    dcopy(u).wait_recv()

            for d in range(2):
                longer = lax.rem(jnp.maximum(u, 0), 2) == d

                def own():
                    return part[u, chunk(d, k), c] + dbuf[u, chunk(d, k)]

                def send(val):
                    part[u, chunk(d, k), c] = val
                    rcopy(u, d, k).start()

                def pass_on():
                    rcopy(u, d, k - 1).wait_recv()
                    send(own() + rbuf[u, d, k - 1])

                if k == 0:

                    @pl.when(valid & longer)
                    def _():
                        send(own())

                elif k == 1:

                    @pl.when(valid & longer)
                    def _():
                        pass_on()

                    @pl.when(valid & jnp.logical_not(longer))
                    def _():
                        send(own())

                else:

                    @pl.when(valid)
                    def _():
                        pass_on()

        @pl.when(t == 4)
        def _():
            for cp in b_own:
                cp.wait_recv()
            for cp in b_fwd:
                cp.start()

        @pl.when(t == 8)
        def _():
            for cp in o_own:
                cp.wait_recv()
            for cp in o_fwd:
                cp.start()

        @pl.when(t == 14)
        def _():
            for cp in b_fwd:
                cp.wait_recv()

        @pl.when(t == 18)
        def _():
            for cp in o_rest:
                cp.wait_recv()

        @pl.when(t == 26)
        def _():
            for cp in o_fwd:
                cp.wait_recv()

        @pl.when(t < UNITS)
        def _():
            row, half, col = unit(t)
            out = jnp.dot(obuf[row, half], bbuf[col], preferred_element_type=F32)
            part[t] = out.reshape(part.shape[1:])
            dcopy(t).start()

        return carry

    lax.fori_loop(0, UNITS + 2 + LAG * REACH + 1, step, 0)

    def finish(u, carry):
        dx, _ = place(u)

        @pl.when(dx > 0)
        def _():
            fcopy(u).wait_recv()

        return carry

    lax.fori_loop(2, UNITS, finish, 0)

    @pl.when(s == HOME)
    def _():
        for t in range(16):
            if t != HOME:
                for u in range(2):
                    pcopy(u, t).wait_recv()

    def drain(u, carry):
        dcopy(u).wait_send()
        dx, _ = place(u)

        @pl.when((u >= 2) & (dx > 0))
        def _():
            fcopy(u).wait_send()

        for d in range(2):
            for k in range(REACH):
                if k:
                    rcopy(u, d, k).wait_send()
                else:

                    @pl.when(lax.rem(u, 2) == d)
                    def _():
                        rcopy(u, d, k).wait_send()

        return carry

    def close():
        @pl.when(s != HOME)
        def _():
            for u in range(2):
                pcopy(u, s).wait_send()

        for cp in b_own + o_own + o_rest + b_fwd + o_fwd:
            cp.wait_send()
        lax.fori_loop(0, UNITS, drain, 0)

    return close


def sketch_scratch(m, k, n, nr):
    nz, piece, dma = nr // 2, m // nr // 2, pltpu.SemaphoreType.DMA
    return [
        pltpu.VMEM((4, 2, m // 2, k), BF16),
        pltpu.VMEM((5, k, n), BF16),
        pltpu.VMEM((UNITS, nz, 2, piece, n), F32),
        pltpu.VMEM((UNITS, nz, piece, n), F32),
        pltpu.VMEM((UNITS, 2, REACH, piece, n), F32),
        pltpu.VMEM((UNITS, piece, n), F32),
        dma((2,)),
        dma((6,)),
        dma((6,)),
        dma((4,)),
        dma((4,)),
        dma((UNITS,)),
        dma((UNITS,)),
        dma((UNITS, 2, REACH)),
        dma((UNITS, 2, REACH)),
        dma((UNITS,)),
        dma((UNITS,)),
        dma((2,)),
        dma((16, 2)),
    ]


def pair_scratch(n, nr):
    dma = pltpu.SemaphoreType.DMA
    return [
        pltpu.VMEM((2, n, n), F32),
        pltpu.VMEM((2, nr, n // nr, n), F32),
        pltpu.VMEM((2, n // nr, n), F32),
        pltpu.VMEM((2, n, n), F32),
        pltpu.VMEM((n, n), F32),
        pltpu.VMEM((n, n), F32),
        dma((3,)),
        dma((3,)),
        dma((2, nr)),
        dma((2, nr)),
        dma((2, nr)),
        dma((2, nr)),
        dma,
        dma,
    ]


def chain_scratch(k, n, ns, nr):
    dma = pltpu.SemaphoreType.DMA
    return [
        pltpu.VMEM((n, n), BF16),
        pltpu.VMEM((n, n), BF16),
        pltpu.VMEM((8, n // 2), F32),
        pltpu.VMEM((8, n // 2), F32),
        pltpu.VMEM((8, k), F32),
        pltpu.VMEM((8, k), F32),
        pltpu.VMEM((8, 128), F32),
        pltpu.VMEM((nr, 8, 128), F32),
        pltpu.VMEM((ns // 2, 8, 128), F32),
        pltpu.VMEM((ns, 8, 128), F32),
        pltpu.VMEM((8, 128), F32),
        pltpu.VMEM((nr, 8, 128), F32),
        pltpu.VMEM((8, 128), F32),
        pltpu.VMEM((8, 128), F32),
        dma((nr,)),
        dma((nr,)),
        dma,
        dma,
        dma((ns,)),
        dma((ns,)),
        dma((nr,)),
        dma((nr,)),
        dma((ns,)),
        dma,
        dma,
        dma,
        pltpu.VMEM((2, 8, 128), F32),
        pltpu.VMEM((2, 8, 128), F32),
        dma((2,)),
        dma((2,)),
    ]


def whole_kernel(ns, nr, ends, omega_ref, basis_ref, vec_ref, ortho_ref, coef_ref, *rest):
    s_ref, p_ref, pair_ref, ahead_ref, uinv_ref = rest[:5]
    first, second = rest[5 : ends[0]], rest[ends[0] : ends[1]]
    close = sketch_kernel(nr // 2, omega_ref, basis_ref, vec_ref, s_ref, p_ref, *first)
    pair_kernel(ns, nr, close, s_ref, pair_ref, ahead_ref, uinv_ref, *second)
    own_basis = first[1].at[0]
    chain_kernel(
        ns,
        nr,
        pair_ref,
        ahead_ref,
        uinv_ref,
        p_ref,
        own_basis,
        vec_ref,
        ortho_ref,
        coef_ref,
        *rest[ends[1] :],
    )


def whole_call(omega, basis, vectors, ns, nr):
    vm = pl.BlockSpec(memory_space=pltpu.VMEM)
    anym = pl.BlockSpec(memory_space=pl.ANY)
    m, k = omega.shape
    n = basis.shape[1]
    kept = [
        pltpu.VMEM((m, n), F32),
        pltpu.VMEM((ns, 2, m // nr // 2, n), F32),
        pltpu.VMEM((m, 2 * n), F32),
        pltpu.VMEM((m, 2 * n), F32),
        pltpu.VMEM((2 * n, 2 * n), F32),
    ]
    one = sketch_scratch(m, k, n, nr)
    two = pair_scratch(n, nr)
    three = chain_scratch(m, 2 * n, ns, nr)
    ends = (len(kept) + len(one), len(kept) + len(one) + len(two))
    return pl.pallas_call(
        functools.partial(whole_kernel, ns, nr, ends),
        out_shape=(
            jax.ShapeDtypeStruct((4, vectors.shape[1] // ns), F32),
            jax.ShapeDtypeStruct((4, n), F32),
        ),
        in_specs=[anym, anym, vm],
        out_specs=(vm, vm),
        scratch_shapes=kept + one + two + three,
        compiler_params=pltpu.CompilerParams(
            collective_id=0, has_side_effects=True, vmem_limit_bytes=60 * 1024 * 1024
        ),
    )(omega.reshape(2, m // 2, k), basis, vectors)


def body(omega, basis, vectors):
    return whole_call(omega, basis, vectors, lax.axis_size("section"), lax.axis_size("row"))


def solution(mesh):
    placed = (P("section", "row"), P("row", "section"), P(None, "row"))
    return jax.shard_map(
        body,
        mesh=mesh,
        in_specs=placed,
        out_specs=(P(None, ("row", "section")), P(None, "section")),
        check_vma=False,
    )
```

```python
import functools

import jax
import jax.numpy as jnp
from jax import lax
from jax.experimental import pallas as pl
from jax.experimental.pallas import tpu as pltpu
from jax.sharding import PartitionSpec as P

F32 = jnp.float32
BF16 = jnp.bfloat16
HI = lax.Precision.HIGHEST
MESH = pl.DeviceIdType.MESH


def split(x):
    hi = x.astype(BF16)
    return hi, (x - hi.astype(F32)).astype(BF16)


def dot3(a, b, dims):
    (ah, al), (bh, bl) = a, b

    def one(x, y):
        return lax.dot_general(x, y, (dims, ((), ())), preferred_element_type=F32)

    return one(ah, bh) + (one(al, bh) + one(ah, bl))


NN = ((1,), (0,))
NT = ((1,), (1,))
TN = ((0,), (0,))


def remote(src, dst, send, recv, section, row):
    return pltpu.make_async_remote_copy(
        src_ref=src,
        dst_ref=dst,
        send_sem=send,
        recv_sem=recv,
        device_id=(section, row),
        device_id_type=MESH,
    )


def packed(c):
    half = c.shape[1] // 2
    return jnp.concatenate([c[:4, :half], c[:4, half:]], axis=0)


def unpacked(c):
    wide = jnp.concatenate([c[:4], c[4:]], axis=1)
    return jnp.concatenate([wide, jnp.zeros_like(wide)], axis=0)


def combine(i, value, cout, dout, din, d_send, d_recv):
    s, r = lax.axis_index("section"), lax.axis_index("row")
    c = lax.rem(r, 2)
    first, second = value[:, :128], value[:, 128:]
    dout[i] = jnp.where(c == 0, second, first)
    swap = remote(dout.at[i], din.at[i], d_send.at[i], d_recv.at[i], s, r + 1 - 2 * c)
    swap.start()
    keep = jnp.where(c == 0, first, second)
    swap.wait_recv()
    cout[...] = keep + din[i]
    swap.wait_send()


def first_products(nr, s_ref, p0_ref, refs):
    probe, cout, cin, c_send, c_recv = refs[4], refs[6], refs[7], refs[14], refs[15]
    r = lax.axis_index("row")
    rows, n = s_ref.shape
    p = p0_ref[...].reshape(rows, n // 2)[:, :128].T[:8]
    probe[...] = p
    combine(0, packed(dot3(split(p), split(s_ref[...]), NN)), cout, *refs[-4:])
    for step in range(1, nr):
        remote(cout, cin.at[r], c_send.at[step], c_recv.at[r], FIRST, lax.rem(r + step, nr)).start()
    cin[pl.ds(r, 1)] = cout[...][None]


def chain_kernel(
    ns,
    nr,
    s_ref,
    next_ref,
    inv_ref,
    cross_ref,
    basis_ref,
    vec_ref,
    ortho_ref,
    coef_ref,
    hi_ref,
    lo_ref,
    kept,
    low_part,
    probe,
    moved,
    cout,
    cin,
    own,
    oin,
    sout,
    sin,
    bout,
    bin_,
    c_send,
    c_recv,
    p_send,
    p_recv,
    o_send,
    o_recv,
    s_send,
    s_recv,
    b_send,
    b_recv,
    k_send,
    k_recv,
    dout,
    din,
    d_send,
    d_recv,
):
    s, r = lax.axis_index("section"), lax.axis_index("row")
    n = kept.shape[1]
    on = active(s)
    off = jnp.logical_not(on)
    odd = lax.rem(s, 2) == 1
    mate = mate_of(s)
    after, before = next_of(s, ns)

    pass_coef = remote(low_part, kept, k_send, k_recv, mate, r)

    @pl.when(on)
    def _():
        sp = split(s_ref[...])
        nx = split(next_ref[...])
        iv = split(inv_ref[...])

        hi_ref[...], lo_ref[...] = split(dot3(iv, split(cross_ref[...]), NN))

        @pl.when(s == FIRST)
        def _():
            for step in range(1, nr):
                peer = lax.rem(r + step, nr)
                remote(cout, cin.at[peer], c_send.at[step], c_recv.at[peer], FIRST, peer).wait()

        @pl.when(s != FIRST)
        def _():
            remote(moved, probe, p_send, p_recv, before, r).wait_recv()

        p = probe[...]
        ahead = dot3(split(p), nx, NN)

        @pl.when(s != FIRST)
        def _():
            for q in range(nr):
                remote(cout, cin.at[q], c_send.at[q], c_recv.at[q], before, q).wait_recv()

        sums = [cin[0], cin[1]]
        for q in range(2, nr):
            sums[q % 2] = sums[q % 2] + cin[q]
        inner = split(unpacked(jnp.concatenate(sums, axis=1)))

        @pl.when(s != LAST)
        def _():
            partial = packed(ahead - dot3(inner, (hi_ref[...], lo_ref[...]), NN))
            combine(1, partial, cout, dout, din, d_send, d_recv)
            for q in range(nr):
                remote(cout, cin.at[r], c_send.at[q], c_recv.at[r], after, q).start()

        coef = dot3(inner, iv, NN)
        low_part[...] = jnp.where(odd, coef[:, :n], coef[:, n:])
        kept[...] = jnp.where(odd, coef[:, n:], coef[:, :n])
        moved[...] = p - dot3(split(coef), sp, NT)

        @pl.when(s != LAST)
        def _():
            remote(moved, probe, p_send, p_recv, after, r).start()

        pass_coef.start()

    @pl.when(off)
    def _():
        pass_coef.wait_recv()

    coef = kept[...]
    coef_ref[...] = coef[:4]
    term = lax.dot_general(coef.astype(BF16), basis_ref[...], (NT, ((), ())), preferred_element_type=F32)
    for k in range(ns // 2):
        own[k] = term[:, k * 128 : (k + 1) * 128]
    outs = []
    for step in range(1, ns):
        t = lax.rem(s + step, ns)
        cp = remote(own.at[lax.div(t, 2)], oin.at[s], o_send.at[step], o_recv.at[s], t, r)
        cp.start()
        outs.append(cp)
    oin[pl.ds(s, 1)] = own[pl.ds(lax.div(s, 2), 1)]

    @pl.when(s == LAST)
    def _():
        m = split(moved[...])
        sq = dot3(m, m, NT)
        sout[...] = jnp.concatenate([sq, jnp.zeros((8, 120), F32)], axis=1)
        copies = []
        for step in range(1, nr):
            peer = lax.rem(r + step, nr)
            cp = remote(sout, sin.at[r], s_send.at[step], s_recv.at[r], s, peer)
            cp.start()
            copies.append(cp)
        sin[pl.ds(r, 1)] = sout[...][None]
        for step in range(1, nr):
            peer = lax.rem(r + step, nr)
            remote(sout, sin.at[peer], s_send.at[step], s_recv.at[peer], s, peer).wait_recv()
        tot = sin[0]
        for q in range(1, nr):
            tot = tot + sin[q]
        bout[...] = tot
        bcs = []
        for t in range(ns):
            if t != LAST:
                cp = remote(bout, bin_, b_send.at[t], b_recv, t, r)
                cp.start()
                bcs.append(cp)
        for cp in copies + bcs:
            cp.wait_send()
        bin_[...] = tot

    for step in range(1, ns):
        t = lax.rem(s + step, ns)
        remote(own.at[0], oin.at[t], o_send.at[step], o_recv.at[t], t, r).wait_recv()
    removed = oin[0]
    for t in range(1, ns):
        removed = removed + oin[t]
    window = pl.ds(pl.multiple_of(lax.div(s, 2) * 128, 128), 128)
    remain = vec_ref[:, window].astype(F32) - removed[:4]
    remain = jnp.where(odd, remain[:, 64:], remain[:, :64])

    @pl.when(s != LAST)
    def _():
        remote(bout, bin_, b_send.at[0], b_recv, LAST, r).wait_recv()

    @pl.when(on & (s != LAST))
    def _():
        for q in range(nr):
            remote(cout, cin.at[q], c_send.at[q], c_recv.at[q], after, q).wait_send()
        remote(moved, probe, p_send, p_recv, after, r).wait_send()

    @pl.when(on)
    def _():
        pass_coef.wait_send()

    small = bin_[...]

    def at(i, k):
        return small[i : i + 1, k : k + 1]

    low = [[None] * 4 for _ in range(4)]
    rows = []
    for i in range(4):
        for k in range(i + 1):
            v = at(i, k)
            for m in range(k):
                v = v - low[i][m] * low[k][m]
            low[i][k] = jnp.sqrt(v) if i == k else v / low[k][k]
        x = remain[i : i + 1]
        for k in range(i):
            x = x - low[i][k] * rows[k]
        rows.append(x / low[i][i])
    ortho_ref[...] = jnp.concatenate(rows, axis=0)
    for cp in outs:
        cp.wait_send()


def eliminate(a):
    n = a.shape[0]
    rows = lax.broadcasted_iota(jnp.int32, (n, n), 0)
    cols = lax.broadcasted_iota(jnp.int32, (n, n), 1)
    lane = lax.broadcasted_iota(jnp.int32, (1, n), 1)
    for k in range(0, n, 2):
        c1 = jnp.broadcast_to(a[:, k : k + 1], (n, n))
        c2 = jnp.broadcast_to(a[:, k + 1 : k + 2], (n, n))
        p, q, s = c1[k : k + 1], c2[k : k + 1], c2[k + 1 : k + 2]
        e = 1.0 / (p * s - q * q)
        r1 = jnp.where(lane == k, 1.0, jnp.where(lane == k + 1, 0.0, a[k : k + 1, :]))
        r2 = jnp.where(lane == k + 1, 1.0, jnp.where(lane == k, 0.0, a[k + 1 : k + 2, :]))
        w1 = (s * e) * r1 - (q * e) * r2
        w2 = (p * e) * r2 - (q * e) * r1
        base = jnp.where((cols == k) | (cols == k + 1), 0.0, a)
        new = base - c1 * w1 - c2 * w2
        last = jnp.where(rows == k + 1, jnp.broadcast_to(w2, (n, n)), new)
        a = jnp.where(rows == k, jnp.broadcast_to(w1, (n, n)), last)
    return a


FIRST, LAST = 1, 14


def active(s):
    x = lax.rem(s, 4)
    return (x == 1) | (x == 2)


def mate_of(s):
    return s + 1 - 2 * lax.rem(s, 2)


def next_of(s, ns):
    odd = lax.rem(s, 2) == 1
    return lax.rem(s + jnp.where(odd, 1, 3), ns), lax.rem(s + ns - jnp.where(odd, 3, 1), ns)


def pair_kernel(
    ns,
    nr,
    close,
    start_chain,
    s_ref,
    pair_ref,
    ahead_ref,
    uinv_ref,
    cross_ref,
    part,
    got,
    red,
    full,
    inv,
    early,
    late,
    mate_early,
    mate_late,
    n_send,
    n_recv,
    rs_send,
    rs_recv,
    ag_send,
    ag_recv,
    i_send,
    i_recv,
):
    s, r = lax.axis_index("section"), lax.axis_index("row")
    n = s_ref.shape[1]
    rows = n // nr
    on = active(s)
    off = jnp.logical_not(on)
    odd = lax.rem(s, 2) == 1
    even = lax.rem(s, 2) == 0
    mate = mate_of(s)
    low, high = pl.ds(0, n), pl.ds(n, n)
    x = lax.rem(s, 4)
    back = jnp.where(x == 1, 3, jnp.where(x == 2, 1, 2))
    last = lax.rem(s + ns - back, ns)
    to_mate = [
        remote(s_ref, pair_ref.at[:, where], n_send.at[0], n_recv.at[0], mate, r) for where in (low, high)
    ]
    to_last = [
        remote(s_ref, ahead_ref.at[:, where], n_send.at[1], n_recv.at[1 + k], last, r)
        for k, where in enumerate((low, high))
    ]

    def span(peer):
        return pl.ds(pl.multiple_of(peer * rows, rows), rows)

    def scatter(i, step):
        peer = lax.rem(r + step, nr)
        return remote(
            part.at[i, span(peer)], got.at[i, step], rs_send.at[i, step], rs_recv.at[i, step], s, peer
        )

    def gather(i, step, sending):
        peer = lax.rem(r + (step if sending else nr - step), nr)
        where = span(r if sending else peer)
        return remote(red.at[i], full.at[i, where], ag_send.at[i, step], ag_recv.at[i, step], s, peer)

    def begin(i):
        for step in range(1, nr):
            scatter(i, step).start()

    def middle(i):
        for step in range(1, nr):
            scatter(i, step).wait_recv()
        total = part[i, span(r), :]
        for step in range(1, nr):
            total = total + got[i, step]
        red[i] = total
        for step in range(1, nr):
            gather(i, step, True).start()
        full[i, span(r), :] = total

    def end(i):
        for step in range(1, nr):
            gather(i, step, False).wait_recv()
        for step in range(1, nr):
            scatter(i, step).wait_send()
            gather(i, step, True).wait_send()

    sp = split(s_ref[...])
    part[0] = dot3(sp, sp, TN)
    begin(0)
    close()

    for k, mine in enumerate((even, odd)):

        @pl.when(mine & off)
        def _():
            to_mate[k].start()

        @pl.when(mine & (s >= 2))
        def _():
            to_last[k].start()

        @pl.when(mine)
        def _():
            pair_ref[:, k * n : (k + 1) * n] = s_ref[...]

    middle(0)

    for k, mine in enumerate((even, odd)):

        @pl.when(mine & on)
        def _():
            to_mate[1 - k].wait_recv()

    @pl.when(on)
    def _():
        part[1] = dot3(split(pair_ref[:, :n]), split(pair_ref[:, n:]), TN)
        begin(1)

    end(0)

    def dot(x, y, dims):
        return lax.dot_general(x, y, (dims, ((), ())), precision=HI, preferred_element_type=F32)

    g = full[0]
    h = n // 2
    eye = lax.broadcasted_iota(jnp.int32, (n, n), 0) == lax.broadcasted_iota(jnp.int32, (n, n), 1)
    d = jnp.where(eye, g, 0.0)
    rs = lax.rsqrt(jnp.sum(d, axis=1, keepdims=True))
    cs = lax.rsqrt(jnp.sum(d, axis=0, keepdims=True))
    g = g * rs * cs
    a, b, c = g[:h, :h], g[:h, h:], g[h:, h:]
    ai = eliminate(a)
    t = dot(ai, b, NN)
    rest = c - dot(b, t, TN)
    early[0] = ai * rs[:h] * cs[:, :h]
    early[1] = t * rs[:h] / cs[:, h:]
    pass_early = remote(early, mate_early, i_send.at[0], i_recv.at[0], mate, r)
    pass_late = remote(late, mate_late, i_send.at[1], i_recv.at[1], mate, r)

    @pl.when(off)
    def _():
        pass_early.start()

    @pl.when(on)
    def _():
        middle(1)

    @pl.when(s == FIRST)
    def _():
        start_chain()

    late[...] = eliminate(rest) * rs[h:] * cs[:, h:]

    @pl.when(off)
    def _():
        pass_late.start()

    def whole_inverse(parts, corner):
        t, ci = parts[1], corner[...]
        u = dot(t, ci, NN)
        top = jnp.concatenate([parts[0] + dot(u, t, NT), -u], axis=1)
        bottom = jnp.concatenate([-u.T, ci], axis=1)
        return jnp.concatenate([top, bottom], axis=0)

    @pl.when(on)
    def _():
        inv[...] = whole_inverse(early, late)
        uinv_ref[n:, :n] = jnp.zeros((n, n), F32)

    @pl.when(on & (s != LAST))
    def _():
        for cp in to_last:
            cp.wait_recv()

    @pl.when(s == LAST)
    def _():
        ahead_ref[...] = jnp.zeros(ahead_ref.shape, F32)

    @pl.when(on)
    def _():
        cross_ref[...] = dot3(split(pair_ref[...]), split(ahead_ref[...]), TN)
        end(1)
        pass_early.wait_recv()
        pass_late.wait_recv()

    @pl.when(on & odd)
    def _():
        mine, theirs = inv[...], whole_inverse(mate_early, mate_late)
        right = dot3(split(full[1]), split(mine), NN)
        uinv_ref[n:, n:] = mine
        uinv_ref[:n, :n] = theirs
        uinv_ref[:n, n:] = -dot3(split(theirs), split(right), NN)

    @pl.when(on & even)
    def _():
        mine, theirs = inv[...], whole_inverse(mate_early, mate_late)
        left = dot3(split(mine), split(full[1]), NN)
        uinv_ref[:n, :n] = mine
        uinv_ref[n:, n:] = theirs
        uinv_ref[:n, n:] = -dot3(split(left), split(theirs), NN)

    @pl.when(off)
    def _():
        pass_early.wait_send()
        pass_late.wait_send()
        to_mate[0].wait_send()

    @pl.when(s >= 2)
    def _():
        to_last[0].wait_send()


def within(t, first, yes, no):
    return jnp.where(t >= first, yes, no)


def unit(t):
    def seg(first, width):
        return lax.div(jnp.maximum(t - first, 0), width), lax.rem(jnp.maximum(t - first, 0), width)

    a, b = seg(4, 2)
    row, half, col = within(t, 2, 0, 0), lax.rem(t, 2), within(t, 2, 0, 4)
    row, half, col = row, within(t, 4, b, half), within(t, 4, 1 + a, col)
    a, b = seg(8, 3)
    row, half, col = within(t, 8, 1 + a, row), within(t, 8, a, half), within(t, 8, b, col)
    row, half, col = within(t, 14, 0, row), within(t, 14, t - 14, half), within(t, 14, 3, col)
    row, half, col = within(t, 16, t - 15, row), within(t, 16, t - 16, half), within(t, 16, 3, col)
    a, b = seg(18, 4)
    row, half, col = within(t, 18, 1 + a, row), within(t, 18, 1 - a, half), within(t, 18, b, col)
    a, b = seg(26, 4)
    row, half, col = within(t, 26, 3, row), within(t, 26, a, half), within(t, 26, b, col)
    return row, half, col


def slot_offset(d):
    return jnp.where(d == 0, 0, jnp.where(d == 1, 3, d - 1))


UNITS = 34
HOME = 1
REACH = 4
LAG = 3


def sketch_kernel(
    nz,
    omega_ref,
    basis_ref,
    vec_ref,
    s_ref,
    p_ref,
    obuf,
    bbuf,
    part,
    dbuf,
    rbuf,
    fbuf,
    l_sem,
    o_send,
    o_recv,
    b_send,
    b_recv,
    d_send,
    d_recv,
    r_send,
    r_recv,
    f_send,
    f_recv,
    p_send,
    p_recv,
):
    s, r = lax.axis_index("section"), lax.axis_index("row")
    y, x = lax.div(s, 4), lax.rem(s, 4)
    z, c = lax.div(r, 2), lax.rem(r, 2)

    def at(dy, dx):
        return lax.rem(y + dy, 4) * 4 + lax.rem(x + dx, 4)

    beside = (lax.rem(z + 1, nz) * 2 + c, lax.rem(z + nz - 1, nz) * 2 + c)
    mate = z * 2 + (1 - c)

    local = [
        pltpu.make_async_copy(omega_ref, obuf.at[0], l_sem.at[0]),
        pltpu.make_async_copy(basis_ref, bbuf.at[0], l_sem.at[1]),
    ]
    for cp in local:
        cp.start()

    barrier = pltpu.get_barrier_semaphore()
    ns, nr = 16, 2 * nz

    def hello(section, row):
        pl.semaphore_signal(barrier, inc=1, device_id=(section, row), device_id_type=MESH)

    for q in range(nr):
        for other in next_of(s, ns):
            hello(other, q)
    for step in range(1, nr):
        hello(s, lax.rem(r + step, nr))
    for step in range(1, ns):
        hello(lax.rem(s + step, ns), r)

    v = vec_ref[...].astype(F32)
    v = jnp.concatenate([v, jnp.zeros_like(v)], axis=0)
    v = jnp.concatenate([v, jnp.zeros((120, v.shape[1]), F32)], axis=0)
    bbuf[4, :, :128] = v.T.astype(BF16)
    bbuf[4, :, 128:] = jnp.zeros((v.shape[1], bbuf.shape[2] - 128), BF16)
    for cp in local:
        cp.wait()
    pl.semaphore_wait(barrier, 3 * nr + ns - 2)

    def ocopy(src, dst, half, sem, dy):
        return remote(obuf.at[src, half], obuf.at[dst, half], o_send.at[sem], o_recv.at[sem], at(dy, 0), r)

    def bcopy(src, dst, half, sem, dx):
        a, b = bbuf.at[src], bbuf.at[dst]
        if half is not None:
            a, b = a.at[pl.ds(512 * half, 512)], b.at[pl.ds(512 * half, 512)]
        return remote(a, b, b_send.at[sem], b_recv.at[sem], at(0, dx), r)

    b_own = [bcopy(0, 1, None, 0, 1), bcopy(0, 2, None, 1, 3)]
    o_own = [ocopy(0, 1, 0, 0, 1), ocopy(0, 2, 1, 1, 3)]
    o_rest = [ocopy(0, 1, 1, 2, 1), ocopy(0, 2, 0, 3, 3)]
    b_fwd = [bcopy(1, 3, 0, 2, 1), bcopy(2, 3, 1, 3, 3)]
    o_fwd = [ocopy(1, 3, 0, 4, 1), ocopy(2, 3, 1, 5, 3)]
    for cp in o_own + b_own + o_rest:
        cp.start()

    def dcopy(u):
        return remote(part.at[u, :, 1 - c], dbuf.at[u], d_send.at[u], d_recv.at[u], s, mate)

    def chunk(d, k):
        far = REACH - k
        return lax.rem(z + (far if d == 0 else nz - far), nz)

    def rcopy(u, d, k):
        return remote(
            part.at[u, chunk(d, k), c],
            rbuf.at[u, d, k],
            r_send.at[u, d, k],
            r_recv.at[u, d, k],
            s,
            beside[d],
        )

    def place(u):
        row, half, col = unit(u)
        dy, dx = slot_offset(row), slot_offset(col)
        start = (lax.rem(y + dy, 4) * 4 + x) * 32 + half * 16
        return dx, pl.ds(pl.multiple_of(start, 16), 16)

    def fcopy(u):
        dx, rows = place(u)
        return remote(fbuf.at[u], s_ref.at[rows], f_send.at[u], f_recv.at[u], at(0, dx), r)

    def pcopy(u, sender):
        return remote(fbuf.at[u], p_ref.at[sender, u], p_send.at[u], p_recv.at[sender, u], HOME, r)

    def step(t, carry):
        done = t - 2 - LAG * REACH

        @pl.when((done >= 0) & (done < UNITS))
        def _():
            rcopy(done, 0, REACH - 1).wait_recv()
            rcopy(done, 1, REACH - 1).wait_recv()
            fbuf[done] = (part[done, z, c] + dbuf[done, z]) + (
                rbuf[done, 0, REACH - 1] + rbuf[done, 1, REACH - 1]
            )

        @pl.when((done >= 2) & (done < UNITS))
        def _():
            dx, rows = place(done)

            @pl.when(dx == 0)
            def _():
                s_ref[rows, :] = fbuf[done]

            @pl.when(dx > 0)
            def _():
                fcopy(done).start()

        @pl.when((done >= 0) & (done < 2))
        def _():
            @pl.when(s == HOME)
            def _():
                p_ref[HOME, done] = fbuf[done]

            @pl.when(s != HOME)
            def _():
                pcopy(done, s).start()

        for k in range(REACH - 1, -1, -1):
            u = t - 2 - LAG * k
            valid = (u >= 0) & (u < UNITS)
            if k == 0:

                @pl.when(valid)
                def _():
                    dcopy(u).wait_recv()

            for d in range(2):
                longer = lax.rem(jnp.maximum(u, 0), 2) == d

                def own():
                    return part[u, chunk(d, k), c] + dbuf[u, chunk(d, k)]

                def send(val):
                    part[u, chunk(d, k), c] = val
                    rcopy(u, d, k).start()

                def pass_on():
                    rcopy(u, d, k - 1).wait_recv()
                    send(own() + rbuf[u, d, k - 1])

                if k == 0:

                    @pl.when(valid & longer)
                    def _():
                        send(own())

                elif k == 1:

                    @pl.when(valid & longer)
                    def _():
                        pass_on()

                    @pl.when(valid & jnp.logical_not(longer))
                    def _():
                        send(own())

                else:

                    @pl.when(valid)
                    def _():
                        pass_on()

        @pl.when(t == 4)
        def _():
            for cp in b_own:
                cp.wait_recv()
            for cp in b_fwd:
                cp.start()

        @pl.when(t == 8)
        def _():
            for cp in o_own:
                cp.wait_recv()
            for cp in o_fwd:
                cp.start()

        @pl.when(t == 14)
        def _():
            for cp in b_fwd:
                cp.wait_recv()

        @pl.when(t == 18)
        def _():
            for cp in o_rest:
                cp.wait_recv()

        @pl.when(t == 26)
        def _():
            for cp in o_fwd:
                cp.wait_recv()

        @pl.when(t < UNITS)
        def _():
            row, half, col = unit(t)
            out = jnp.dot(obuf[row, half], bbuf[col], preferred_element_type=F32)
            part[t] = out.reshape(part.shape[1:])
            dcopy(t).start()

        return carry

    lax.fori_loop(0, UNITS + 2 + LAG * REACH + 1, step, 0)

    def finish(u, carry):
        dx, _ = place(u)

        @pl.when(dx > 0)
        def _():
            fcopy(u).wait_recv()

        return carry

    lax.fori_loop(2, UNITS, finish, 0)

    @pl.when(s == HOME)
    def _():
        for t in range(16):
            if t != HOME:
                for u in range(2):
                    pcopy(u, t).wait_recv()

    def drain(u, carry):
        dcopy(u).wait_send()
        dx, _ = place(u)

        @pl.when((u >= 2) & (dx > 0))
        def _():
            fcopy(u).wait_send()

        for d in range(2):
            for k in range(REACH):
                if k:
                    rcopy(u, d, k).wait_send()
                else:

                    @pl.when(lax.rem(u, 2) == d)
                    def _():
                        rcopy(u, d, k).wait_send()

        return carry

    def close():
        @pl.when(s != HOME)
        def _():
            for u in range(2):
                pcopy(u, s).wait_send()

        for cp in b_own + o_own + o_rest + b_fwd + o_fwd:
            cp.wait_send()
        lax.fori_loop(0, UNITS, drain, 0)

    return close


def sketch_scratch(m, k, n, nr):
    nz, piece, dma = nr // 2, m // nr // 2, pltpu.SemaphoreType.DMA
    return [
        pltpu.VMEM((4, 2, m // 2, k), BF16),
        pltpu.VMEM((5, k, n), BF16),
        pltpu.VMEM((UNITS, nz, 2, piece, n), F32),
        pltpu.VMEM((UNITS, nz, piece, n), F32),
        pltpu.VMEM((UNITS, 2, REACH, piece, n), F32),
        pltpu.VMEM((UNITS, piece, n), F32),
        dma((2,)),
        dma((6,)),
        dma((6,)),
        dma((4,)),
        dma((4,)),
        dma((UNITS,)),
        dma((UNITS,)),
        dma((UNITS, 2, REACH)),
        dma((UNITS, 2, REACH)),
        dma((UNITS,)),
        dma((UNITS,)),
        dma((2,)),
        dma((16, 2)),
    ]


def pair_scratch(n, nr):
    dma = pltpu.SemaphoreType.DMA
    return [
        pltpu.VMEM((2, n, n), F32),
        pltpu.VMEM((2, nr, n // nr, n), F32),
        pltpu.VMEM((2, n // nr, n), F32),
        pltpu.VMEM((2, n, n), F32),
        pltpu.VMEM((n, n), F32),
        pltpu.VMEM((2, n // 2, n // 2), F32),
        pltpu.VMEM((n // 2, n // 2), F32),
        pltpu.VMEM((2, n // 2, n // 2), F32),
        pltpu.VMEM((n // 2, n // 2), F32),
        dma((3,)),
        dma((3,)),
        dma((2, nr)),
        dma((2, nr)),
        dma((2, nr)),
        dma((2, nr)),
        dma((2,)),
        dma((2,)),
    ]


def chain_scratch(k, n, ns, nr):
    dma = pltpu.SemaphoreType.DMA
    return [
        pltpu.VMEM((n, n), BF16),
        pltpu.VMEM((n, n), BF16),
        pltpu.VMEM((8, n // 2), F32),
        pltpu.VMEM((8, n // 2), F32),
        pltpu.VMEM((8, k), F32),
        pltpu.VMEM((8, k), F32),
        pltpu.VMEM((8, 128), F32),
        pltpu.VMEM((nr, 8, 128), F32),
        pltpu.VMEM((ns // 2, 8, 128), F32),
        pltpu.VMEM((ns, 8, 128), F32),
        pltpu.VMEM((8, 128), F32),
        pltpu.VMEM((nr, 8, 128), F32),
        pltpu.VMEM((8, 128), F32),
        pltpu.VMEM((8, 128), F32),
        dma((nr,)),
        dma((nr,)),
        dma,
        dma,
        dma((ns,)),
        dma((ns,)),
        dma((nr,)),
        dma((nr,)),
        dma((ns,)),
        dma,
        dma,
        dma,
        pltpu.VMEM((2, 8, 128), F32),
        pltpu.VMEM((2, 8, 128), F32),
        dma((2,)),
        dma((2,)),
    ]


def whole_kernel(ns, nr, ends, omega_ref, basis_ref, vec_ref, ortho_ref, coef_ref, *rest):
    s_ref, p_ref, pair_ref, ahead_ref, uinv_ref, cross_ref = rest[:6]
    first, second = rest[6 : ends[0]], rest[ends[0] : ends[1]]
    third = rest[ends[1] :]
    close = sketch_kernel(nr // 2, omega_ref, basis_ref, vec_ref, s_ref, p_ref, *first)

    def start_chain():
        first_products(nr, pair_ref, p_ref, third)

    pair_kernel(
        ns, nr, close, start_chain, s_ref, pair_ref, ahead_ref, uinv_ref, cross_ref, *second
    )
    own_basis = first[1].at[0]
    chain_kernel(
        ns,
        nr,
        pair_ref,
        ahead_ref,
        uinv_ref,
        cross_ref,
        own_basis,
        vec_ref,
        ortho_ref,
        coef_ref,
        *third,
    )


def whole_call(omega, basis, vectors, ns, nr):
    vm = pl.BlockSpec(memory_space=pltpu.VMEM)
    anym = pl.BlockSpec(memory_space=pl.ANY)
    m, k = omega.shape
    n = basis.shape[1]
    kept = [
        pltpu.VMEM((m, n), F32),
        pltpu.VMEM((ns, 2, m // nr // 2, n), F32),
        pltpu.VMEM((m, 2 * n), F32),
        pltpu.VMEM((m, 2 * n), F32),
        pltpu.VMEM((2 * n, 2 * n), F32),
        pltpu.VMEM((2 * n, 2 * n), F32),
    ]
    one = sketch_scratch(m, k, n, nr)
    two = pair_scratch(n, nr)
    three = chain_scratch(m, 2 * n, ns, nr)
    ends = (len(kept) + len(one), len(kept) + len(one) + len(two))
    return pl.pallas_call(
        functools.partial(whole_kernel, ns, nr, ends),
        out_shape=(
            jax.ShapeDtypeStruct((4, vectors.shape[1] // ns), F32),
            jax.ShapeDtypeStruct((4, n), F32),
        ),
        in_specs=[anym, anym, vm],
        out_specs=(vm, vm),
        scratch_shapes=kept + one + two + three,
        compiler_params=pltpu.CompilerParams(
            collective_id=0, has_side_effects=True, vmem_limit_bytes=60 * 1024 * 1024
        ),
    )(omega.reshape(2, m // 2, k), basis, vectors)


def body(omega, basis, vectors):
    return whole_call(omega, basis, vectors, lax.axis_size("section"), lax.axis_size("row"))


def solution(mesh):
    placed = (P("section", "row"), P("row", "section"), P(None, "row"))
    return jax.shard_map(
        body,
        mesh=mesh,
        in_specs=placed,
        out_specs=(P(None, ("row", "section")), P(None, "section")),
        check_vma=False,
    )
```

```python
import functools

import jax
import jax.numpy as jnp
from jax import lax
from jax.experimental import pallas as pl
from jax.experimental.pallas import tpu as pltpu
from jax.sharding import PartitionSpec as P

F32 = jnp.float32
BF16 = jnp.bfloat16
HI = lax.Precision.HIGHEST
MESH = pl.DeviceIdType.MESH


def split(x):
    hi = x.astype(BF16)
    return hi, (x - hi.astype(F32)).astype(BF16)


def dot3(a, b, dims):
    (ah, al), (bh, bl) = a, b

    def one(x, y):
        return lax.dot_general(x, y, (dims, ((), ())), preferred_element_type=F32)

    return one(ah, bh) + (one(al, bh) + one(ah, bl))


NN = ((1,), (0,))
NT = ((1,), (1,))
TN = ((0,), (0,))


def remote(src, dst, send, recv, section, row):
    return pltpu.make_async_remote_copy(
        src_ref=src,
        dst_ref=dst,
        send_sem=send,
        recv_sem=recv,
        device_id=(section, row),
        device_id_type=MESH,
    )


def packed(c):
    half = c.shape[1] // 2
    return jnp.concatenate([c[:4, :half], c[:4, half:]], axis=0)


def unpacked(c):
    wide = jnp.concatenate([c[:4], c[4:]], axis=1)
    return jnp.concatenate([wide, jnp.zeros_like(wide)], axis=0)


def combine(i, value, cout, dout, din, d_send, d_recv):
    s, r = lax.axis_index("section"), lax.axis_index("row")
    c = lax.rem(r, 2)
    first, second = value[:, :128], value[:, 128:]
    dout[i] = jnp.where(c == 0, second, first)
    swap = remote(dout.at[i], din.at[i], d_send.at[i], d_recv.at[i], s, r + 1 - 2 * c)
    swap.start()
    keep = jnp.where(c == 0, first, second)
    swap.wait_recv()
    cout[...] = keep + din[i]
    swap.wait_send()


def first_products(nr, s_ref, p0_ref, refs):
    probe, cout, cin, c_send, c_recv = refs[4], refs[6], refs[7], refs[14], refs[15]
    r = lax.axis_index("row")
    rows, n = s_ref.shape
    p = p0_ref[...].reshape(rows, n // 2)[:, :128].T[:8]
    probe[...] = p
    combine(0, packed(dot3(split(p), split(s_ref[...]), NN)), cout, *refs[-4:])
    for step in range(1, nr):
        remote(cout, cin.at[r], c_send.at[step], c_recv.at[r], FIRST, lax.rem(r + step, nr)).start()
    cin[pl.ds(r, 1)] = cout[...][None]


def chain_kernel(
    ns,
    nr,
    s_ref,
    next_ref,
    inv_ref,
    cross_ref,
    basis_ref,
    vec_ref,
    ortho_ref,
    coef_ref,
    hi_ref,
    lo_ref,
    kept,
    low_part,
    probe,
    moved,
    cout,
    cin,
    own,
    oin,
    sout,
    sin,
    bout,
    bin_,
    c_send,
    c_recv,
    p_send,
    p_recv,
    o_send,
    o_recv,
    s_send,
    s_recv,
    b_send,
    b_recv,
    k_send,
    k_recv,
    dout,
    din,
    d_send,
    d_recv,
):
    s, r = lax.axis_index("section"), lax.axis_index("row")
    n = kept.shape[1]
    on = active(s)
    off = jnp.logical_not(on)
    odd = lax.rem(s, 2) == 1
    mate = mate_of(s)
    after, before = next_of(s, ns)

    pass_coef = remote(low_part, kept, k_send, k_recv, mate, r)

    @pl.when(on)
    def _():
        sp = split(s_ref[...])
        nx = split(next_ref[...])
        iv = split(inv_ref[...])

        hi_ref[...], lo_ref[...] = split(dot3(iv, split(cross_ref[...]), NN))

        @pl.when(s == FIRST)
        def _():
            for step in range(1, nr):
                peer = lax.rem(r + step, nr)
                remote(cout, cin.at[peer], c_send.at[step], c_recv.at[peer], FIRST, peer).wait()

        @pl.when(s != FIRST)
        def _():
            remote(moved, probe, p_send, p_recv, before, r).wait_recv()

        p = probe[...]
        ahead = dot3(split(p), nx, NN)

        @pl.when(s != FIRST)
        def _():
            for q in range(nr):
                remote(cout, cin.at[q], c_send.at[q], c_recv.at[q], before, q).wait_recv()

        sums = [cin[0], cin[1]]
        for q in range(2, nr):
            sums[q % 2] = sums[q % 2] + cin[q]
        inner = split(unpacked(jnp.concatenate(sums, axis=1)))

        @pl.when(s != LAST)
        def _():
            partial = packed(ahead - dot3(inner, (hi_ref[...], lo_ref[...]), NN))
            combine(1, partial, cout, dout, din, d_send, d_recv)
            for q in range(nr):
                remote(cout, cin.at[r], c_send.at[q], c_recv.at[r], after, q).start()

        coef = dot3(inner, iv, NN)
        low_part[...] = jnp.where(odd, coef[:, :n], coef[:, n:])
        kept[...] = jnp.where(odd, coef[:, n:], coef[:, :n])
        moved[...] = p - dot3(split(coef), sp, NT)

        @pl.when(s != LAST)
        def _():
            remote(moved, probe, p_send, p_recv, after, r).start()

        pass_coef.start()

    @pl.when(off)
    def _():
        pass_coef.wait_recv()

    coef = kept[...]
    coef_ref[...] = coef[:4]
    term = lax.dot_general(coef.astype(BF16), basis_ref[...], (NT, ((), ())), preferred_element_type=F32)
    for k in range(ns // 2):
        own[k] = term[:, k * 128 : (k + 1) * 128]
    outs = []
    for step in range(1, ns):
        t = lax.rem(s + step, ns)
        cp = remote(own.at[lax.div(t, 2)], oin.at[s], o_send.at[step], o_recv.at[s], t, r)
        cp.start()
        outs.append(cp)
    oin[pl.ds(s, 1)] = own[pl.ds(lax.div(s, 2), 1)]

    @pl.when(s == LAST)
    def _():
        m = split(moved[...])
        sq = dot3(m, m, NT)
        sout[...] = jnp.concatenate([sq, jnp.zeros((8, 120), F32)], axis=1)
        copies = []
        for step in range(1, nr):
            peer = lax.rem(r + step, nr)
            cp = remote(sout, sin.at[r], s_send.at[step], s_recv.at[r], s, peer)
            cp.start()
            copies.append(cp)
        sin[pl.ds(r, 1)] = sout[...][None]
        for step in range(1, nr):
            peer = lax.rem(r + step, nr)
            remote(sout, sin.at[peer], s_send.at[step], s_recv.at[peer], s, peer).wait_recv()
        tot = sin[0]
        for q in range(1, nr):
            tot = tot + sin[q]
        bout[...] = tot
        bcs = []
        for t in range(ns):
            if t != LAST:
                cp = remote(bout, bin_, b_send.at[t], b_recv, t, r)
                cp.start()
                bcs.append(cp)
        for cp in copies + bcs:
            cp.wait_send()
        bin_[...] = tot

    for step in range(1, ns):
        t = lax.rem(s + step, ns)
        remote(own.at[0], oin.at[t], o_send.at[step], o_recv.at[t], t, r).wait_recv()
    removed = oin[0]
    for t in range(1, ns):
        removed = removed + oin[t]
    window = pl.ds(pl.multiple_of(lax.div(s, 2) * 128, 128), 128)
    remain = vec_ref[:, window].astype(F32) - removed[:4]
    remain = jnp.where(odd, remain[:, 64:], remain[:, :64])

    @pl.when(s != LAST)
    def _():
        remote(bout, bin_, b_send.at[0], b_recv, LAST, r).wait_recv()

    @pl.when(on & (s != LAST))
    def _():
        for q in range(nr):
            remote(cout, cin.at[q], c_send.at[q], c_recv.at[q], after, q).wait_send()
        remote(moved, probe, p_send, p_recv, after, r).wait_send()

    @pl.when(on)
    def _():
        pass_coef.wait_send()

    small = bin_[...]

    def at(i, k):
        return small[i : i + 1, k : k + 1]

    low = [[None] * 4 for _ in range(4)]
    rows = []
    for i in range(4):
        for k in range(i + 1):
            v = at(i, k)
            for m in range(k):
                v = v - low[i][m] * low[k][m]
            low[i][k] = jnp.sqrt(v) if i == k else v / low[k][k]
        x = remain[i : i + 1]
        for k in range(i):
            x = x - low[i][k] * rows[k]
        rows.append(x / low[i][i])
    ortho_ref[...] = jnp.concatenate(rows, axis=0)
    for cp in outs:
        cp.wait_send()


def eliminate(a):
    n = a.shape[0]
    cols = lax.broadcasted_iota(jnp.int32, (n, n), 1)
    lane = lax.broadcasted_iota(jnp.int32, (1, n), 1)
    sub = lax.broadcasted_iota(jnp.int32, (8, n), 0)
    for k in range(0, n, 4):
        c = [jnp.broadcast_to(a[:, k + i : k + i + 1], (n, n)) for i in range(4)]
        b = [[c[j][k + i : k + i + 1] for j in range(4)] for i in range(4)]
        inside = (lane >= k) & (lane < k + 4)
        r = [
            jnp.where(lane == k + i, 1.0, jnp.where(inside, 0.0, a[k + i : k + i + 1, :])) for i in range(4)
        ]
        e = 1.0 / (b[0][0] * b[1][1] - b[0][1] * b[0][1])
        a00, a01, a11 = b[1][1] * e, -b[0][1] * e, b[0][0] * e
        f00 = a00 * b[0][2] + a01 * b[1][2]
        f01 = a00 * b[0][3] + a01 * b[1][3]
        f10 = a01 * b[0][2] + a11 * b[1][2]
        f11 = a01 * b[0][3] + a11 * b[1][3]
        s00 = b[2][2] - (b[0][2] * f00 + b[1][2] * f10)
        s01 = b[2][3] - (b[0][2] * f01 + b[1][2] * f11)
        s11 = b[3][3] - (b[0][3] * f01 + b[1][3] * f11)
        g = 1.0 / (s00 * s11 - s01 * s01)
        z2 = r[2] - (f00 * r[0] + f10 * r[1])
        z3 = r[3] - (f01 * r[0] + f11 * r[1])
        w2 = g * (s11 * z2 - s01 * z3)
        w3 = g * (s00 * z3 - s01 * z2)
        w0 = (a00 * r[0] + a01 * r[1]) - (f00 * w2 + f01 * w3)
        w1 = (a01 * r[0] + a11 * r[1]) - (f10 * w2 + f11 * w3)
        base = jnp.where((cols >= k) & (cols < k + 4), 0.0, a)
        new = ((base - c[0] * w0) - c[1] * w1) - (c[2] * w2 + c[3] * w3)
        at = k // 8 * 8
        group = new[at : at + 8]
        for i, w in enumerate((w0, w1, w2, w3)):
            group = jnp.where(sub == k - at + i, jnp.broadcast_to(w, (8, n)), group)
        pieces = [new[:at], group, new[at + 8 :]]
        a = jnp.concatenate([p for p in pieces if p.shape[0]], axis=0)
    return a


FIRST, LAST = 1, 14


def active(s):
    x = lax.rem(s, 4)
    return (x == 1) | (x == 2)


def mate_of(s):
    return s + 1 - 2 * lax.rem(s, 2)


def next_of(s, ns):
    odd = lax.rem(s, 2) == 1
    return lax.rem(s + jnp.where(odd, 1, 3), ns), lax.rem(s + ns - jnp.where(odd, 3, 1), ns)


def pair_kernel(
    ns,
    nr,
    close,
    start_chain,
    s_ref,
    pair_ref,
    ahead_ref,
    uinv_ref,
    cross_ref,
    part,
    got,
    red,
    full,
    inv,
    early,
    late,
    mate_early,
    mate_late,
    n_send,
    n_recv,
    rs_send,
    rs_recv,
    ag_send,
    ag_recv,
    i_send,
    i_recv,
):
    s, r = lax.axis_index("section"), lax.axis_index("row")
    n = s_ref.shape[1]
    rows = n // nr
    on = active(s)
    off = jnp.logical_not(on)
    odd = lax.rem(s, 2) == 1
    even = lax.rem(s, 2) == 0
    mate = mate_of(s)
    low, high = pl.ds(0, n), pl.ds(n, n)
    x = lax.rem(s, 4)
    back = jnp.where(x == 1, 3, jnp.where(x == 2, 1, 2))
    last = lax.rem(s + ns - back, ns)
    to_mate = [
        remote(s_ref, pair_ref.at[:, where], n_send.at[0], n_recv.at[0], mate, r) for where in (low, high)
    ]
    to_last = [
        remote(s_ref, ahead_ref.at[:, where], n_send.at[1], n_recv.at[1 + k], last, r)
        for k, where in enumerate((low, high))
    ]

    def span(peer):
        return pl.ds(pl.multiple_of(peer * rows, rows), rows)

    def scatter(i, step):
        peer = lax.rem(r + step, nr)
        return remote(
            part.at[i, span(peer)], got.at[i, step], rs_send.at[i, step], rs_recv.at[i, step], s, peer
        )

    def gather(i, step, sending):
        peer = lax.rem(r + (step if sending else nr - step), nr)
        where = span(r if sending else peer)
        return remote(red.at[i], full.at[i, where], ag_send.at[i, step], ag_recv.at[i, step], s, peer)

    def begin(i):
        for step in range(1, nr):
            scatter(i, step).start()

    def middle(i):
        for step in range(1, nr):
            scatter(i, step).wait_recv()
        total = part[i, span(r), :]
        for step in range(1, nr):
            total = total + got[i, step]
        red[i] = total
        for step in range(1, nr):
            gather(i, step, True).start()
        full[i, span(r), :] = total

    def end(i):
        for step in range(1, nr):
            gather(i, step, False).wait_recv()
        for step in range(1, nr):
            scatter(i, step).wait_send()
            gather(i, step, True).wait_send()

    sp = split(s_ref[...])
    part[0] = dot3(sp, sp, TN)
    begin(0)
    close()

    for k, mine in enumerate((even, odd)):

        @pl.when(mine & off)
        def _():
            to_mate[k].start()

        @pl.when(mine & (s >= 2))
        def _():
            to_last[k].start()

        @pl.when(mine)
        def _():
            pair_ref[:, k * n : (k + 1) * n] = s_ref[...]

    middle(0)

    for k, mine in enumerate((even, odd)):

        @pl.when(mine & on)
        def _():
            to_mate[1 - k].wait_recv()

    @pl.when(on)
    def _():
        part[1] = dot3(split(pair_ref[:, :n]), split(pair_ref[:, n:]), TN)
        begin(1)

    end(0)

    def dot(x, y, dims):
        return lax.dot_general(x, y, (dims, ((), ())), precision=HI, preferred_element_type=F32)

    g = full[0]
    h = n // 2
    eye = lax.broadcasted_iota(jnp.int32, (n, n), 0) == lax.broadcasted_iota(jnp.int32, (n, n), 1)
    d = jnp.where(eye, g, 0.0)
    rs = lax.rsqrt(jnp.sum(d, axis=1, keepdims=True))
    cs = lax.rsqrt(jnp.sum(d, axis=0, keepdims=True))
    g = g * rs * cs
    a, b, c = g[:h, :h], g[:h, h:], g[h:, h:]
    ai = eliminate(a)
    t = dot(ai, b, NN)
    rest = c - dot(b, t, TN)
    early[0] = ai * rs[:h] * cs[:, :h]
    early[1] = t * rs[:h] / cs[:, h:]
    pass_early = remote(early, mate_early, i_send.at[0], i_recv.at[0], mate, r)
    pass_late = remote(late, mate_late, i_send.at[1], i_recv.at[1], mate, r)

    @pl.when(off)
    def _():
        pass_early.start()

    @pl.when(on)
    def _():
        middle(1)

    @pl.when(s == FIRST)
    def _():
        start_chain()

    late[...] = eliminate(rest) * rs[h:] * cs[:, h:]

    @pl.when(off)
    def _():
        pass_late.start()

    def whole_inverse(parts, corner):
        t, ci = parts[1], corner[...]
        u = dot(t, ci, NN)
        top = jnp.concatenate([parts[0] + dot(u, t, NT), -u], axis=1)
        bottom = jnp.concatenate([-u.T, ci], axis=1)
        return jnp.concatenate([top, bottom], axis=0)

    @pl.when(on)
    def _():
        inv[...] = whole_inverse(early, late)
        uinv_ref[n:, :n] = jnp.zeros((n, n), F32)

    @pl.when(on & (s != LAST))
    def _():
        for cp in to_last:
            cp.wait_recv()

    @pl.when(s == LAST)
    def _():
        ahead_ref[...] = jnp.zeros(ahead_ref.shape, F32)

    @pl.when(on)
    def _():
        cross_ref[...] = dot3(split(pair_ref[...]), split(ahead_ref[...]), TN)
        end(1)
        pass_early.wait_recv()
        pass_late.wait_recv()

    @pl.when(on & odd)
    def _():
        mine, theirs = inv[...], whole_inverse(mate_early, mate_late)
        right = dot3(split(full[1]), split(mine), NN)
        uinv_ref[n:, n:] = mine
        uinv_ref[:n, :n] = theirs
        uinv_ref[:n, n:] = -dot3(split(theirs), split(right), NN)

    @pl.when(on & even)
    def _():
        mine, theirs = inv[...], whole_inverse(mate_early, mate_late)
        left = dot3(split(mine), split(full[1]), NN)
        uinv_ref[:n, :n] = mine
        uinv_ref[n:, n:] = theirs
        uinv_ref[:n, n:] = -dot3(split(left), split(theirs), NN)

    @pl.when(off)
    def _():
        pass_early.wait_send()
        pass_late.wait_send()
        to_mate[0].wait_send()

    @pl.when(s >= 2)
    def _():
        to_last[0].wait_send()


def within(t, first, yes, no):
    return jnp.where(t >= first, yes, no)


def unit(t):
    def seg(first, width):
        return lax.div(jnp.maximum(t - first, 0), width), lax.rem(jnp.maximum(t - first, 0), width)

    a, b = seg(4, 2)
    row, half, col = within(t, 2, 0, 0), lax.rem(t, 2), within(t, 2, 0, 4)
    row, half, col = row, within(t, 4, b, half), within(t, 4, 1 + a, col)
    a, b = seg(8, 3)
    row, half, col = within(t, 8, 1 + a, row), within(t, 8, a, half), within(t, 8, b, col)
    row, half, col = within(t, 14, 0, row), within(t, 14, t - 14, half), within(t, 14, 3, col)
    row, half, col = within(t, 16, t - 15, row), within(t, 16, t - 16, half), within(t, 16, 3, col)
    a, b = seg(18, 4)
    row, half, col = within(t, 18, 1 + a, row), within(t, 18, 1 - a, half), within(t, 18, b, col)
    a, b = seg(26, 4)
    row, half, col = within(t, 26, 3, row), within(t, 26, a, half), within(t, 26, b, col)
    return row, half, col


def slot_offset(d):
    return jnp.where(d == 0, 0, jnp.where(d == 1, 3, d - 1))


UNITS = 34
HOME = 1
REACH = 4
LAG = 4


def sketch_kernel(
    nz,
    omega_ref,
    basis_ref,
    vec_ref,
    s_ref,
    p_ref,
    obuf,
    bbuf,
    part,
    dbuf,
    rbuf,
    fbuf,
    l_sem,
    o_send,
    o_recv,
    b_send,
    b_recv,
    d_send,
    d_recv,
    r_send,
    r_recv,
    f_send,
    f_recv,
    p_send,
    p_recv,
):
    s, r = lax.axis_index("section"), lax.axis_index("row")
    y, x = lax.div(s, 4), lax.rem(s, 4)
    z, c = lax.div(r, 2), lax.rem(r, 2)

    def at(dy, dx):
        return lax.rem(y + dy, 4) * 4 + lax.rem(x + dx, 4)

    beside = (lax.rem(z + 1, nz) * 2 + c, lax.rem(z + nz - 1, nz) * 2 + c)
    mate = z * 2 + (1 - c)

    local = [
        pltpu.make_async_copy(omega_ref, obuf.at[0], l_sem.at[0]),
        pltpu.make_async_copy(basis_ref, bbuf.at[0], l_sem.at[1]),
    ]
    for cp in local:
        cp.start()

    barrier = pltpu.get_barrier_semaphore()
    ns, nr = 16, 2 * nz

    def hello(section, row):
        pl.semaphore_signal(barrier, inc=1, device_id=(section, row), device_id_type=MESH)

    for q in range(nr):
        for other in next_of(s, ns):
            hello(other, q)
    for step in range(1, nr):
        hello(s, lax.rem(r + step, nr))
    for step in range(1, ns):
        hello(lax.rem(s + step, ns), r)

    v = vec_ref[...].astype(F32)
    v = jnp.concatenate([v, jnp.zeros_like(v)], axis=0)
    v = jnp.concatenate([v, jnp.zeros((120, v.shape[1]), F32)], axis=0)
    bbuf[4, :, :128] = v.T.astype(BF16)
    bbuf[4, :, 128:] = jnp.zeros((v.shape[1], bbuf.shape[2] - 128), BF16)
    for cp in local:
        cp.wait()
    pl.semaphore_wait(barrier, 3 * nr + ns - 2)

    def ocopy(src, dst, half, sem, dy):
        return remote(obuf.at[src, half], obuf.at[dst, half], o_send.at[sem], o_recv.at[sem], at(dy, 0), r)

    def bcopy(src, dst, half, sem, dx):
        a, b = bbuf.at[src], bbuf.at[dst]
        if half is not None:
            a, b = a.at[pl.ds(512 * half, 512)], b.at[pl.ds(512 * half, 512)]
        return remote(a, b, b_send.at[sem], b_recv.at[sem], at(0, dx), r)

    b_own = [bcopy(0, 1, None, 0, 1), bcopy(0, 2, None, 1, 3)]
    o_own = [ocopy(0, 1, 0, 0, 1), ocopy(0, 2, 1, 1, 3)]
    o_rest = [ocopy(0, 1, 1, 2, 1), ocopy(0, 2, 0, 3, 3)]
    b_fwd = [bcopy(1, 3, 0, 2, 1), bcopy(2, 3, 1, 3, 3)]
    o_fwd = [ocopy(1, 3, 0, 4, 1), ocopy(2, 3, 1, 5, 3)]
    for cp in o_own + b_own + o_rest:
        cp.start()

    def dcopy(u):
        return remote(part.at[u, :, 1 - c], dbuf.at[u], d_send.at[u], d_recv.at[u], s, mate)

    def chunk(d, k):
        far = REACH - k
        return lax.rem(z + (far if d == 0 else nz - far), nz)

    def rcopy(u, d, k):
        return remote(
            part.at[u, chunk(d, k), c],
            rbuf.at[u, d, k],
            r_send.at[u, d, k],
            r_recv.at[u, d, k],
            s,
            beside[d],
        )

    def place(u):
        row, half, col = unit(u)
        dy, dx = slot_offset(row), slot_offset(col)
        start = (lax.rem(y + dy, 4) * 4 + x) * 32 + half * 16
        return dx, pl.ds(pl.multiple_of(start, 16), 16)

    def fcopy(u):
        dx, rows = place(u)
        return remote(fbuf.at[u], s_ref.at[rows], f_send.at[u], f_recv.at[u], at(0, dx), r)

    def pcopy(u, sender):
        return remote(fbuf.at[u], p_ref.at[sender, u], p_send.at[u], p_recv.at[sender, u], HOME, r)

    def step(t, carry):
        done = t - 2 - LAG * REACH

        @pl.when((done >= 0) & (done < UNITS))
        def _():
            rcopy(done, 0, REACH - 1).wait_recv()
            rcopy(done, 1, REACH - 1).wait_recv()
            fbuf[done] = (part[done, z, c] + dbuf[done, z]) + (
                rbuf[done, 0, REACH - 1] + rbuf[done, 1, REACH - 1]
            )

        @pl.when((done >= 2) & (done < UNITS))
        def _():
            dx, rows = place(done)

            @pl.when(dx == 0)
            def _():
                s_ref[rows, :] = fbuf[done]

            @pl.when(dx > 0)
            def _():
                fcopy(done).start()

        @pl.when((done >= 0) & (done < 2))
        def _():
            @pl.when(s == HOME)
            def _():
                p_ref[HOME, done] = fbuf[done]

            @pl.when(s != HOME)
            def _():
                pcopy(done, s).start()

        for k in range(REACH - 1, -1, -1):
            u = t - 2 - LAG * k
            valid = (u >= 0) & (u < UNITS)
            if k == 0:

                @pl.when(valid)
                def _():
                    dcopy(u).wait_recv()

            for d in range(2):
                longer = lax.rem(jnp.maximum(u, 0), 2) == d

                def own():
                    return part[u, chunk(d, k), c] + dbuf[u, chunk(d, k)]

                def send(val):
                    part[u, chunk(d, k), c] = val
                    rcopy(u, d, k).start()

                def pass_on():
                    rcopy(u, d, k - 1).wait_recv()
                    send(own() + rbuf[u, d, k - 1])

                if k == 0:

                    @pl.when(valid & longer)
                    def _():
                        send(own())

                elif k == 1:

                    @pl.when(valid & longer)
                    def _():
                        pass_on()

                    @pl.when(valid & jnp.logical_not(longer))
                    def _():
                        send(own())

                else:

                    @pl.when(valid)
                    def _():
                        pass_on()

        @pl.when(t == 4)
        def _():
            for cp in b_own:
                cp.wait_recv()
            for cp in b_fwd:
                cp.start()

        @pl.when(t == 8)
        def _():
            for cp in o_own:
                cp.wait_recv()
            for cp in o_fwd:
                cp.start()

        @pl.when(t == 14)
        def _():
            for cp in b_fwd:
                cp.wait_recv()

        @pl.when(t == 18)
        def _():
            for cp in o_rest:
                cp.wait_recv()

        @pl.when(t == 26)
        def _():
            for cp in o_fwd:
                cp.wait_recv()

        @pl.when(t < UNITS)
        def _():
            row, half, col = unit(t)
            out = jnp.dot(obuf[row, half], bbuf[col], preferred_element_type=F32)
            part[t] = out.reshape(part.shape[1:])
            dcopy(t).start()

        return carry

    lax.fori_loop(0, UNITS + 2 + LAG * REACH + 1, step, 0)

    def finish(u, carry):
        dx, _ = place(u)

        @pl.when(dx > 0)
        def _():
            fcopy(u).wait_recv()

        return carry

    lax.fori_loop(2, UNITS, finish, 0)

    @pl.when(s == HOME)
    def _():
        for t in range(16):
            if t != HOME:
                for u in range(2):
                    pcopy(u, t).wait_recv()

    def drain(u, carry):
        dcopy(u).wait_send()
        dx, _ = place(u)

        @pl.when((u >= 2) & (dx > 0))
        def _():
            fcopy(u).wait_send()

        for d in range(2):
            for k in range(REACH):
                if k:
                    rcopy(u, d, k).wait_send()
                else:

                    @pl.when(lax.rem(u, 2) == d)
                    def _():
                        rcopy(u, d, k).wait_send()

        return carry

    def close():
        @pl.when(s != HOME)
        def _():
            for u in range(2):
                pcopy(u, s).wait_send()

        for cp in b_own + o_own + o_rest + b_fwd + o_fwd:
            cp.wait_send()
        lax.fori_loop(0, UNITS, drain, 0)

    return close


def sketch_scratch(m, k, n, nr):
    nz, piece, dma = nr // 2, m // nr // 2, pltpu.SemaphoreType.DMA
    return [
        pltpu.VMEM((4, 2, m // 2, k), BF16),
        pltpu.VMEM((5, k, n), BF16),
        pltpu.VMEM((UNITS, nz, 2, piece, n), F32),
        pltpu.VMEM((UNITS, nz, piece, n), F32),
        pltpu.VMEM((UNITS, 2, REACH, piece, n), F32),
        pltpu.VMEM((UNITS, piece, n), F32),
        dma((2,)),
        dma((6,)),
        dma((6,)),
        dma((4,)),
        dma((4,)),
        dma((UNITS,)),
        dma((UNITS,)),
        dma((UNITS, 2, REACH)),
        dma((UNITS, 2, REACH)),
        dma((UNITS,)),
        dma((UNITS,)),
        dma((2,)),
        dma((16, 2)),
    ]


def pair_scratch(n, nr):
    dma = pltpu.SemaphoreType.DMA
    return [
        pltpu.VMEM((2, n, n), F32),
        pltpu.VMEM((2, nr, n // nr, n), F32),
        pltpu.VMEM((2, n // nr, n), F32),
        pltpu.VMEM((2, n, n), F32),
        pltpu.VMEM((n, n), F32),
        pltpu.VMEM((2, n // 2, n // 2), F32),
        pltpu.VMEM((n // 2, n // 2), F32),
        pltpu.VMEM((2, n // 2, n // 2), F32),
        pltpu.VMEM((n // 2, n // 2), F32),
        dma((3,)),
        dma((3,)),
        dma((2, nr)),
        dma((2, nr)),
        dma((2, nr)),
        dma((2, nr)),
        dma((2,)),
        dma((2,)),
    ]


def chain_scratch(k, n, ns, nr):
    dma = pltpu.SemaphoreType.DMA
    return [
        pltpu.VMEM((n, n), BF16),
        pltpu.VMEM((n, n), BF16),
        pltpu.VMEM((8, n // 2), F32),
        pltpu.VMEM((8, n // 2), F32),
        pltpu.VMEM((8, k), F32),
        pltpu.VMEM((8, k), F32),
        pltpu.VMEM((8, 128), F32),
        pltpu.VMEM((nr, 8, 128), F32),
        pltpu.VMEM((ns // 2, 8, 128), F32),
        pltpu.VMEM((ns, 8, 128), F32),
        pltpu.VMEM((8, 128), F32),
        pltpu.VMEM((nr, 8, 128), F32),
        pltpu.VMEM((8, 128), F32),
        pltpu.VMEM((8, 128), F32),
        dma((nr,)),
        dma((nr,)),
        dma,
        dma,
        dma((ns,)),
        dma((ns,)),
        dma((nr,)),
        dma((nr,)),
        dma((ns,)),
        dma,
        dma,
        dma,
        pltpu.VMEM((2, 8, 128), F32),
        pltpu.VMEM((2, 8, 128), F32),
        dma((2,)),
        dma((2,)),
    ]


def whole_kernel(ns, nr, ends, omega_ref, basis_ref, vec_ref, ortho_ref, coef_ref, *rest):
    s_ref, p_ref, pair_ref, ahead_ref, uinv_ref, cross_ref = rest[:6]
    first, second = rest[6 : ends[0]], rest[ends[0] : ends[1]]
    third = rest[ends[1] :]
    close = sketch_kernel(nr // 2, omega_ref, basis_ref, vec_ref, s_ref, p_ref, *first)

    def start_chain():
        first_products(nr, pair_ref, p_ref, third)

    pair_kernel(
        ns, nr, close, start_chain, s_ref, pair_ref, ahead_ref, uinv_ref, cross_ref, *second
    )
    own_basis = first[1].at[0]
    chain_kernel(
        ns,
        nr,
        pair_ref,
        ahead_ref,
        uinv_ref,
        cross_ref,
        own_basis,
        vec_ref,
        ortho_ref,
        coef_ref,
        *third,
    )


def whole_call(omega, basis, vectors, ns, nr):
    vm = pl.BlockSpec(memory_space=pltpu.VMEM)
    anym = pl.BlockSpec(memory_space=pl.ANY)
    m, k = omega.shape
    n = basis.shape[1]
    kept = [
        pltpu.VMEM((m, n), F32),
        pltpu.VMEM((ns, 2, m // nr // 2, n), F32),
        pltpu.VMEM((m, 2 * n), F32),
        pltpu.VMEM((m, 2 * n), F32),
        pltpu.VMEM((2 * n, 2 * n), F32),
        pltpu.VMEM((2 * n, 2 * n), F32),
    ]
    one = sketch_scratch(m, k, n, nr)
    two = pair_scratch(n, nr)
    three = chain_scratch(m, 2 * n, ns, nr)
    ends = (len(kept) + len(one), len(kept) + len(one) + len(two))
    return pl.pallas_call(
        functools.partial(whole_kernel, ns, nr, ends),
        out_shape=(
            jax.ShapeDtypeStruct((4, vectors.shape[1] // ns), F32),
            jax.ShapeDtypeStruct((4, n), F32),
        ),
        in_specs=[anym, anym, vm],
        out_specs=(vm, vm),
        scratch_shapes=kept + one + two + three,
        compiler_params=pltpu.CompilerParams(
            collective_id=0, has_side_effects=True, vmem_limit_bytes=60 * 1024 * 1024
        ),
    )(omega.reshape(2, m // 2, k), basis, vectors)


def body(omega, basis, vectors):
    return whole_call(omega, basis, vectors, lax.axis_size("section"), lax.axis_size("row"))


def solution(mesh):
    placed = (P("section", "row"), P("row", "section"), P(None, "row"))
    return jax.shard_map(
        body,
        mesh=mesh,
        in_specs=placed,
        out_specs=(P(None, ("row", "section")), P(None, "section")),
        check_vma=False,
    )
```

```python
import functools

import jax
import jax.numpy as jnp
from jax import lax
from jax.experimental import pallas as pl
from jax.experimental.pallas import tpu as pltpu
from jax.sharding import PartitionSpec as P

F32 = jnp.float32
BF16 = jnp.bfloat16
HI = lax.Precision.HIGHEST
MESH = pl.DeviceIdType.MESH


def split(x):
    hi = x.astype(BF16)
    return hi, (x - hi.astype(F32)).astype(BF16)


def dot3(a, b, dims):
    (ah, al), (bh, bl) = a, b

    def one(x, y):
        return lax.dot_general(x, y, (dims, ((), ())), preferred_element_type=F32)

    return one(ah, bh) + (one(al, bh) + one(ah, bl))


NN = ((1,), (0,))
NT = ((1,), (1,))
TN = ((0,), (0,))


def far_first(count):
    return sorted(range(count), key=lambda k: (-min(k, count - k), k))


def remote(src, dst, send, recv, section, row):
    return pltpu.make_async_remote_copy(
        src_ref=src,
        dst_ref=dst,
        send_sem=send,
        recv_sem=recv,
        device_id=(section, row),
        device_id_type=MESH,
    )


def packed(c):
    half = c.shape[1] // 2
    return jnp.concatenate([c[:4, :half], c[:4, half:]], axis=0)


def unpacked(c):
    wide = jnp.concatenate([c[:4], c[4:]], axis=1)
    return jnp.concatenate([wide, jnp.zeros_like(wide)], axis=0)


def combine(i, value, cout, dout, din, d_send, d_recv):
    s, r = lax.axis_index("section"), lax.axis_index("row")
    c = lax.rem(r, 2)
    first, second = value[:, :128], value[:, 128:]
    dout[i] = jnp.where(c == 0, second, first)
    swap = remote(dout.at[i], din.at[i], d_send.at[i], d_recv.at[i], s, r + 1 - 2 * c)
    swap.start()
    keep = jnp.where(c == 0, first, second)
    swap.wait_recv()
    cout[...] = keep + din[i]
    swap.wait_send()


def first_products(nr, s_ref, p0_ref, refs):
    probe, cout, cin, c_send, c_recv = refs[4], refs[6], refs[7], refs[14], refs[15]
    r = lax.axis_index("row")
    rows, n = s_ref.shape
    p = p0_ref[...].reshape(rows, n // 2)[:, :128].T[:8]
    probe[...] = p
    combine(0, packed(dot3(split(p), split(s_ref[...]), NN)), cout, *refs[-4:])
    for step in far_first(nr)[:-1]:
        remote(cout, cin.at[r], c_send.at[step], c_recv.at[r], FIRST, lax.rem(r + step, nr)).start()
    cin[pl.ds(r, 1)] = cout[...][None]


def chain_kernel(
    ns,
    nr,
    s_ref,
    next_ref,
    inv_ref,
    cross_ref,
    basis_ref,
    vec_ref,
    ortho_ref,
    coef_ref,
    hi_ref,
    lo_ref,
    kept,
    low_part,
    probe,
    moved,
    cout,
    cin,
    own,
    oin,
    sout,
    sin,
    bout,
    bin_,
    c_send,
    c_recv,
    p_send,
    p_recv,
    o_send,
    o_recv,
    s_send,
    s_recv,
    b_send,
    b_recv,
    k_send,
    k_recv,
    dout,
    din,
    d_send,
    d_recv,
):
    s, r = lax.axis_index("section"), lax.axis_index("row")
    n = kept.shape[1]
    on = active(s)
    off = jnp.logical_not(on)
    odd = lax.rem(s, 2) == 1
    mate = mate_of(s)
    after, before = next_of(s, ns)

    pass_coef = remote(low_part, kept, k_send, k_recv, mate, r)

    @pl.when(on)
    def _():
        sp = split(s_ref[...])
        nx = split(next_ref[...])
        iv = split(inv_ref[...])

        @pl.when(s != FIRST)
        def _():
            hi_ref[...], lo_ref[...] = split(dot3(iv, split(cross_ref[...]), NN))

        @pl.when(s == FIRST)
        def _():
            for step in range(1, nr):
                peer = lax.rem(r + step, nr)
                remote(cout, cin.at[peer], c_send.at[step], c_recv.at[peer], FIRST, peer).wait()

        @pl.when(s != FIRST)
        def _():
            remote(moved, probe, p_send, p_recv, before, r).wait_recv()

        p = probe[...]
        ahead = dot3(split(p), nx, NN)

        @pl.when(s != FIRST)
        def _():
            for q in range(nr):
                remote(cout, cin.at[q], c_send.at[q], c_recv.at[q], before, q).wait_recv()

        sums = [cin[0], cin[1]]
        for q in range(2, nr):
            sums[q % 2] = sums[q % 2] + cin[q]
        inner = split(unpacked(jnp.concatenate(sums, axis=1)))

        def hand_on(change):
            combine(1, packed(ahead - change), cout, dout, din, d_send, d_recv)
            for k in far_first(nr):
                remote(cout, cin.at[r], c_send.at[k], c_recv.at[r], after, lax.rem(r + k, nr)).start()

        @pl.when(s == FIRST)
        def _():
            hand_on(dot3(split(dot3(inner, iv, NN)), split(cross_ref[...]), NN))

        @pl.when((s != FIRST) & (s != LAST))
        def _():
            hand_on(dot3(inner, (hi_ref[...], lo_ref[...]), NN))

        coef = dot3(inner, iv, NN)
        low_part[...] = jnp.where(odd, coef[:, :n], coef[:, n:])
        kept[...] = jnp.where(odd, coef[:, n:], coef[:, :n])
        moved[...] = p - dot3(split(coef), sp, NT)

        @pl.when(s != LAST)
        def _():
            remote(moved, probe, p_send, p_recv, after, r).start()

        pass_coef.start()

        @pl.when(s == LAST)
        def _():
            m = split(moved[...])
            sq = dot3(m, m, NT)
            sout[...] = jnp.concatenate([sq, jnp.zeros((8, 120), F32)], axis=1)
            for step in range(1, nr):
                peer = lax.rem(r + step, nr)
                remote(sout, sin.at[r], s_send.at[step], s_recv.at[r], s, peer).start()
            sin[pl.ds(r, 1)] = sout[...][None]

    @pl.when(off)
    def _():
        pass_coef.wait_recv()

    coef = kept[...]
    coef_ref[...] = coef[:4]
    term = lax.dot_general(coef.astype(BF16), basis_ref[...], (NT, ((), ())), preferred_element_type=F32)
    for k in range(ns // 2):
        own[k] = term[:, k * 128 : (k + 1) * 128]
    outs = []
    for step in range(1, ns):
        t = lax.rem(s + step, ns)
        cp = remote(own.at[lax.div(t, 2)], oin.at[s], o_send.at[step], o_recv.at[s], t, r)
        cp.start()
        outs.append(cp)
    oin[pl.ds(s, 1)] = own[pl.ds(lax.div(s, 2), 1)]

    @pl.when(s == LAST)
    def _():
        for step in range(1, nr):
            peer = lax.rem(r + step, nr)
            remote(sout, sin.at[peer], s_send.at[step], s_recv.at[peer], s, peer).wait()
        tot = sin[0]
        for q in range(1, nr):
            tot = tot + sin[q]
        bout[...] = tot
        bcs = []
        for t in range(ns):
            if t != LAST:
                cp = remote(bout, bin_, b_send.at[t], b_recv, t, r)
                cp.start()
                bcs.append(cp)
        for cp in bcs:
            cp.wait_send()
        bin_[...] = tot

    for step in range(1, ns):
        t = lax.rem(s + step, ns)
        remote(own.at[0], oin.at[t], o_send.at[step], o_recv.at[t], t, r).wait_recv()
    removed = oin[0]
    for t in range(1, ns):
        removed = removed + oin[t]
    window = pl.ds(pl.multiple_of(lax.div(s, 2) * 128, 128), 128)
    remain = vec_ref[:, window].astype(F32) - removed[:4]
    remain = jnp.where(odd, remain[:, 64:], remain[:, :64])

    @pl.when(s != LAST)
    def _():
        remote(bout, bin_, b_send.at[0], b_recv, LAST, r).wait_recv()

    @pl.when(on & (s != LAST))
    def _():
        for q in range(nr):
            remote(cout, cin.at[q], c_send.at[q], c_recv.at[q], after, q).wait_send()
        remote(moved, probe, p_send, p_recv, after, r).wait_send()

    @pl.when(on)
    def _():
        pass_coef.wait_send()

    small = bin_[...]

    def at(i, k):
        return small[i : i + 1, k : k + 1]

    low = [[None] * 4 for _ in range(4)]
    rows = []
    for i in range(4):
        for k in range(i + 1):
            v = at(i, k)
            for m in range(k):
                v = v - low[i][m] * low[k][m]
            low[i][k] = jnp.sqrt(v) if i == k else v / low[k][k]
        x = remain[i : i + 1]
        for k in range(i):
            x = x - low[i][k] * rows[k]
        rows.append(x / low[i][i])
    ortho_ref[...] = jnp.concatenate(rows, axis=0)
    for cp in outs:
        cp.wait_send()


def eliminate(a):
    n = a.shape[0]
    cols = lax.broadcasted_iota(jnp.int32, (n, n), 1)
    lane = lax.broadcasted_iota(jnp.int32, (1, n), 1)
    sub = lax.broadcasted_iota(jnp.int32, (8, n), 0)
    for k in range(0, n, 4):
        c = [jnp.broadcast_to(a[:, k + i : k + i + 1], (n, n)) for i in range(4)]
        b = [[c[j][k + i : k + i + 1] for j in range(4)] for i in range(4)]
        inside = (lane >= k) & (lane < k + 4)
        r = [
            jnp.where(lane == k + i, 1.0, jnp.where(inside, 0.0, a[k + i : k + i + 1, :])) for i in range(4)
        ]
        e = 1.0 / (b[0][0] * b[1][1] - b[0][1] * b[0][1])
        a00, a01, a11 = b[1][1] * e, -b[0][1] * e, b[0][0] * e
        f00 = a00 * b[0][2] + a01 * b[1][2]
        f01 = a00 * b[0][3] + a01 * b[1][3]
        f10 = a01 * b[0][2] + a11 * b[1][2]
        f11 = a01 * b[0][3] + a11 * b[1][3]
        s00 = b[2][2] - (b[0][2] * f00 + b[1][2] * f10)
        s01 = b[2][3] - (b[0][2] * f01 + b[1][2] * f11)
        s11 = b[3][3] - (b[0][3] * f01 + b[1][3] * f11)
        g = 1.0 / (s00 * s11 - s01 * s01)
        z2 = r[2] - (f00 * r[0] + f10 * r[1])
        z3 = r[3] - (f01 * r[0] + f11 * r[1])
        w2 = g * (s11 * z2 - s01 * z3)
        w3 = g * (s00 * z3 - s01 * z2)
        w0 = (a00 * r[0] + a01 * r[1]) - (f00 * w2 + f01 * w3)
        w1 = (a01 * r[0] + a11 * r[1]) - (f10 * w2 + f11 * w3)
        base = jnp.where((cols >= k) & (cols < k + 4), 0.0, a)
        new = ((base - c[0] * w0) - c[1] * w1) - (c[2] * w2 + c[3] * w3)
        at = k // 8 * 8
        group = new[at : at + 8]
        for i, w in enumerate((w0, w1, w2, w3)):
            group = jnp.where(sub == k - at + i, jnp.broadcast_to(w, (8, n)), group)
        pieces = [new[:at], group, new[at + 8 :]]
        a = jnp.concatenate([p for p in pieces if p.shape[0]], axis=0)
    return a


FIRST, LAST = 1, 14


def active(s):
    x = lax.rem(s, 4)
    return (x == 1) | (x == 2)


def mate_of(s):
    return s + 1 - 2 * lax.rem(s, 2)


def next_of(s, ns):
    odd = lax.rem(s, 2) == 1
    return lax.rem(s + jnp.where(odd, 1, 3), ns), lax.rem(s + ns - jnp.where(odd, 3, 1), ns)


def pair_kernel(
    ns,
    nr,
    close,
    start_chain,
    s_ref,
    pair_ref,
    ahead_ref,
    uinv_ref,
    cross_ref,
    part,
    got,
    red,
    full,
    inv,
    early,
    late,
    mate_early,
    mate_late,
    n_send,
    n_recv,
    rs_send,
    rs_recv,
    ag_send,
    ag_recv,
    i_send,
    i_recv,
):
    s, r = lax.axis_index("section"), lax.axis_index("row")
    n = s_ref.shape[1]
    rows = n // nr
    on = active(s)
    off = jnp.logical_not(on)
    odd = lax.rem(s, 2) == 1
    even = lax.rem(s, 2) == 0
    mate = mate_of(s)
    low, high = pl.ds(0, n), pl.ds(n, n)
    x = lax.rem(s, 4)
    back = jnp.where(x == 1, 3, jnp.where(x == 2, 1, 2))
    last = lax.rem(s + ns - back, ns)
    to_mate = [
        remote(s_ref, pair_ref.at[:, where], n_send.at[0], n_recv.at[0], mate, r) for where in (low, high)
    ]
    to_last = [
        remote(s_ref, ahead_ref.at[:, where], n_send.at[1], n_recv.at[1 + k], last, r)
        for k, where in enumerate((low, high))
    ]

    def span(peer):
        return pl.ds(pl.multiple_of(peer * rows, rows), rows)

    def scatter(i, step):
        peer = lax.rem(r + step, nr)
        return remote(
            part.at[i, span(peer)], got.at[i, step], rs_send.at[i, step], rs_recv.at[i, step], s, peer
        )

    def gather(i, step, sending):
        peer = lax.rem(r + (step if sending else nr - step), nr)
        where = span(r if sending else peer)
        return remote(red.at[i], full.at[i, where], ag_send.at[i, step], ag_recv.at[i, step], s, peer)

    def begin(i):
        for step in far_first(nr)[:-1]:
            scatter(i, step).start()

    def middle(i):
        for step in range(1, nr):
            scatter(i, step).wait_recv()
        total = part[i, span(r), :]
        for step in range(1, nr):
            total = total + got[i, step]
        red[i] = total
        for step in far_first(nr)[:-1]:
            gather(i, step, True).start()
        full[i, span(r), :] = total

    def end(i):
        for step in range(1, nr):
            gather(i, step, False).wait_recv()
        for step in range(1, nr):
            scatter(i, step).wait_send()
            gather(i, step, True).wait_send()

    sp = split(s_ref[...])
    part[0] = dot3(sp, sp, TN)
    begin(0)
    close()

    for k, mine in enumerate((even, odd)):

        @pl.when(mine & off)
        def _():
            to_mate[k].start()

        @pl.when(mine & (s >= 2))
        def _():
            to_last[k].start()

        @pl.when(mine)
        def _():
            pair_ref[:, k * n : (k + 1) * n] = s_ref[...]

    middle(0)

    for k, mine in enumerate((even, odd)):

        @pl.when(mine & on)
        def _():
            to_mate[1 - k].wait_recv()

    @pl.when(on)
    def _():
        part[1] = dot3(split(pair_ref[:, :n]), split(pair_ref[:, n:]), TN)
        begin(1)

    end(0)

    def dot(x, y, dims):
        return lax.dot_general(x, y, (dims, ((), ())), precision=HI, preferred_element_type=F32)

    g = full[0]
    h = n // 2
    eye = lax.broadcasted_iota(jnp.int32, (n, n), 0) == lax.broadcasted_iota(jnp.int32, (n, n), 1)
    d = jnp.where(eye, g, 0.0)
    rs = lax.rsqrt(jnp.sum(d, axis=1, keepdims=True))
    cs = lax.rsqrt(jnp.sum(d, axis=0, keepdims=True))
    g = g * rs * cs
    a, b, c = g[:h, :h], g[:h, h:], g[h:, h:]
    ai = eliminate(a)
    t = dot(ai, b, NN)
    rest = c - dot(b, t, TN)
    early[0] = ai * rs[:h] * cs[:, :h]
    early[1] = t * rs[:h] / cs[:, h:]
    pass_early = remote(early, mate_early, i_send.at[0], i_recv.at[0], mate, r)
    pass_late = remote(late, mate_late, i_send.at[1], i_recv.at[1], mate, r)

    @pl.when(off)
    def _():
        pass_early.start()

    @pl.when(on)
    def _():
        middle(1)

    @pl.when(s == FIRST)
    def _():
        start_chain()

    late[...] = eliminate(rest) * rs[h:] * cs[:, h:]

    @pl.when(off)
    def _():
        pass_late.start()

    def whole_inverse(parts, corner):
        t, ci = parts[1], corner[...]
        u = dot(t, ci, NN)
        top = jnp.concatenate([parts[0] + dot(u, t, NT), -u], axis=1)
        bottom = jnp.concatenate([-u.T, ci], axis=1)
        return jnp.concatenate([top, bottom], axis=0)

    @pl.when(on)
    def _():
        inv[...] = whole_inverse(early, late)
        uinv_ref[n:, :n] = jnp.zeros((n, n), F32)

    @pl.when(on & (s != LAST))
    def _():
        for cp in to_last:
            cp.wait_recv()

    @pl.when(s == LAST)
    def _():
        ahead_ref[...] = jnp.zeros(ahead_ref.shape, F32)

    @pl.when(on)
    def _():
        cross_ref[...] = dot3(split(pair_ref[...]), split(ahead_ref[...]), TN)
        end(1)
        pass_early.wait_recv()
        pass_late.wait_recv()

    @pl.when(on & odd)
    def _():
        mine, theirs = inv[...], whole_inverse(mate_early, mate_late)
        right = dot3(split(full[1]), split(mine), NN)
        uinv_ref[n:, n:] = mine
        uinv_ref[:n, :n] = theirs
        uinv_ref[:n, n:] = -dot3(split(theirs), split(right), NN)

    @pl.when(on & even)
    def _():
        mine, theirs = inv[...], whole_inverse(mate_early, mate_late)
        left = dot3(split(mine), split(full[1]), NN)
        uinv_ref[:n, :n] = mine
        uinv_ref[n:, n:] = theirs
        uinv_ref[:n, n:] = -dot3(split(left), split(theirs), NN)

    @pl.when(off)
    def _():
        pass_early.wait_send()
        pass_late.wait_send()
        to_mate[0].wait_send()

    @pl.when(s >= 2)
    def _():
        to_last[0].wait_send()


def within(t, first, yes, no):
    return jnp.where(t >= first, yes, no)


def unit(t):
    def seg(first, width):
        return lax.div(jnp.maximum(t - first, 0), width), lax.rem(jnp.maximum(t - first, 0), width)

    a, b = seg(4, 2)
    row, half, col = within(t, 2, 0, 0), lax.rem(t, 2), within(t, 2, 0, 4)
    row, half, col = row, within(t, 4, b, half), within(t, 4, 1 + a, col)
    a, b = seg(8, 3)
    row, half, col = within(t, 8, 1 + a, row), within(t, 8, a, half), within(t, 8, b, col)
    row, half, col = within(t, 14, 0, row), within(t, 14, t - 14, half), within(t, 14, 3, col)
    row, half, col = within(t, 16, t - 15, row), within(t, 16, t - 16, half), within(t, 16, 3, col)
    a, b = seg(18, 4)
    row, half, col = within(t, 18, 1 + a, row), within(t, 18, 1 - a, half), within(t, 18, b, col)
    a, b = seg(26, 4)
    row, half, col = within(t, 26, 3, row), within(t, 26, a, half), within(t, 26, b, col)
    return row, half, col


def slot_offset(d):
    return jnp.where(d == 0, 0, jnp.where(d == 1, 3, d - 1))


UNITS = 34
HOME = 1
REACH = 4
LAG = 4


def sketch_kernel(
    nz,
    omega_ref,
    basis_ref,
    vec_ref,
    s_ref,
    p_ref,
    obuf,
    bbuf,
    part,
    dbuf,
    rbuf,
    fbuf,
    l_sem,
    o_send,
    o_recv,
    b_send,
    b_recv,
    d_send,
    d_recv,
    r_send,
    r_recv,
    f_send,
    f_recv,
    p_send,
    p_recv,
):
    s, r = lax.axis_index("section"), lax.axis_index("row")
    y, x = lax.div(s, 4), lax.rem(s, 4)
    z, c = lax.div(r, 2), lax.rem(r, 2)

    def at(dy, dx):
        return lax.rem(y + dy, 4) * 4 + lax.rem(x + dx, 4)

    beside = (lax.rem(z + 1, nz) * 2 + c, lax.rem(z + nz - 1, nz) * 2 + c)
    mate = z * 2 + (1 - c)

    local = [
        pltpu.make_async_copy(omega_ref, obuf.at[0], l_sem.at[0]),
        pltpu.make_async_copy(basis_ref, bbuf.at[0], l_sem.at[1]),
    ]
    for cp in local:
        cp.start()

    barrier = pltpu.get_barrier_semaphore()
    ns, nr = 16, 2 * nz

    def hello(section, row):
        pl.semaphore_signal(barrier, inc=1, device_id=(section, row), device_id_type=MESH)

    for q in range(nr):
        for other in next_of(s, ns):
            hello(other, q)
    for step in range(1, nr):
        hello(s, lax.rem(r + step, nr))
    for step in range(1, ns):
        hello(lax.rem(s + step, ns), r)

    v = vec_ref[...].astype(F32)
    v = jnp.concatenate([v, jnp.zeros_like(v)], axis=0)
    v = jnp.concatenate([v, jnp.zeros((120, v.shape[1]), F32)], axis=0)
    bbuf[4, :, :128] = v.T.astype(BF16)
    bbuf[4, :, 128:] = jnp.zeros((v.shape[1], bbuf.shape[2] - 128), BF16)
    for cp in local:
        cp.wait()
    pl.semaphore_wait(barrier, 3 * nr + ns - 2)

    def ocopy(src, dst, half, sem, dy):
        return remote(obuf.at[src, half], obuf.at[dst, half], o_send.at[sem], o_recv.at[sem], at(dy, 0), r)

    def bcopy(src, dst, half, sem, dx):
        a, b = bbuf.at[src], bbuf.at[dst]
        if half is not None:
            a, b = a.at[pl.ds(512 * half, 512)], b.at[pl.ds(512 * half, 512)]
        return remote(a, b, b_send.at[sem], b_recv.at[sem], at(0, dx), r)

    b_own = [bcopy(0, 1, None, 0, 1), bcopy(0, 2, None, 1, 3)]
    o_own = [ocopy(0, 1, 0, 0, 1), ocopy(0, 2, 1, 1, 3)]
    o_rest = [ocopy(0, 1, 1, 2, 1), ocopy(0, 2, 0, 3, 3)]
    b_fwd = [bcopy(1, 3, 0, 2, 1), bcopy(2, 3, 1, 3, 3)]
    o_fwd = [ocopy(1, 3, 0, 4, 1), ocopy(2, 3, 1, 5, 3)]
    for cp in o_own + b_own + o_rest:
        cp.start()

    def dcopy(u):
        return remote(part.at[u, :, 1 - c], dbuf.at[u], d_send.at[u], d_recv.at[u], s, mate)

    def chunk(d, k):
        far = REACH - k
        return lax.rem(z + (far if d == 0 else nz - far), nz)

    def rcopy(u, d, k):
        return remote(
            part.at[u, chunk(d, k), c],
            rbuf.at[u, d, k],
            r_send.at[u, d, k],
            r_recv.at[u, d, k],
            s,
            beside[d],
        )

    def place(u):
        row, half, col = unit(u)
        dy, dx = slot_offset(row), slot_offset(col)
        start = (lax.rem(y + dy, 4) * 4 + x) * 32 + half * 16
        return dx, pl.ds(pl.multiple_of(start, 16), 16)

    def fcopy(u):
        dx, rows = place(u)
        return remote(fbuf.at[u], s_ref.at[rows], f_send.at[u], f_recv.at[u], at(0, dx), r)

    def pcopy(u, sender):
        return remote(fbuf.at[u], p_ref.at[sender, u], p_send.at[u], p_recv.at[sender, u], HOME, r)

    def step(t, carry):
        done = t - 2 - LAG * REACH

        @pl.when((done >= 0) & (done < UNITS))
        def _():
            rcopy(done, 0, REACH - 1).wait_recv()
            rcopy(done, 1, REACH - 1).wait_recv()
            fbuf[done] = (part[done, z, c] + dbuf[done, z]) + (
                rbuf[done, 0, REACH - 1] + rbuf[done, 1, REACH - 1]
            )

        @pl.when((done >= 2) & (done < UNITS))
        def _():
            dx, rows = place(done)

            @pl.when(dx == 0)
            def _():
                s_ref[rows, :] = fbuf[done]

            @pl.when(dx > 0)
            def _():
                fcopy(done).start()

        @pl.when((done >= 0) & (done < 2))
        def _():
            @pl.when(s == HOME)
            def _():
                p_ref[HOME, done] = fbuf[done]

            @pl.when(s != HOME)
            def _():
                pcopy(done, s).start()

        for k in range(REACH - 1, -1, -1):
            u = t - 2 - LAG * k
            valid = (u >= 0) & (u < UNITS)
            if k == 0:

                @pl.when(valid)
                def _():
                    dcopy(u).wait_recv()

            for d in range(2):
                longer = lax.rem(jnp.maximum(u, 0), 2) == d

                def own():
                    return part[u, chunk(d, k), c] + dbuf[u, chunk(d, k)]

                def send(val):
                    part[u, chunk(d, k), c] = val
                    rcopy(u, d, k).start()

                def pass_on():
                    rcopy(u, d, k - 1).wait_recv()
                    send(own() + rbuf[u, d, k - 1])

                if k == 0:

                    @pl.when(valid & longer)
                    def _():
                        send(own())

                elif k == 1:

                    @pl.when(valid & longer)
                    def _():
                        pass_on()

                    @pl.when(valid & jnp.logical_not(longer))
                    def _():
                        send(own())

                else:

                    @pl.when(valid)
                    def _():
                        pass_on()

        @pl.when(t == 4)
        def _():
            for cp in b_own:
                cp.wait_recv()
            for cp in b_fwd:
                cp.start()

        @pl.when(t == 8)
        def _():
            for cp in o_own:
                cp.wait_recv()
            for cp in o_fwd:
                cp.start()

        @pl.when(t == 14)
        def _():
            for cp in b_fwd:
                cp.wait_recv()

        @pl.when(t == 18)
        def _():
            for cp in o_rest:
                cp.wait_recv()

        @pl.when(t == 26)
        def _():
            for cp in o_fwd:
                cp.wait_recv()

        @pl.when(t < UNITS)
        def _():
            row, half, col = unit(t)
            out = jnp.dot(obuf[row, half], bbuf[col], preferred_element_type=F32)
            part[t] = out.reshape(part.shape[1:])
            dcopy(t).start()

        return carry

    lax.fori_loop(0, UNITS + 2 + LAG * REACH + 1, step, 0)

    def finish(u, carry):
        dx, _ = place(u)

        @pl.when(dx > 0)
        def _():
            fcopy(u).wait_recv()

        return carry

    lax.fori_loop(2, UNITS, finish, 0)

    @pl.when(s == HOME)
    def _():
        for t in range(16):
            if t != HOME:
                for u in range(2):
                    pcopy(u, t).wait_recv()

    def drain(u, carry):
        dcopy(u).wait_send()
        dx, _ = place(u)

        @pl.when((u >= 2) & (dx > 0))
        def _():
            fcopy(u).wait_send()

        for d in range(2):
            for k in range(REACH):
                if k:
                    rcopy(u, d, k).wait_send()
                else:

                    @pl.when(lax.rem(u, 2) == d)
                    def _():
                        rcopy(u, d, k).wait_send()

        return carry

    def close():
        @pl.when(s != HOME)
        def _():
            for u in range(2):
                pcopy(u, s).wait_send()

        for cp in b_own + o_own + o_rest + b_fwd + o_fwd:
            cp.wait_send()
        lax.fori_loop(0, UNITS, drain, 0)

    return close


def sketch_scratch(m, k, n, nr):
    nz, piece, dma = nr // 2, m // nr // 2, pltpu.SemaphoreType.DMA
    return [
        pltpu.VMEM((4, 2, m // 2, k), BF16),
        pltpu.VMEM((5, k, n), BF16),
        pltpu.VMEM((UNITS, nz, 2, piece, n), F32),
        pltpu.VMEM((UNITS, nz, piece, n), F32),
        pltpu.VMEM((UNITS, 2, REACH, piece, n), F32),
        pltpu.VMEM((UNITS, piece, n), F32),
        dma((2,)),
        dma((6,)),
        dma((6,)),
        dma((4,)),
        dma((4,)),
        dma((UNITS,)),
        dma((UNITS,)),
        dma((UNITS, 2, REACH)),
        dma((UNITS, 2, REACH)),
        dma((UNITS,)),
        dma((UNITS,)),
        dma((2,)),
        dma((16, 2)),
    ]


def pair_scratch(n, nr):
    dma = pltpu.SemaphoreType.DMA
    return [
        pltpu.VMEM((2, n, n), F32),
        pltpu.VMEM((2, nr, n // nr, n), F32),
        pltpu.VMEM((2, n // nr, n), F32),
        pltpu.VMEM((2, n, n), F32),
        pltpu.VMEM((n, n), F32),
        pltpu.VMEM((2, n // 2, n // 2), F32),
        pltpu.VMEM((n // 2, n // 2), F32),
        pltpu.VMEM((2, n // 2, n // 2), F32),
        pltpu.VMEM((n // 2, n // 2), F32),
        dma((3,)),
        dma((3,)),
        dma((2, nr)),
        dma((2, nr)),
        dma((2, nr)),
        dma((2, nr)),
        dma((2,)),
        dma((2,)),
    ]


def chain_scratch(k, n, ns, nr):
    dma = pltpu.SemaphoreType.DMA
    return [
        pltpu.VMEM((n, n), BF16),
        pltpu.VMEM((n, n), BF16),
        pltpu.VMEM((8, n // 2), F32),
        pltpu.VMEM((8, n // 2), F32),
        pltpu.VMEM((8, k), F32),
        pltpu.VMEM((8, k), F32),
        pltpu.VMEM((8, 128), F32),
        pltpu.VMEM((nr, 8, 128), F32),
        pltpu.VMEM((ns // 2, 8, 128), F32),
        pltpu.VMEM((ns, 8, 128), F32),
        pltpu.VMEM((8, 128), F32),
        pltpu.VMEM((nr, 8, 128), F32),
        pltpu.VMEM((8, 128), F32),
        pltpu.VMEM((8, 128), F32),
        dma((nr,)),
        dma((nr,)),
        dma,
        dma,
        dma((ns,)),
        dma((ns,)),
        dma((nr,)),
        dma((nr,)),
        dma((ns,)),
        dma,
        dma,
        dma,
        pltpu.VMEM((2, 8, 128), F32),
        pltpu.VMEM((2, 8, 128), F32),
        dma((2,)),
        dma((2,)),
    ]


def whole_kernel(ns, nr, ends, omega_ref, basis_ref, vec_ref, ortho_ref, coef_ref, *rest):
    s_ref, p_ref, pair_ref, ahead_ref, uinv_ref, cross_ref = rest[:6]
    first, second = rest[6 : ends[0]], rest[ends[0] : ends[1]]
    third = rest[ends[1] :]
    close = sketch_kernel(nr // 2, omega_ref, basis_ref, vec_ref, s_ref, p_ref, *first)

    def start_chain():
        first_products(nr, pair_ref, p_ref, third)

    pair_kernel(
        ns, nr, close, start_chain, s_ref, pair_ref, ahead_ref, uinv_ref, cross_ref, *second
    )
    own_basis = first[1].at[0]
    chain_kernel(
        ns,
        nr,
        pair_ref,
        ahead_ref,
        uinv_ref,
        cross_ref,
        own_basis,
        vec_ref,
        ortho_ref,
        coef_ref,
        *third,
    )


def whole_call(omega, basis, vectors, ns, nr):
    vm = pl.BlockSpec(memory_space=pltpu.VMEM)
    anym = pl.BlockSpec(memory_space=pl.ANY)
    m, k = omega.shape
    n = basis.shape[1]
    kept = [
        pltpu.VMEM((m, n), F32),
        pltpu.VMEM((ns, 2, m // nr // 2, n), F32),
        pltpu.VMEM((m, 2 * n), F32),
        pltpu.VMEM((m, 2 * n), F32),
        pltpu.VMEM((2 * n, 2 * n), F32),
        pltpu.VMEM((2 * n, 2 * n), F32),
    ]
    one = sketch_scratch(m, k, n, nr)
    two = pair_scratch(n, nr)
    three = chain_scratch(m, 2 * n, ns, nr)
    ends = (len(kept) + len(one), len(kept) + len(one) + len(two))
    return pl.pallas_call(
        functools.partial(whole_kernel, ns, nr, ends),
        out_shape=(
            jax.ShapeDtypeStruct((4, vectors.shape[1] // ns), F32),
            jax.ShapeDtypeStruct((4, n), F32),
        ),
        in_specs=[anym, anym, vm],
        out_specs=(vm, vm),
        scratch_shapes=kept + one + two + three,
        compiler_params=pltpu.CompilerParams(
            collective_id=0, has_side_effects=True, vmem_limit_bytes=60 * 1024 * 1024
        ),
    )(omega.reshape(2, m // 2, k), basis, vectors)


def body(omega, basis, vectors):
    return whole_call(omega, basis, vectors, lax.axis_size("section"), lax.axis_size("row"))


def solution(mesh):
    placed = (P("section", "row"), P("row", "section"), P(None, "row"))
    return jax.shard_map(
        body,
        mesh=mesh,
        in_specs=placed,
        out_specs=(P(None, ("row", "section")), P(None, "section")),
        check_vma=False,
    )
```
